16 devices in a mesh: dp: 2 (over y, z), sp: 8 (over x, core).
Axes of the slice: x: 4, y: 2, z: 1, core: 2. Of those that a mesh axis runs over, the one named last changes fastest.
The devices are a block of a 4x4x8 slice.
Arguments:
- hidden: bfloat16 [16, 1024, 2048], P('dp', 'sp'), parts along dimension 0
- norm_w: bfloat16 [2048], replicated
- w_qkv: bfloat16 [2048, 3072], replicated
- w_out: bfloat16 [32, 64, 2048], replicated
- long_factor: float32 [32], replicated
- grad_out: bfloat16 [16, 1024, 2048], P('dp', 'sp'), parts along dimension 0
Outputs:
- output 1: bfloat16 [16, 1024, 2048], P('dp', 'sp'), parts along dimension 0
- output 2: bfloat16 [16, 1024, 2048], P('dp', 'sp'), parts along dimension 0
- output 3: float32 [4096, 3072], P('dp'), parts along dimension 0
- output 4: float32 [64, 64, 2048], P('dp'), parts along dimension 0
- output 5: float32 [4096], P('dp'), parts along dimension 0
There are 2 independent parts. The reference program is written for one: setup_inputs(seed, part) draws one part's arguments, and reference() takes and returns one part's arrays. A program takes and returns all parts, laid end to end along the dimension named above; an argument that names none is the same for every part.
All inputs are finite; a program needn't handle non-finite values.
Results may differ from the reference program's by a relative error of at most 0.0104791.
Values are sent between devices in bfloat16 or wider.
A program may use at most 768 MiB of HBM per device.

```python
import math
import jax
import jax.numpy as jnp
from jax import lax

N_BATCH = 8
SEQ_LEN = 1024
D_MODEL = 2048
N_HEADS = 32
N_KV_HEADS = 8
HEAD_DIM = 64
ROT_DIM = 64

Q_WIDTH = N_HEADS * HEAD_DIM
KV_WIDTH = N_KV_HEADS * HEAD_DIM
QKV_WIDTH = Q_WIDTH + 2 * KV_WIDTH
GROUP_SIZE = N_HEADS // N_KV_HEADS
HALF_ROT = ROT_DIM // 2
NORM_EPS = 1e-5
ROPE_BASE = 10000.0
ROPE_GAIN = math.sqrt(1.0 + math.log(32.0) / math.log(4096.0))
MASK_VALUE = -1e30


def setup_inputs(seed: int = 0, part: int = 0) -> dict:
    part_key = jax.random.fold_in(jax.random.key(seed), part)
    key_hidden, key_grad = jax.random.split(part_key, 2)
    key_norm, key_qkv, key_out, key_factor = jax.random.split(jax.random.key(seed + 1), 4)
    act_shape = (N_BATCH, SEQ_LEN, D_MODEL)
    hidden = jax.random.normal(key_hidden, act_shape, jnp.float32)
    grad_out = jax.random.normal(key_grad, act_shape, jnp.float32)
    norm_w = jax.random.uniform(key_norm, (D_MODEL,), jnp.float32, 0.5, 1.5)
    w_qkv = jax.random.normal(key_qkv, (D_MODEL, QKV_WIDTH), jnp.float32) * (D_MODEL ** -0.5)
    out_std = (SEQ_LEN / (64.0 * Q_WIDTH)) ** 0.5
    w_out = jax.random.normal(key_out, (N_HEADS, HEAD_DIM, D_MODEL), jnp.float32) * out_std
    long_factor = jnp.exp(jax.random.uniform(key_factor, (HALF_ROT,), jnp.float32, 0.0, math.log(48.0)))
    return {
        'hidden': hidden.astype(jnp.bfloat16),
        'norm_w': norm_w.astype(jnp.bfloat16),
        'w_qkv': w_qkv.astype(jnp.bfloat16),
        'w_out': w_out.astype(jnp.bfloat16),
        'long_factor': long_factor,
        'grad_out': grad_out.astype(jnp.bfloat16),
    }


def to_grid(values):
    return values.astype(jnp.bfloat16).astype(jnp.float32)


def rope_tables(long_factor):
    positions = jnp.arange(SEQ_LEN).astype(jnp.float32)
    exponent = jnp.arange(HALF_ROT).astype(jnp.float32) / HALF_ROT
    inv_freq = 1.0 / (long_factor.astype(jnp.float32) * jnp.power(ROPE_BASE, exponent))
    angles = positions[:, None] * inv_freq[None, :]
    return jnp.cos(angles) * ROPE_GAIN, jnp.sin(angles) * ROPE_GAIN


def rotate(head_vals, cos_t, sin_t):
    cos_b = cos_t[None, :, None, :]
    sin_b = sin_t[None, :, None, :]
    first_half = head_vals[..., :HALF_ROT]
    second_half = head_vals[..., HALF_ROT:ROT_DIM]
    return jnp.concatenate([first_half * cos_b - second_half * sin_b, second_half * cos_b + first_half * sin_b, head_vals[..., ROT_DIM:]], axis=-1)


def head_attention(q_head, k_head, v_head):
    causal = jnp.arange(SEQ_LEN)[:, None] >= jnp.arange(SEQ_LEN)[None, :]
    scores = jnp.einsum('bqe,bse->bqs', q_head, k_head) * (HEAD_DIM ** -0.5)
    prob_mat = to_grid(jax.nn.softmax(jnp.where(causal[None], scores, MASK_VALUE), axis=-1))
    return to_grid(jnp.einsum('bqs,bse->bqe', prob_mat, v_head))


def attention(queries, key_vals, value_vals):
    head_major = jnp.moveaxis(queries, 2, 0)
    kv_index = jnp.arange(N_HEADS) // GROUP_SIZE
    saved_head = jax.checkpoint(head_attention)

    def one_head(operand):
        q_head, kv_id = operand
        k_head = lax.dynamic_index_in_dim(key_vals, kv_id, axis=2, keepdims=False)
        v_head = lax.dynamic_index_in_dim(value_vals, kv_id, axis=2, keepdims=False)
        return saved_head(q_head, k_head, v_head)

    per_head = lax.map(one_head, (head_major, kv_index))
    return jnp.moveaxis(per_head, 0, 2)


def block_forward(hidden_f, gain, w_qkv_f, w_out_f, cos_t, sin_t):
    inv_rms = lax.rsqrt(jnp.mean(hidden_f * hidden_f, axis=-1, keepdims=True) + NORM_EPS)
    normed = to_grid(hidden_f * inv_rms * gain)
    fused_qkv = jnp.dot(normed.reshape(N_BATCH * SEQ_LEN, D_MODEL), w_qkv_f, preferred_element_type=jnp.float32)
    fused_qkv = fused_qkv.reshape(N_BATCH, SEQ_LEN, QKV_WIDTH)
    queries = fused_qkv[..., :Q_WIDTH].reshape(N_BATCH, SEQ_LEN, N_HEADS, HEAD_DIM)
    key_vals = fused_qkv[..., Q_WIDTH:Q_WIDTH + KV_WIDTH].reshape(N_BATCH, SEQ_LEN, N_KV_HEADS, HEAD_DIM)
    value_vals = fused_qkv[..., Q_WIDTH + KV_WIDTH:].reshape(N_BATCH, SEQ_LEN, N_KV_HEADS, HEAD_DIM)
    attn_out = attention(to_grid(rotate(queries, cos_t, sin_t)), to_grid(rotate(key_vals, cos_t, sin_t)), to_grid(value_vals))
    projected = jnp.dot(attn_out.reshape(N_BATCH * SEQ_LEN, Q_WIDTH), w_out_f.reshape(Q_WIDTH, D_MODEL), preferred_element_type=jnp.float32)
    return (hidden_f + projected.reshape(N_BATCH, SEQ_LEN, D_MODEL)).astype(jnp.bfloat16)


def reference(hidden, norm_w, w_qkv, w_out, long_factor, grad_out):
    cos_t, sin_t = rope_tables(long_factor)

    def forward(hidden_f, gain, w_qkv_f, w_out_f):
        return block_forward(hidden_f, gain, w_qkv_f, w_out_f, cos_t, sin_t)

    block_out, pullback = jax.vjp(forward, hidden.astype(jnp.float32), norm_w.astype(jnp.float32), w_qkv.astype(jnp.float32), w_out.astype(jnp.float32))
    grad_hidden, grad_norm_w, grad_w_qkv, grad_w_out = pullback(grad_out)
    return (block_out, grad_hidden.astype(jnp.bfloat16), grad_w_qkv, grad_w_out, grad_norm_w)
```

```python
import functools
import math

import jax
import jax.numpy as jnp
from jax import lax
from jax.experimental import pallas as pl
from jax.experimental.pallas import tpu as pltpu
from jax.sharding import Mesh, PartitionSpec as P

NORM_EPS = 1e-5
ROPE_BASE = 10000.0
ROPE_GAIN = math.sqrt(1.0 + math.log(32.0) / math.log(4096.0))
MASK_VALUE = -1e30
LOG2E = math.log2(math.e)
CORES = 2
BF16 = jnp.bfloat16
F32 = jnp.float32
VMEM_LIMIT = 60 * 1024 * 1024

NN = (((1,), (0,)), ((), ()))
NT = (((1,), (1,)), ((), ()))
TN = (((0,), (0,)), ((), ()))


def dot(a, b, dims=NN):
    return lax.dot_general(a, b, dims, preferred_element_type=F32)


def cost(flops, nbytes, trans=0):
    return pl.CostEstimate(flops=int(flops), bytes_accessed=int(nbytes), transcendentals=int(trans))


def params(n_axes=1):
    return pltpu.CompilerParams(dimension_semantics=("arbitrary",) * n_axes, vmem_limit_bytes=VMEM_LIMIT)


def rope_rows(block, cos, sin, direction):
    half = cos.shape[0]
    a, b = block[:half], block[half:2 * half]
    s = sin * direction
    return jnp.concatenate([a * cos - b * s, b * cos + a * s], axis=0)


def kv_proj_kernel(x_ref, g_ref, wk_ref, wv_ref, cos_ref, sin_ref, h_ref, kv_ref):
    nb, tok, d = x_ref.shape
    kvh, _, e2, _ = kv_ref.shape
    e = e2 // 2
    x = x_ref[...].reshape(nb * tok, d).astype(F32)
    inv = lax.rsqrt(jnp.mean(x * x, axis=-1, keepdims=True) + NORM_EPS)
    h = (x * inv * g_ref[...].astype(F32)).astype(BF16)
    h_ref[...] = h.reshape(nb, tok, d)
    cos, sin = cos_ref[...], sin_ref[...]
    k = dot(wk_ref[...], h, NT)
    for i in range(kvh):
        for b in range(nb):
            kv_ref[i, b, 0:e] = rope_rows(k[i * e:(i + 1) * e, b * tok:(b + 1) * tok], cos, sin, 1.0).astype(BF16)
    v = dot(wv_ref[...], h, NT)
    for i in range(kvh):
        for b in range(nb):
            kv_ref[i, b, e:2 * e] = v[i * e:(i + 1) * e, b * tok:(b + 1) * tok].astype(BF16)


def q_proj_kernel(h_ref, w_ref, cos_ref, sin_ref, q_ref):
    nb, tok, d = h_ref.shape
    e = 2 * cos_ref.shape[0]
    rows = w_ref.shape[0]
    h = h_ref[...].reshape(nb * tok, d)
    cos, sin = cos_ref[...], sin_ref[...]
    scale = e ** -0.5
    step = 4 * e
    for r in range(0, rows, step):
        blk = dot(w_ref[r:r + step], h, NT)
        for i in range(0, step, e):
            for b in range(nb):
                q_ref[b, r + i:r + i + e] = (rope_rows(blk[i:i + e, b * tok:(b + 1) * tok], cos, sin, 1.0).astype(BF16)
                                             * scale).astype(BF16)


def do_proj_kernel(g_ref, w_ref, o_ref):
    nb, tok, d = g_ref.shape
    rows = w_ref.shape[0]
    g = g_ref[...].reshape(nb * tok, d)
    step = 256
    for r in range(0, rows, step):
        blk = dot(w_ref[r:r + step], g, NT)
        for b in range(nb):
            o_ref[b, r:r + step] = blk[:, b * tok:(b + 1) * tok].astype(BF16)


def drop_scalar(kernel):
    def wrapped(_, *refs):
        kernel(*refs)
    return wrapped


def attn_kernel(ids, q0_ref, q1_ref, do0_ref, do1_ref, kv_ref, h0_ref, h1_ref, g0_ref, g1_ref, cos_ref, sin_ref,
                own_ref, par_ref, send_ref, s_ref, acc_ref, kvt_ref, gacc_ref):
    chip, core = ids[0], ids[1]
    b_id = pl.program_id(0)
    chips = kv_ref.shape[0]
    rows, tok = q0_ref.shape[1], q0_ref.shape[2]
    e = kv_ref.shape[3] // 2
    reps = rows // e
    blk = 2 * tok
    width = reps * blk

    def heads_to_lanes(first_ref, second_ref):
        full = jnp.concatenate([first_ref[0], second_ref[0]], axis=1)
        return jnp.concatenate([full[i * e:(i + 1) * e] for i in range(reps)], axis=1)

    qt = heads_to_lanes(q0_ref, q1_ref)
    dot_t = heads_to_lanes(do0_ref, do1_ref)
    zero = jnp.zeros_like(qt)
    q_pad = jnp.concatenate([qt, zero], axis=0)
    do_pad = jnp.concatenate([zero, dot_t], axis=0)

    def kv_block(j):
        return jnp.concatenate([kv_ref[j, 0, 0], kv_ref[j, 1, 0]], axis=1)

    def forward_block(j, masked, m_old, l_old):
        kv = kv_block(j)
        kvt = kv.T
        kvt_ref[j] = kvt
        v_t = kv[e:2 * e]
        ms, ls = [], []
        for i in range(reps):
            cols = slice(i * blk, (i + 1) * blk)
            t = dot(kvt, q_pad[:, cols]) * LOG2E
            if masked:
                r = lax.broadcasted_iota(jnp.int32, (blk, blk), 0)
                c = lax.broadcasted_iota(jnp.int32, (blk, blk), 1)
                shift = (1 - 2 * core) * tok
                k_pos = jnp.where(r < tok, r, r - tok + shift)
                q_pos = jnp.where(c < tok, c, c - tok + shift)
                t = jnp.where(k_pos <= q_pos, t, MASK_VALUE)
            s_ref[j, :, cols] = t
            mx = jnp.max(t, axis=0, keepdims=True)
            if masked:
                m_new = mx
                p = jnp.exp2(t - m_new)
                l_new = jnp.sum(p, axis=0, keepdims=True)
                acc_ref[:, cols] = dot(v_t, p.astype(BF16))
            else:
                mo = m_old[:, cols]
                m_new = jnp.maximum(mo, mx)
                p = jnp.exp2(t - m_new)
                alpha = jnp.exp2(mo - m_new)
                l_new = l_old[:, cols] * alpha + jnp.sum(p, axis=0, keepdims=True)
                acc_ref[:, cols] = acc_ref[:, cols] * alpha + dot(v_t, p.astype(BF16))
            ms.append(m_new)
            ls.append(l_new)
        return jnp.concatenate(ms, axis=1), jnp.concatenate(ls, axis=1)

    m, l = forward_block(chip, True, None, None)
    m, l = lax.fori_loop(0, chip, lambda j, ml: forward_block(j, False, *ml), (m, l))

    o_t = acc_ref[...] * (1.0 / l)
    delta = jnp.sum(o_t * dot_t.astype(F32), axis=0, keepdims=True)
    lse = m + jnp.log2(l)
    o_b = o_t.astype(BF16)

    def backward_block(j, first):
        kv = kv_block(j)
        kvt = kvt_ref[j]
        k_t = kv[0:e]
        dk = jnp.zeros((e, blk), F32)
        dv = jnp.zeros((e, blk), F32)
        for i in range(reps):
            cols = slice(i * blk, (i + 1) * blk)
            p = jnp.exp2(s_ref[j, :, cols] - lse[:, cols])
            dp = dot(kvt, do_pad[:, cols])
            ds = (p * (dp - delta[:, cols])).astype(BF16)
            dv = dv + dot(dot_t[:, cols], p.astype(BF16), NT)
            dk = dk + dot(qt[:, cols], ds, NT)
            dq = dot(k_t, ds)
            if first:
                acc_ref[:, cols] = dq
            else:
                acc_ref[:, cols] = acc_ref[:, cols] + dq
        send_ref[j, 0:2 * e, pl.ds(pl.multiple_of(b_id * blk, blk), blk)] = jnp.concatenate([dk, dv], axis=0).astype(BF16)

    backward_block(chip, True)

    def backward_step(j, carry):
        backward_block(j, False)
        return carry

    lax.fori_loop(0, chip, backward_step, 0)

    def zero_step(j, carry):
        send_ref[j, 0:2 * e, pl.ds(pl.multiple_of(b_id * blk, blk), blk)] = jnp.zeros((2 * e, blk), BF16)
        return carry

    lax.fori_loop(chip + 1, chips, zero_step, 0)

    cos = jnp.concatenate([cos_ref[0], cos_ref[1]], axis=1)
    sin = jnp.concatenate([sin_ref[0], sin_ref[1]], axis=1)
    o_rows, dq_rows = [], []
    for i in range(reps):
        cols = slice(i * blk, (i + 1) * blk)
        o_rows.append(o_b[:, cols])
        dq = (acc_ref[:, cols] * (e ** -0.5)).astype(BF16).astype(F32)
        dq_rows.append(rope_rows(dq, cos, sin, -1.0).astype(BF16))
    o_full = jnp.concatenate(o_rows, axis=0)
    dq_full = jnp.concatenate(dq_rows, axis=0)
    own_ref[0, 0] = o_full[:, :tok]
    par_ref[0, 0] = o_full[:, tok:]
    own_ref[1, 0] = dq_full[:, :tok]
    par_ref[1, 0] = dq_full[:, tok:]

    d = h0_ref.shape[2]
    step = 512

    @pl.when(b_id == 0)
    def _():
        gacc_ref[...] = jnp.zeros_like(gacc_ref)

    for c in range(0, d, step):
        cs = slice(c, c + step)
        hh = jnp.concatenate([h0_ref[0, :, cs], h1_ref[0, :, cs]], axis=0)
        gg = jnp.concatenate([g0_ref[0, :, cs], g1_ref[0, :, cs]], axis=0)
        gacc_ref[0:rows, cs] += dot(dq_full, hh)
        gacc_ref[rows:2 * rows, cs] += dot(o_full, gg)

    @pl.when(b_id == pl.num_programs(0) - 1)
    def _():
        for j in range(chips):
            n = rows // chips
            send_ref[j, 2 * e:2 * e + n] = gacc_ref[j * n:(j + 1) * n].astype(BF16)
            send_ref[j, 2 * e + n:2 * e + 2 * n] = gacc_ref[rows + j * n:rows + (j + 1) * n].astype(BF16)


def kv_grad_kernel(*refs, stages):
    recv = refs[:stages]
    h0_ref, h1_ref, cos_ref, sin_ref, own_ref, par_ref, send_ref, gacc_ref = refs[stages:]
    b_id = pl.program_id(0)
    tok = h0_ref.shape[1]
    e2 = own_ref.shape[1] // stages
    e = e2 // 2
    cos = jnp.concatenate([cos_ref[0], cos_ref[1]], axis=1)
    sin = jnp.concatenate([sin_ref[0], sin_ref[1]], axis=1)
    parts = []
    for r in recv:
        total = r[0].astype(F32)
        for j in range(1, r.shape[0]):
            total = total + r[j].astype(F32)
        total = total.astype(BF16).astype(F32)
        parts.append(jnp.concatenate([rope_rows(total[0:e], cos, sin, -1.0), total[e:2 * e]], axis=0).astype(BF16))
    gf = jnp.concatenate(parts, axis=0)
    own_ref[0] = gf[:, :tok]
    par_ref[0] = gf[:, tok:]

    @pl.when(b_id == 0)
    def _():
        gacc_ref[...] = jnp.zeros_like(gacc_ref)

    d = h0_ref.shape[2]
    step = 512
    for c in range(0, d, step):
        cs = slice(c, c + step)
        hh = jnp.concatenate([h0_ref[0, :, cs], h1_ref[0, :, cs]], axis=0)
        gacc_ref[:, cs] += dot(gf, hh)

    @pl.when(b_id == pl.num_programs(0) - 1)
    def _():
        n = send_ref.shape[1]
        for j in range(send_ref.shape[0]):
            send_ref[j] = gacc_ref[j * n:(j + 1) * n].astype(BF16)


def out_kernel(ids, x_ref, w_ref, *refs, stages):
    core = ids[1]
    o_refs, y_ref = refs[:-1], refs[-1]
    nb, tok, d = x_ref.shape
    rows = o_refs[0].shape[2]
    for b in range(nb):
        total = x_ref[b].astype(F32)
        lhs = jnp.concatenate([o[0, b] for o in o_refs], axis=0)
        half = stages * rows
        w_own = w_ref[pl.ds(pl.multiple_of(core * half, half), half), :]
        w_par = w_ref[pl.ds(pl.multiple_of((1 - core) * half, half), half), :]
        total = total + (dot(lhs[:half], w_own, TN) + dot(lhs[half:], w_par, TN))
        y_ref[b] = total.astype(BF16)


def norm_grad_kernel(ids, x_ref, go_ref, g_ref, wt_ref, kv0_ref, kv1_ref, *refs, stages):
    core = ids[1]
    q_refs = refs[:2 * stages]
    gh_ref, gn_ref = refs[2 * stages:]
    nb, tok, d = x_ref.shape
    rows = q_refs[0].shape[2]
    half = stages * rows
    kv_rows = kv0_ref.shape[1]
    e2 = kv_rows // stages
    e = e2 // 2
    kv_half = kv_rows // 2
    g = g_ref[...].astype(F32)

    @pl.when(pl.program_id(0) == 0)
    def _():
        gn_ref[...] = jnp.zeros_like(gn_ref)

    def pick(ref, b):
        full = ref[b]
        ks = jnp.concatenate([full[i * e2:i * e2 + e] for i in range(stages)], axis=0)
        vs = jnp.concatenate([full[i * e2 + e:(i + 1) * e2] for i in range(stages)], axis=0)
        return ks, vs

    for b in range(nb):
        total = jnp.zeros((tok, d), F32)
        for side in range(2):
            who = core if side == 0 else 1 - core
            qs = jnp.concatenate([q[0, b] for q in q_refs[side * stages:(side + 1) * stages]], axis=0)
            ks, vs = pick(kv0_ref if side == 0 else kv1_ref, b)
            total = total + dot(qs, wt_ref[pl.ds(pl.multiple_of(who * half, half), half), :], TN)
            base = 2 * half
            total = total + dot(ks, wt_ref[pl.ds(pl.multiple_of(base + who * kv_half, kv_half), kv_half), :], TN)
            base = base + 2 * kv_half
            total = total + dot(vs, wt_ref[pl.ds(pl.multiple_of(base + who * kv_half, kv_half), kv_half), :], TN)
        x = x_ref[b].astype(F32)
        inv = lax.rsqrt(jnp.mean(x * x, axis=-1, keepdims=True) + NORM_EPS)
        unit = x * inv
        gu = total * g
        mean_dot = jnp.mean(gu * unit, axis=-1, keepdims=True)
        gh_ref[b] = (go_ref[b].astype(F32) + inv * (gu - unit * mean_dot)).astype(BF16)
        gn_ref[...] += jnp.sum((total * unit).reshape(tok // 8, 8, d), axis=0)


def assemble_kernel(in_ref, out_ref):
    chips, n, d = in_ref.shape[0], in_ref.shape[-2], in_ref.shape[-1]
    blk = in_ref[...].reshape(chips * n, d)
    for c in range(0, d, 512):
        out_ref[c:c + 512, :] = blk[:, c:c + 512].astype(F32).T


def solution(mesh):
    chips = mesh.shape['sp'] // CORES
    mesh2 = Mesh(mesh.devices.reshape(mesh.shape['dp'], chips, CORES), ('dp', 'x', 'core'))
    swap = [(i, CORES - 1 - i) for i in range(CORES)]

    def device_step(hidden, norm_w, w_qkv, w_out, long_factor, grad_out):
        n_batch, tok, d = hidden.shape
        n_heads, e = w_out.shape[0], w_out.shape[1]
        kv_heads = (w_qkv.shape[1] // e - n_heads) // 2
        reps = n_heads // kv_heads
        stages = kv_heads // CORES
        rows = reps * e
        q_half = stages * rows
        kv_half = stages * e
        e2 = 2 * e
        half_rot = long_factor.shape[0]
        chip = lax.axis_index('x')
        core = lax.axis_index('core')
        ids = jnp.stack([chip, core]).astype(jnp.int32)
        tiles = 2
        nb = n_batch // tiles

        x_par = lax.ppermute(hidden, 'core', swap)
        go_par = lax.ppermute(grad_out, 'core', swap)
        wt = w_qkv.T
        w_o = w_out.reshape(n_heads * e, d)
        norm2 = norm_w.reshape(1, d)

        exponent = jnp.arange(half_rot, dtype=F32) / half_rot
        inv_freq = 1.0 / (long_factor * jnp.power(ROPE_BASE, exponent))
        sides = jnp.stack([core, 1 - core])
        positions = ((chip * CORES + sides)[:, None] * tok + jnp.arange(tok)[None, :]).astype(F32)
        angles = inv_freq[None, :, None] * positions[:, None, :]
        cos_t, sin_t = jnp.cos(angles) * ROPE_GAIN, jnp.sin(angles) * ROPE_GAIN

        tok_spec = pl.BlockSpec((nb, tok, d), lambda i, _: (i, 0, 0))
        rot_spec = pl.BlockSpec((half_rot, tok), lambda i, _: (0, 0))

        def kv_proj(x, side):
            kb = 2 * q_half // kv_half
            return pl.pallas_call(
                drop_scalar(kv_proj_kernel),
                out_shape=(jax.ShapeDtypeStruct((n_batch, tok, d), BF16), jax.ShapeDtypeStruct((stages, n_batch, e2, tok), BF16)),
                grid_spec=pltpu.PrefetchScalarGridSpec(
                    num_scalar_prefetch=1, grid=(tiles,),
                    in_specs=[tok_spec, pl.BlockSpec((1, d), lambda i, _: (0, 0)),
                              pl.BlockSpec((kv_half, d), lambda i, c: (kb + c[1], 0)),
                              pl.BlockSpec((kv_half, d), lambda i, c: (kb + CORES + c[1], 0)), rot_spec, rot_spec],
                    out_specs=(tok_spec, pl.BlockSpec((stages, nb, e2, tok), lambda i, _: (0, i, 0, 0)))),
                compiler_params=params(), name='kv_proj',
                cost_estimate=cost(2 * n_batch * tok * d * 2 * kv_half, 3 * n_batch * tok * d * 2),
            )(ids, x, norm2, wt, wt, cos_t[side], sin_t[side])

        def q_proj(h, side):
            return pl.pallas_call(
                drop_scalar(q_proj_kernel),
                out_shape=jax.ShapeDtypeStruct((n_batch, q_half, tok), BF16),
                grid_spec=pltpu.PrefetchScalarGridSpec(
                    num_scalar_prefetch=1, grid=(tiles,),
                    in_specs=[tok_spec, pl.BlockSpec((q_half, d), lambda i, c: (c[1], 0)), rot_spec, rot_spec],
                    out_specs=pl.BlockSpec((nb, q_half, tok), lambda i, _: (i, 0, 0))),
                compiler_params=params(), name='q_proj',
                cost_estimate=cost(2 * n_batch * tok * d * q_half, 3 * n_batch * tok * d * 2),
            )(ids, h, wt, cos_t[side], sin_t[side])

        def do_proj(g):
            return pl.pallas_call(
                drop_scalar(do_proj_kernel),
                out_shape=jax.ShapeDtypeStruct((n_batch, q_half, tok), BF16),
                grid_spec=pltpu.PrefetchScalarGridSpec(
                    num_scalar_prefetch=1, grid=(tiles,),
                    in_specs=[tok_spec, pl.BlockSpec((q_half, d), lambda i, c: (c[1], 0))],
                    out_specs=pl.BlockSpec((nb, q_half, tok), lambda i, _: (i, 0, 0))),
                compiler_params=params(), name='do_proj',
                cost_estimate=cost(2 * n_batch * tok * d * q_half, 3 * n_batch * tok * d * 2),
            )(ids, g, w_o)

        h_own, kv_own = kv_proj(hidden, 0)
        h_par, kv_par = kv_proj(x_par, 1)
        gathered = [lax.all_gather(jnp.stack([kv_own[s], kv_par[s]]), 'x') for s in range(stages)]
        q_own, q_par = q_proj(h_own, 0), q_proj(h_par, 1)
        do_own, do_par = do_proj(grad_out), do_proj(go_par)

        def attention(s):
            blk = 2 * tok
            q_spec = pl.BlockSpec((1, rows, tok), lambda b, _: (b, s, 0))
            t_spec = pl.BlockSpec((1, tok, d), lambda b, _: (b, 0, 0))
            r_spec = pl.BlockSpec((2, half_rot, tok), lambda b, _: (0, 0, 0))
            o_spec = pl.BlockSpec((2, 1, rows, tok), lambda b, _: (0, b, 0, 0))
            return pl.pallas_call(
                attn_kernel,
                out_shape=(jax.ShapeDtypeStruct((2, n_batch, rows, tok), BF16), jax.ShapeDtypeStruct((2, n_batch, rows, tok), BF16),
                           jax.ShapeDtypeStruct((chips, e2 + 2 * rows // chips, d), BF16)),
                grid_spec=pltpu.PrefetchScalarGridSpec(
                    num_scalar_prefetch=1, grid=(n_batch,),
                    in_specs=[q_spec, q_spec, q_spec, q_spec,
                              pl.BlockSpec((chips, 2, 1, e2, tok), lambda b, _: (0, 0, b, 0, 0)),
                              t_spec, t_spec, t_spec, t_spec, r_spec, r_spec],
                    out_specs=(o_spec, o_spec, pl.BlockSpec((chips, e2 + 2 * rows // chips, d), lambda b, _: (0, 0, 0))),
                    scratch_shapes=[pltpu.VMEM((chips, blk, reps * blk), F32), pltpu.VMEM((e, reps * blk), F32),
                                    pltpu.VMEM((chips, blk, e2), BF16), pltpu.VMEM((2 * rows, d), F32)]),
                compiler_params=params(), name=f'attn_{s}',
                cost_estimate=cost(4e10, 3e7, 3e7),
            )(ids, q_own, q_par, do_own, do_par, gathered[s], h_own, h_par, grad_out, go_par, cos_t, sin_t)

        own, par, recv = [], [], []
        for s in range(stages):
            own_s, par_s, send_s = attention(s)
            own.append(own_s)
            par.append(lax.ppermute(par_s, 'core', swap))
            recv.append(lax.all_to_all(send_s, 'x', 0, 0, tiled=True))

        n_w = 2 * rows // chips
        shards = [jnp.sum(r[:, e2:].astype(F32), axis=0).astype(BF16) for r in recv]

        blk = 2 * tok
        kv_own_g, kv_par_g, send_kv = pl.pallas_call(
            functools.partial(kv_grad_kernel, stages=stages),
            out_shape=(jax.ShapeDtypeStruct((n_batch, stages * e2, tok), BF16), jax.ShapeDtypeStruct((n_batch, stages * e2, tok), BF16),
                       jax.ShapeDtypeStruct((chips, stages * e2 // chips, d), BF16)),
            grid=(n_batch,),
            in_specs=[pl.BlockSpec((chips, e2, blk), lambda b: (0, 0, b))] * stages
            + [pl.BlockSpec((1, tok, d), lambda b: (b, 0, 0))] * 2 + [pl.BlockSpec((2, half_rot, tok), lambda b: (0, 0, 0))] * 2,
            out_specs=(pl.BlockSpec((1, stages * e2, tok), lambda b: (b, 0, 0)), pl.BlockSpec((1, stages * e2, tok), lambda b: (b, 0, 0)),
                       pl.BlockSpec((chips, stages * e2 // chips, d), lambda b: (0, 0, 0))),
            scratch_shapes=[pltpu.VMEM((stages * e2, d), F32)],
            compiler_params=params(), name='kv_grad',
            cost_estimate=cost(2 * 2 * n_batch * tok * d * stages * e2, 3e7),
        )(*recv, h_own, h_par, cos_t, sin_t)
        kv_other_g = lax.ppermute(kv_par_g, 'core', swap)
        recv_kv = lax.all_to_all(send_kv, 'x', 0, 0, tiled=True)
        shard_kv = jnp.sum(recv_kv.astype(F32), axis=0).astype(BF16)

        nb2 = 2
        t2_spec = pl.BlockSpec((nb2, tok, d), lambda b, _: (b, 0, 0))
        block_out = pl.pallas_call(
            functools.partial(out_kernel, stages=stages),
            out_shape=jax.ShapeDtypeStruct((n_batch, tok, d), BF16),
            grid_spec=pltpu.PrefetchScalarGridSpec(
                num_scalar_prefetch=1, grid=(n_batch // nb2,),
                in_specs=[t2_spec, pl.BlockSpec((n_heads * e, d), lambda b, _: (0, 0))]
                + [pl.BlockSpec((1, nb2, rows, tok), lambda b, _: (0, b, 0, 0))] * (2 * stages),
                out_specs=t2_spec),
            compiler_params=params(), name='out_proj',
            cost_estimate=cost(2 * n_batch * tok * d * n_heads * e, 3e7),
        )(ids, hidden, w_o, *own, *par)

        grad_hidden, gn = pl.pallas_call(
            functools.partial(norm_grad_kernel, stages=stages),
            out_shape=(jax.ShapeDtypeStruct((n_batch, tok, d), BF16), jax.ShapeDtypeStruct((8, d), F32)),
            grid_spec=pltpu.PrefetchScalarGridSpec(
                num_scalar_prefetch=1, grid=(n_batch // nb2,),
                in_specs=[t2_spec, t2_spec, pl.BlockSpec((1, d), lambda b, _: (0, 0)),
                          pl.BlockSpec(wt.shape, lambda b, _: (0, 0))]
                + [pl.BlockSpec((nb2, stages * e2, tok), lambda b, _: (b, 0, 0))] * 2
                + [pl.BlockSpec((1, nb2, rows, tok), lambda b, _: (1, b, 0, 0))] * (2 * stages),
                out_specs=(t2_spec, pl.BlockSpec((8, d), lambda b, _: (0, 0)))),
            compiler_params=params(), name='norm_grad',
            cost_estimate=cost(2 * n_batch * tok * d * wt.shape[0], 4e7),
        )(ids, hidden, grad_out, norm2, wt, kv_own_g, kv_other_g, *own, *par)

        gn_row = jnp.sum(gn, axis=0, keepdims=True)
        gn_hi = gn_row.astype(BF16)
        gn_lo = (gn_row - gn_hi.astype(F32)).astype(BF16)
        pad = jnp.zeros((14, d), BF16)
        tail = lax.all_gather(jnp.concatenate([shard_kv, gn_hi, gn_lo, pad], axis=0), ('x', 'core'))
        main = [lax.all_gather(s, ('x', 'core')) for s in shards]
        main = [m.reshape(chips, CORES, n_w, d) for m in main]
        tail = tail.reshape(chips, CORES, -1, d)
        n_kv = shard_kv.shape[0]

        n_q = rows // chips
        q_part = jnp.stack([m[:, :, :n_q] for m in main])
        o_part = jnp.stack([m[:, :, n_q:] for m in main])
        grad_w_out = jnp.transpose(o_part, (2, 0, 1, 3, 4)).reshape(n_heads, e, d).astype(F32)
        q_cols = jnp.transpose(q_part, (2, 0, 1, 3, 4)).reshape(n_heads * e, d)
        k_cols = jnp.transpose(tail[:, :, :e], (1, 0, 2, 3)).reshape(kv_heads * e, d)
        v_cols = jnp.transpose(tail[:, :, e:2 * e], (1, 0, 2, 3)).reshape(kv_heads * e, d)
        grad_w_qkv = jnp.concatenate([q_cols, k_cols, v_cols], axis=0).astype(F32).T
        gn_all = tail[:, :, n_kv:n_kv + 2].astype(F32)
        grad_norm_w = jnp.sum(gn_all, axis=(0, 1, 2))
        return block_out, grad_hidden, grad_w_qkv, grad_w_out, grad_norm_w

    tok_spec = P('dp', ('x', 'core'), None)
    return jax.shard_map(device_step, mesh=mesh2,
                         in_specs=(tok_spec, P(), P(), P(), P(), tok_spec),
                         out_specs=(tok_spec, tok_spec, P('dp', None), P('dp', None, None), P('dp')),
                         check_vma=False)
```

```python
import functools
import math

import jax
import jax.numpy as jnp
from jax import lax
from jax.experimental import pallas as pl
from jax.experimental.pallas import tpu as pltpu
from jax.sharding import Mesh, PartitionSpec as P


NORM_EPS = 1e-5
ROPE_BASE = 10000.0
ROPE_GAIN = math.sqrt(1.0 + math.log(32.0) / math.log(4096.0))
MASK_VALUE = -1e30
LOG2E = math.log2(math.e)
CORES = 2
BF16 = jnp.bfloat16
F32 = jnp.float32
VMEM_LIMIT = 60 * 1024 * 1024

NN = (((1,), (0,)), ((), ()))
NT = (((1,), (1,)), ((), ()))


def dot(a, b, dims=NN):
    return lax.dot_general(a, b, dims, preferred_element_type=F32)


def cost(flops, nbytes, trans=0):
    return pl.CostEstimate(flops=int(flops), bytes_accessed=int(nbytes), transcendentals=int(trans))


def params(n_axes=1):
    return pltpu.CompilerParams(dimension_semantics=("arbitrary",) * n_axes, vmem_limit_bytes=VMEM_LIMIT)


def rope_rows(block, cos, sin, direction):
    half = cos.shape[0]
    a, b = block[:half], block[half:2 * half]
    s = sin * direction
    return jnp.concatenate([a * cos - b * s, b * cos + a * s], axis=0)


def kv_proj_kernel(x_ref, g_ref, wk_ref, wv_ref, cos_ref, sin_ref, h_ref, kv_ref):
    nb, tok, d = x_ref.shape
    kvh, _, e2, _ = kv_ref.shape
    e = e2 // 2
    x = x_ref[...].reshape(nb * tok, d).astype(F32)
    inv = lax.rsqrt(jnp.mean(x * x, axis=-1, keepdims=True) + NORM_EPS)
    h = (x * inv * g_ref[...].astype(F32)).astype(BF16)
    h_ref[...] = h.reshape(nb, tok, d)
    cos, sin = cos_ref[...], sin_ref[...]
    k = dot(h, wk_ref[...]).T
    for i in range(kvh):
        for b in range(nb):
            kv_ref[i, b, 0:e] = rope_rows(k[i * e:(i + 1) * e, b * tok:(b + 1) * tok], cos, sin, 1.0).astype(BF16)
    v = dot(h, wv_ref[...]).T
    for i in range(kvh):
        for b in range(nb):
            kv_ref[i, b, e:2 * e] = v[i * e:(i + 1) * e, b * tok:(b + 1) * tok].astype(BF16)


def q_proj_kernel(h0_ref, h1_ref, w_ref, cos_ref, sin_ref, q0_ref, q1_ref):
    nb, tok, d = h0_ref.shape
    e = 2 * cos_ref.shape[1]
    rows = w_ref.shape[1]
    scale = e ** -0.5
    step = 4 * e

    def run(h_ref, q_ref, side):
        h = h_ref[...].reshape(nb * tok, d)
        cos, sin = cos_ref[side], sin_ref[side]
        for r in range(0, rows, step):
            blk = dot(h, w_ref[:, r:r + step]).T
            for i in range(0, step, e):
                for b in range(nb):
                    q_ref[b, r + i:r + i + e] = (rope_rows(blk[i:i + e, b * tok:(b + 1) * tok], cos, sin, 1.0).astype(BF16)
                                                 * scale).astype(BF16)

    half = pl.num_programs(0) // 2
    pl.when(pl.program_id(0) < half)(lambda: run(h0_ref, q0_ref, 0))
    pl.when(pl.program_id(0) >= half)(lambda: run(h1_ref, q1_ref, 1))


def do_proj_kernel(g0_ref, g1_ref, w_ref, o0_ref, o1_ref):
    nb, tok, d = g0_ref.shape
    rows = w_ref.shape[0]
    step = 256

    def run(g_ref, o_ref):
        g = g_ref[...].reshape(nb * tok, d)
        for r in range(0, rows, step):
            blk = dot(w_ref[r:r + step], g, NT)
            for b in range(nb):
                o_ref[b, r:r + step] = blk[:, b * tok:(b + 1) * tok].astype(BF16)

    half = pl.num_programs(0) // 2
    pl.when(pl.program_id(0) < half)(lambda: run(g0_ref, o0_ref))
    pl.when(pl.program_id(0) >= half)(lambda: run(g1_ref, o1_ref))


def drop_scalar(kernel):
    def wrapped(_, *refs):
        kernel(*refs)

    return wrapped


def attn_kernel(ids, q0_ref, q1_ref, do0_ref, do1_ref, kv_ref, h0_ref, h1_ref, g0_ref, g1_ref, cos_ref, sin_ref,
                own_ref, par_ref, send_ref, s_ref, acc_ref, kvt_ref, lhs_ref, gacc_ref):
    chip, core = ids[0], ids[1]
    b_id = pl.program_id(0)
    chips = kv_ref.shape[0]
    rows, tok = q0_ref.shape[1], q0_ref.shape[2]
    e = kv_ref.shape[3] // 2
    reps = rows // e
    blk = 2 * tok

    def heads_to_lanes(first_ref, second_ref):
        full = jnp.concatenate([first_ref[0], second_ref[0]], axis=1)
        return jnp.concatenate([full[i * e:(i + 1) * e] for i in range(reps)], axis=1)

    qt = heads_to_lanes(q0_ref, q1_ref)
    dot_t = heads_to_lanes(do0_ref, do1_ref)
    zero = jnp.zeros_like(qt)
    q_pad = jnp.concatenate([qt, zero], axis=0)
    do_pad = jnp.concatenate([zero, dot_t], axis=0)
    head_cols = [slice(i * blk, (i + 1) * blk) for i in range(reps)]

    def kv_block(j):
        return jnp.concatenate([kv_ref[j, 0, 0], kv_ref[j, 1, 0]], axis=1)

    def scores(j, masked):
        kvt = kv_block(j).T
        kvt_ref[j] = kvt
        tops = []
        for cols in head_cols:
            t = dot(kvt, q_pad[:, cols])
            if masked:
                r = lax.broadcasted_iota(jnp.int32, (blk, blk), 0)
                c = lax.broadcasted_iota(jnp.int32, (blk, blk), 1)
                shift = (1 - 2 * core) * tok
                k_pos = jnp.where(r < tok, r, r - tok + shift)
                q_pos = jnp.where(c < tok, c, c - tok + shift)
                t = jnp.where(k_pos <= q_pos, t, MASK_VALUE)
            s_ref[j, :, cols] = t
            tops.append(jnp.max(t, axis=0, keepdims=True))
        return jnp.concatenate(tops, axis=1) * LOG2E

    def accumulate(j, m):
        v_t = kv_block(j)[e:2 * e]
        sums, outs = [], []
        for cols in head_cols:
            p = jnp.exp2(s_ref[j, :, cols] * LOG2E - m[:, cols])
            sums.append(jnp.sum(p, axis=0, keepdims=True))
            outs.append(dot(v_t, p.astype(BF16)))
        return jnp.concatenate(sums, axis=1), jnp.concatenate(outs, axis=1)

    acc_ref[...] = jnp.zeros_like(acc_ref)
    m = scores(chip, True)

    def forward_step(j, carry):
        m, l = carry
        prev = jnp.where(j == 0, chip, j - 1)
        add_l, add_o = accumulate(prev, m)
        m_new = jnp.maximum(m, scores(j, False))
        alpha = jnp.exp2(m - m_new)
        acc_ref[...] = (acc_ref[...] + add_o) * alpha
        return m_new, (l + add_l) * alpha

    m, l = lax.fori_loop(0, chip, forward_step, (m, jnp.zeros_like(m)))
    add_l, add_o = accumulate(jnp.where(chip == 0, chip, chip - 1), m)
    l = l + add_l

    o_t = (acc_ref[...] + add_o) * (1.0 / l)
    delta = jnp.sum(o_t * dot_t.astype(F32), axis=0, keepdims=True)
    lse = m + jnp.log2(l)
    o_b = o_t.astype(BF16)

    def backward_block(j, first):
        kvt = kvt_ref[j]
        k_t = kv_block(j)[0:e]
        dk = jnp.zeros((e, blk), F32)
        dv = jnp.zeros((e, blk), F32)
        for cols in head_cols:
            p = jnp.exp2(s_ref[j, :, cols] * LOG2E - lse[:, cols])
            dp = dot(kvt, do_pad[:, cols])
            ds = (p * (dp - delta[:, cols])).astype(BF16)
            dv = dv + dot(dot_t[:, cols], p.astype(BF16), NT)
            dk = dk + dot(qt[:, cols], ds, NT)
            dq = dot(k_t, ds)
            if first:
                acc_ref[:, cols] = dq
            else:
                acc_ref[:, cols] = acc_ref[:, cols] + dq
        send_ref[j, 0:2 * e, pl.ds(pl.multiple_of(b_id * blk, blk), blk)] = jnp.concatenate([dk, dv], axis=0).astype(BF16)

    backward_block(chip, True)

    def backward_step(j, carry):
        backward_block(j, False)
        return carry

    lax.fori_loop(0, chip, backward_step, 0)

    def zero_step(j, carry):
        send_ref[j, 0:2 * e, pl.ds(pl.multiple_of(b_id * blk, blk), blk)] = jnp.zeros((2 * e, blk), BF16)
        return carry

    lax.fori_loop(chip + 1, chips, zero_step, 0)

    cos = jnp.concatenate([cos_ref[0], cos_ref[1]], axis=1)
    sin = jnp.concatenate([sin_ref[0], sin_ref[1]], axis=1)
    dq_rows = []
    for cols in head_cols:
        dq = (acc_ref[:, cols] * (e ** -0.5)).astype(BF16).astype(F32)
        dq_rows.append(rope_rows(dq, cos, sin, -1.0).astype(BF16))
    o_full = jnp.concatenate([o_b[:, cols] for cols in head_cols], axis=0)
    dq_full = jnp.concatenate(dq_rows, axis=0)
    own_ref[0, 0] = o_full[:, :tok]
    par_ref[0, 0] = o_full[:, tok:]
    own_ref[1, 0] = dq_full[:, :tok]
    par_ref[1, 0] = dq_full[:, tok:]

    d = h0_ref.shape[2]
    step = 512
    odd = lax.rem(b_id, 2)
    lhs_ref[odd, 0:rows] = dq_full
    lhs_ref[odd, rows:2 * rows] = o_full

    def weight_grads(first):
        for c in range(0, d, step):
            cs = slice(c, c + step)
            for r, (a_ref, b_ref) in enumerate(((h0_ref, h1_ref), (g0_ref, g1_ref))):
                rs = slice(r * rows, (r + 1) * rows)
                lhs = jnp.concatenate([lhs_ref[0, rs], lhs_ref[1, rs]], axis=1)
                rhs = jnp.concatenate([a_ref[0, :, cs], b_ref[0, :, cs], a_ref[1, :, cs], b_ref[1, :, cs]], axis=0)
                if first:
                    gacc_ref[rs, cs] = dot(lhs, rhs)
                else:
                    gacc_ref[rs, cs] += dot(lhs, rhs)

    pl.when(b_id == 1)(lambda: weight_grads(True))
    pl.when((odd == 1) & (b_id > 1))(lambda: weight_grads(False))

    @pl.when(b_id == pl.num_programs(0) - 1)
    def _():
        for j in range(chips):
            n = rows // chips
            send_ref[j, 2 * e:2 * e + n] = gacc_ref[j * n:(j + 1) * n].astype(BF16)
            send_ref[j, 2 * e + n:2 * e + 2 * n] = gacc_ref[rows + j * n:rows + (j + 1) * n].astype(BF16)


def kv_grad_kernel(*refs, stages):
    recv = refs[:stages]
    h0_ref, h1_ref, cos_ref, sin_ref, own_ref, par_ref, send_ref, gacc_ref = refs[stages:]
    b_id = pl.program_id(0)
    tok = h0_ref.shape[1]
    e2 = own_ref.shape[1] // stages
    e = e2 // 2
    cos = jnp.concatenate([cos_ref[0], cos_ref[1]], axis=1)
    sin = jnp.concatenate([sin_ref[0], sin_ref[1]], axis=1)
    parts = []
    for r in recv:
        total = r[0].astype(F32)
        for j in range(1, r.shape[0]):
            total = total + r[j].astype(F32)
        total = total.astype(BF16).astype(F32)
        parts.append(jnp.concatenate([rope_rows(total[0:e], cos, sin, -1.0), total[e:2 * e]], axis=0).astype(BF16))
    gf = jnp.concatenate(parts, axis=0)
    own_ref[0] = gf[:, :tok]
    par_ref[0] = gf[:, tok:]

    @pl.when(b_id == 0)
    def _():
        gacc_ref[...] = jnp.zeros_like(gacc_ref)

    d = h0_ref.shape[2]
    step = 512
    for c in range(0, d, step):
        cs = slice(c, c + step)
        hh = jnp.concatenate([h0_ref[0, :, cs], h1_ref[0, :, cs]], axis=0)
        gacc_ref[:, cs] += dot(gf, hh)

    @pl.when(b_id == pl.num_programs(0) - 1)
    def _():
        n = send_ref.shape[1]
        for j in range(send_ref.shape[0]):
            send_ref[j] = gacc_ref[j * n:(j + 1) * n].astype(BF16)


def out_kernel(ids, x_ref, w_ref, *refs, stages):
    core = ids[1]
    o_refs, (y_ref, lhs_ref) = refs[:-2], refs[-2:]
    nb, tok, d = x_ref.shape
    rows = o_refs[0].shape[2]
    half = stages * rows
    for side in range(2):
        base = (core if side == 0 else 1 - core) * half
        for s in range(stages):
            for b in range(nb):
                lhs_ref[b * tok:(b + 1) * tok, pl.ds(pl.multiple_of(base + s * rows, rows), rows)] = o_refs[side * stages + s][0, b].T
    lhs = lhs_ref[...]
    step = 512
    for c in range(0, d, step):
        prod = dot(lhs, w_ref[:, c:c + step])
        y_ref[:, :, c:c + step] = (x_ref[:, :, c:c + step].astype(F32) + prod.reshape(nb, tok, step)).astype(BF16)


def norm_grad_kernel(ids, x_ref, go_ref, g_ref, w_ref, kv0_ref, kv1_ref, *refs, stages):
    core = ids[1]
    q_refs = refs[:2 * stages]
    gh_ref, gn_ref, lhs_ref, tot_ref = refs[2 * stages:]
    nb, tok, d = x_ref.shape
    rows = q_refs[0].shape[2]
    half = stages * rows
    e2 = kv0_ref.shape[1] // stages
    e = e2 // 2
    kv_half = stages * e
    for side in range(2):
        who = core if side == 0 else 1 - core
        kv_ref = kv0_ref if side == 0 else kv1_ref
        for b in range(nb):
            ts = slice(b * tok, (b + 1) * tok)
            for s in range(stages):
                lhs_ref[ts, pl.ds(pl.multiple_of(who * half + s * rows, rows), rows)] = q_refs[side * stages + s][0, b].T
            ks = jnp.concatenate([kv_ref[b, i * e2:i * e2 + e] for i in range(stages)], axis=0)
            vs = jnp.concatenate([kv_ref[b, i * e2 + e:(i + 1) * e2] for i in range(stages)], axis=0)
            base = 2 * half
            lhs_ref[ts, pl.ds(pl.multiple_of(base + who * kv_half, kv_half), kv_half)] = ks.T
            base = base + 2 * kv_half
            lhs_ref[ts, pl.ds(pl.multiple_of(base + who * kv_half, kv_half), kv_half)] = vs.T
    lhs = lhs_ref[...]
    step = 256
    for c in range(0, d, step):
        tot_ref[:, c:c + step] = dot(lhs, w_ref[c:c + step, :], NT)

    @pl.when(pl.program_id(0) == 0)
    def _():
        gn_ref[...] = jnp.zeros_like(gn_ref)

    g = g_ref[...].astype(F32)
    for b in range(nb):
        total = tot_ref[b * tok:(b + 1) * tok]
        x = x_ref[b].astype(F32)
        inv = lax.rsqrt(jnp.mean(x * x, axis=-1, keepdims=True) + NORM_EPS)
        unit = x * inv
        gu = total * g
        mean_dot = jnp.mean(gu * unit, axis=-1, keepdims=True)
        gh_ref[b] = (go_ref[b].astype(F32) + inv * (gu - unit * mean_dot)).astype(BF16)
        gn_ref[...] += jnp.sum((total * unit).reshape(tok // 8, 8, d), axis=0)


def transpose_to(out_ref, blk):
    for c in range(0, blk.shape[1], 256):
        out_ref[c:c + 256, :] = blk[:, c:c + 256].astype(F32).T


def assemble_main_kernel(*refs, stages, n_q):
    ins, (wq_ref, wo_ref) = refs[:stages], refs[stages:]
    for s in range(stages):
        @pl.when(pl.program_id(1) == s)
        def _(ref=ins[s]):
            chips, _, n, d = ref.shape
            transpose_to(wq_ref, ref[:, 0, 0:n_q].reshape(chips * n_q, d))
            wo_ref[...] = ref[:, 0, n_q:n].astype(F32)


def assemble_tail_kernel(in_ref, _, out_ref):
    chips, _, n, d = in_ref.shape
    transpose_to(out_ref, in_ref[:, 0].reshape(chips * n, d))


def solution(mesh):
    chips = mesh.shape['sp'] // CORES
    mesh2 = Mesh(mesh.devices.reshape(mesh.shape['dp'], chips, CORES), ('dp', 'x', 'core'))
    swap = [(i, CORES - 1 - i) for i in range(CORES)]

    def device_step(hidden, norm_w, w_qkv, w_out, long_factor, grad_out):
        n_batch, tok, d = hidden.shape
        n_heads, e = w_out.shape[0], w_out.shape[1]
        kv_heads = (w_qkv.shape[1] // e - n_heads) // 2
        reps = n_heads // kv_heads
        stages = kv_heads // CORES
        rows = reps * e
        q_half = stages * rows
        kv_half = stages * e
        e2 = 2 * e
        half_rot = long_factor.shape[0]
        chip = lax.axis_index('x')
        core = lax.axis_index('core')
        ids = jnp.stack([chip, core]).astype(jnp.int32)
        tiles = 2
        nb = n_batch // tiles

        x_par = lax.ppermute(hidden, 'core', swap)
        go_par = lax.ppermute(grad_out, 'core', swap)
        w_o = w_out.reshape(n_heads * e, d)
        norm2 = norm_w.reshape(1, d)

        exponent = jnp.arange(half_rot, dtype=F32) / half_rot
        inv_freq = 1.0 / (long_factor * jnp.power(ROPE_BASE, exponent))
        sides = jnp.stack([core, 1 - core])
        positions = ((chip * CORES + sides)[:, None] * tok + jnp.arange(tok)[None, :]).astype(F32)
        angles = inv_freq[None, :, None] * positions[:, None, :]
        cos_t, sin_t = jnp.cos(angles) * ROPE_GAIN, jnp.sin(angles) * ROPE_GAIN

        tok_spec = pl.BlockSpec((nb, tok, d), lambda i, _: (i, 0, 0))
        rot_spec = pl.BlockSpec((half_rot, tok), lambda i, _: (0, 0))

        def kv_proj(x, side):
            kb = 2 * q_half // kv_half
            return pl.pallas_call(
                drop_scalar(kv_proj_kernel),
                out_shape=(jax.ShapeDtypeStruct((n_batch, tok, d), BF16), jax.ShapeDtypeStruct((stages, n_batch, e2, tok), BF16)),
                grid_spec=pltpu.PrefetchScalarGridSpec(
                    num_scalar_prefetch=1, grid=(tiles,),
                    in_specs=[tok_spec, pl.BlockSpec((1, d), lambda i, _: (0, 0)),
                              pl.BlockSpec((d, kv_half), lambda i, c: (0, kb + c[1])),
                              pl.BlockSpec((d, kv_half), lambda i, c: (0, kb + CORES + c[1])), rot_spec, rot_spec],
                    out_specs=(tok_spec, pl.BlockSpec((stages, nb, e2, tok), lambda i, _: (0, i, 0, 0)))),
                compiler_params=params(), name='kv_proj',
                cost_estimate=cost(2 * n_batch * tok * d * 2 * kv_half, 3 * n_batch * tok * d * 2),
            )(ids, x, norm2, w_qkv, w_qkv, cos_t[side], sin_t[side])

        first = lambda i: jnp.minimum(i, tiles - 1)
        second = lambda i: jnp.maximum(i - tiles, 0)
        own_spec = pl.BlockSpec((nb, tok, d), lambda i, _: (first(i), 0, 0))
        par_spec = pl.BlockSpec((nb, tok, d), lambda i, _: (second(i), 0, 0))
        own_out = pl.BlockSpec((nb, q_half, tok), lambda i, _: (first(i), 0, 0))
        par_out = pl.BlockSpec((nb, q_half, tok), lambda i, _: (second(i), 0, 0))
        both_rot = pl.BlockSpec((2, half_rot, tok), lambda i, _: (0, 0, 0))
        q_shapes = (jax.ShapeDtypeStruct((n_batch, q_half, tok), BF16), jax.ShapeDtypeStruct((n_batch, q_half, tok), BF16))

        def q_proj(h0, h1):
            return pl.pallas_call(
                drop_scalar(q_proj_kernel), out_shape=q_shapes,
                grid_spec=pltpu.PrefetchScalarGridSpec(
                    num_scalar_prefetch=1, grid=(2 * tiles,),
                    in_specs=[own_spec, par_spec, pl.BlockSpec((d, q_half), lambda i, c: (0, c[1])), both_rot, both_rot],
                    out_specs=(own_out, par_out)),
                compiler_params=params(), name='q_proj',
                cost_estimate=cost(4 * n_batch * tok * d * q_half, 6 * n_batch * tok * d * 2),
            )(ids, h0, h1, w_qkv, cos_t, sin_t)

        def do_proj(g0, g1):
            return pl.pallas_call(
                drop_scalar(do_proj_kernel), out_shape=q_shapes,
                grid_spec=pltpu.PrefetchScalarGridSpec(
                    num_scalar_prefetch=1, grid=(2 * tiles,),
                    in_specs=[own_spec, par_spec, pl.BlockSpec((q_half, d), lambda i, c: (c[1], 0))],
                    out_specs=(own_out, par_out)),
                compiler_params=params(), name='do_proj',
                cost_estimate=cost(4 * n_batch * tok * d * q_half, 6 * n_batch * tok * d * 2),
            )(ids, g0, g1, w_o)

        h_own, kv_own = kv_proj(hidden, 0)
        h_par, kv_par = kv_proj(x_par, 1)
        gathered = []
        for s in range(stages):
            gathered.append(lax.all_gather(jnp.stack([kv_own[s], kv_par[s]]), 'x'))
        q_own, q_par = q_proj(h_own, h_par)
        do_own, do_par = do_proj(grad_out, go_par)

        def attention(s):
            blk = 2 * tok
            q_spec = pl.BlockSpec((1, rows, tok), lambda b, _: (b, s, 0))
            t_spec = pl.BlockSpec((2, tok, d), lambda b, _: (b // 2, 0, 0))
            r_spec = pl.BlockSpec((2, half_rot, tok), lambda b, _: (0, 0, 0))
            o_spec = pl.BlockSpec((2, 1, rows, tok), lambda b, _: (0, b, 0, 0))
            return pl.pallas_call(
                attn_kernel,
                out_shape=(jax.ShapeDtypeStruct((2, n_batch, rows, tok), BF16), jax.ShapeDtypeStruct((2, n_batch, rows, tok), BF16),
                           jax.ShapeDtypeStruct((chips, e2 + 2 * rows // chips, d), BF16)),
                grid_spec=pltpu.PrefetchScalarGridSpec(
                    num_scalar_prefetch=1, grid=(n_batch,),
                    in_specs=[q_spec, q_spec, q_spec, q_spec,
                              pl.BlockSpec((chips, 2, 1, e2, tok), lambda b, _: (0, 0, b, 0, 0)),
                              t_spec, t_spec, t_spec, t_spec, r_spec, r_spec],
                    out_specs=(o_spec, o_spec, pl.BlockSpec((chips, e2 + 2 * rows // chips, d), lambda b, _: (0, 0, 0))),
                    scratch_shapes=[pltpu.VMEM((chips, blk, reps * blk), F32), pltpu.VMEM((e, reps * blk), F32),
                                    pltpu.VMEM((chips, blk, e2), BF16), pltpu.VMEM((2, 2 * rows, blk), BF16),
                                    pltpu.VMEM((2 * rows, d), F32)]),
                compiler_params=params(),
                cost_estimate=cost(4e10, 3e7, 3e7),
            )(ids, q_own, q_par, do_own, do_par, gathered[s], h_own, h_par, grad_out, go_par, cos_t, sin_t)

        own, par, recv = [], [], []
        for s in range(stages):
            own_s, par_s, send_s = attention(s)
            own.append(own_s)
            par.append(lax.ppermute(par_s, 'core', swap))
            recv.append(lax.all_to_all(send_s, 'x', 0, 0, tiled=True))

        n_w = 2 * rows // chips
        shards = [jnp.sum(r[:, e2:].astype(F32), axis=0).astype(BF16) for r in recv]

        blk = 2 * tok
        kv_own_g, kv_par_g, send_kv = pl.pallas_call(
            functools.partial(kv_grad_kernel, stages=stages),
            out_shape=(jax.ShapeDtypeStruct((n_batch, stages * e2, tok), BF16), jax.ShapeDtypeStruct((n_batch, stages * e2, tok), BF16),
                       jax.ShapeDtypeStruct((chips, stages * e2 // chips, d), BF16)),
            grid=(n_batch,),
            in_specs=[pl.BlockSpec((chips, e2, blk), lambda b: (0, 0, b))] * stages
            + [pl.BlockSpec((1, tok, d), lambda b: (b, 0, 0))] * 2 + [pl.BlockSpec((2, half_rot, tok), lambda b: (0, 0, 0))] * 2,
            out_specs=(pl.BlockSpec((1, stages * e2, tok), lambda b: (b, 0, 0)), pl.BlockSpec((1, stages * e2, tok), lambda b: (b, 0, 0)),
                       pl.BlockSpec((chips, stages * e2 // chips, d), lambda b: (0, 0, 0))),
            scratch_shapes=[pltpu.VMEM((stages * e2, d), F32)],
            compiler_params=params(), name='kv_grad',
            cost_estimate=cost(2 * 2 * n_batch * tok * d * stages * e2, 3e7),
        )(*recv, h_own, h_par, cos_t, sin_t)
        kv_other_g = lax.ppermute(kv_par_g, 'core', swap)
        recv_kv = lax.all_to_all(send_kv, 'x', 0, 0, tiled=True)
        shard_kv = jnp.sum(recv_kv.astype(F32), axis=0).astype(BF16)

        nb2 = nb
        t2_spec = pl.BlockSpec((nb2, tok, d), lambda b, _: (b, 0, 0))
        block_out = pl.pallas_call(
            functools.partial(out_kernel, stages=stages),
            out_shape=jax.ShapeDtypeStruct((n_batch, tok, d), BF16),
            grid_spec=pltpu.PrefetchScalarGridSpec(
                num_scalar_prefetch=1, grid=(n_batch // nb2,),
                in_specs=[t2_spec, pl.BlockSpec((n_heads * e, d), lambda b, _: (0, 0))]
                + [pl.BlockSpec((1, nb2, rows, tok), lambda b, _: (0, b, 0, 0))] * (2 * stages),
                out_specs=t2_spec, scratch_shapes=[pltpu.VMEM((nb2 * tok, n_heads * e), BF16)]),
            compiler_params=params(), name='out_proj',
            cost_estimate=cost(2 * n_batch * tok * d * n_heads * e, 3e7),
        )(ids, hidden, w_o, *own, *par)

        grad_hidden, gn = pl.pallas_call(
            functools.partial(norm_grad_kernel, stages=stages),
            out_shape=(jax.ShapeDtypeStruct((n_batch, tok, d), BF16), jax.ShapeDtypeStruct((8, d), F32)),
            grid_spec=pltpu.PrefetchScalarGridSpec(
                num_scalar_prefetch=1, grid=(n_batch // nb2,),
                in_specs=[t2_spec, t2_spec, pl.BlockSpec((1, d), lambda b, _: (0, 0)),
                          pl.BlockSpec(w_qkv.shape, lambda b, _: (0, 0))]
                + [pl.BlockSpec((nb2, stages * e2, tok), lambda b, _: (b, 0, 0))] * 2
                + [pl.BlockSpec((1, nb2, rows, tok), lambda b, _: (1, b, 0, 0))] * (2 * stages),
                out_specs=(t2_spec, pl.BlockSpec((8, d), lambda b, _: (0, 0))),
                scratch_shapes=[pltpu.VMEM((nb2 * tok, w_qkv.shape[1]), BF16), pltpu.VMEM((nb2 * tok, d), F32)]),
            compiler_params=params(), name='norm_grad',
            cost_estimate=cost(2 * n_batch * tok * d * w_qkv.shape[1], 4e7),
        )(ids, hidden, grad_out, norm2, w_qkv, kv_own_g, kv_other_g, *own, *par)

        gn_row = jnp.sum(gn, axis=0, keepdims=True)
        gn_hi = gn_row.astype(BF16)
        gn_lo = (gn_row - gn_hi.astype(F32)).astype(BF16)
        pad = jnp.zeros((14, d), BF16)
        tail = lax.all_gather(jnp.concatenate([shard_kv, gn_hi, gn_lo, pad], axis=0), ('x', 'core'))
        tail = tail.reshape(chips, CORES, -1, d)
        n_kv = shard_kv.shape[0]
        n_q = rows // chips
        main = [lax.all_gather(s, ('x', 'core')).reshape(chips, CORES, n_w, d) for s in shards]
        w_cols, grad_w_out = pl.pallas_call(
            functools.partial(assemble_main_kernel, stages=stages, n_q=n_q),
            out_shape=(jax.ShapeDtypeStruct(w_qkv.shape, F32), jax.ShapeDtypeStruct((n_heads, e, d), F32)),
            grid=(CORES, stages),
            in_specs=[pl.BlockSpec((chips, 1, n_w, d), lambda p, s: (0, p, 0, 0))] * stages,
            out_specs=(pl.BlockSpec((d, rows), lambda p, s: (0, p * stages + s)),
                       pl.BlockSpec((reps, e, d), lambda p, s: (p * stages + s, 0, 0))),
            compiler_params=params(2), name='assemble_main', cost_estimate=cost(2e9, 6e7),
        )(*main)
        kcol = 2 * q_half // kv_half
        grad_w_qkv = pl.pallas_call(
            assemble_tail_kernel,
            out_shape=jax.ShapeDtypeStruct(w_qkv.shape, F32),
            grid=(CORES, 2),
            in_specs=[pl.BlockSpec((chips, 1, e, d), lambda p, k: (0, p, k, 0)), pl.BlockSpec(memory_space=pl.ANY)],
            out_specs=pl.BlockSpec((d, kv_half), lambda p, k: (0, kcol + k * CORES + p)),
            input_output_aliases={1: 0},
            compiler_params=params(2), name='assemble_tail', cost_estimate=cost(1e9, 2e7),
        )(tail, w_cols)
        gn_all = tail[:, :, n_kv:n_kv + 2].astype(F32)
        grad_norm_w = jnp.sum(gn_all, axis=(0, 1, 2))
        return block_out, grad_hidden, grad_w_qkv, grad_w_out, grad_norm_w

    tok_spec = P('dp', ('x', 'core'), None)
    return jax.shard_map(device_step, mesh=mesh2,
                         in_specs=(tok_spec, P(), P(), P(), P(), tok_spec),
                         out_specs=(tok_spec, tok_spec, P('dp', None), P('dp', None, None), P('dp')),
                         check_vma=False)
```

```python
import functools
import math

import jax
import jax.numpy as jnp
from jax import lax
from jax.experimental import pallas as pl
from jax.experimental.pallas import tpu as pltpu
from jax.sharding import Mesh, PartitionSpec as P


NORM_EPS = 1e-5
ROPE_BASE = 10000.0
ROPE_GAIN = math.sqrt(1.0 + math.log(32.0) / math.log(4096.0))
MASK_VALUE = -1e30
LOG2E = math.log2(math.e)
CORES = 2
BF16 = jnp.bfloat16
F32 = jnp.float32
VMEM_LIMIT = 60 * 1024 * 1024

NN = (((1,), (0,)), ((), ()))
NT = (((1,), (1,)), ((), ()))


def dot(a, b, dims=NN):
    return lax.dot_general(a, b, dims, preferred_element_type=F32)


def cost(flops, nbytes, trans=0):
    return pl.CostEstimate(flops=int(flops), bytes_accessed=int(nbytes), transcendentals=int(trans))


def params(n_axes=1):
    return pltpu.CompilerParams(dimension_semantics=("arbitrary",) * n_axes, vmem_limit_bytes=VMEM_LIMIT)


def rope_rows(block, cos, sin, direction):
    half = cos.shape[0]
    a, b = block[:half], block[half:2 * half]
    s = sin * direction
    return jnp.concatenate([a * cos - b * s, b * cos + a * s], axis=0)


def kv_proj_kernel(x_ref, g_ref, wk_ref, wv_ref, cos_ref, sin_ref, *refs):
    nb, tok, d = x_ref.shape
    stages = (wk_ref.shape[1] // (2 * cos_ref.shape[0]))
    h_ref, kv_refs = refs[-stages - 1], refs[-stages:]
    e2 = kv_refs[0].shape[2]
    e = e2 // 2
    x = x_ref[...].reshape(nb * tok, d).astype(F32)
    inv = lax.rsqrt(jnp.mean(x * x, axis=-1, keepdims=True) + NORM_EPS)
    h = (x * inv * g_ref[...].astype(F32)).astype(BF16)
    h_ref[...] = h.reshape(nb, tok, d)
    cos, sin = cos_ref[...], sin_ref[...]
    k = dot(h, wk_ref[...]).T
    v = dot(h, wv_ref[...]).T
    for i in range(stages):
        for b in range(nb):
            kv_refs[i][0, b, 0:e] = rope_rows(k[i * e:(i + 1) * e, b * tok:(b + 1) * tok], cos, sin, 1.0).astype(BF16)
            kv_refs[i][0, b, e:2 * e] = v[i * e:(i + 1) * e, b * tok:(b + 1) * tok].astype(BF16)


def q_proj_kernel(h0_ref, h1_ref, w_ref, cos_ref, sin_ref, q0_ref, q1_ref):
    nb, tok, d = h0_ref.shape
    e = 2 * cos_ref.shape[1]
    rows = w_ref.shape[1]
    scale = e ** -0.5
    step = 4 * e

    def run(h_ref, q_ref, side):
        h = h_ref[...].reshape(nb * tok, d)
        cos, sin = cos_ref[side], sin_ref[side]
        for r in range(0, rows, step):
            blk = dot(h, w_ref[:, r:r + step]).T
            for i in range(0, step, e):
                for b in range(nb):
                    q_ref[b, r + i:r + i + e] = (rope_rows(blk[i:i + e, b * tok:(b + 1) * tok], cos, sin, 1.0).astype(BF16)
                                                 * scale).astype(BF16)

    half = pl.num_programs(0) // 2
    pl.when(pl.program_id(0) < half)(lambda: run(h0_ref, q0_ref, 0))
    pl.when(pl.program_id(0) >= half)(lambda: run(h1_ref, q1_ref, 1))


def do_proj_kernel(g0_ref, g1_ref, w_ref, o0_ref, o1_ref):
    nb, tok, d = g0_ref.shape
    rows = w_ref.shape[0]
    step = 512

    def run(g_ref, o_ref):
        g = g_ref[...].reshape(nb * tok, d)
        for r in range(0, rows, step):
            blk = dot(w_ref[r:r + step], g, NT)
            for b in range(nb):
                o_ref[b, r:r + step] = blk[:, b * tok:(b + 1) * tok].astype(BF16)

    half = pl.num_programs(0) // 2
    pl.when(pl.program_id(0) < half)(lambda: run(g0_ref, o0_ref))
    pl.when(pl.program_id(0) >= half)(lambda: run(g1_ref, o1_ref))


def drop_scalar(kernel):
    def wrapped(_, *refs):
        kernel(*refs)

    return wrapped


def attn_kernel(ids, q0_ref, q1_ref, do0_ref, do1_ref, kv_ref, h0_ref, h1_ref, g0_ref, g1_ref, cos_ref, sin_ref,
                own_ref, par_ref, *refs):
    sends, (s_ref, p_ref, ds_ref, acc_ref, ml_ref, kvt_ref, lhs_ref, gacc_ref) = refs[:-8], refs[-8:]
    send_ref, g_send_ref = sends[0], sends[-1]
    chip, core = ids[0], ids[1]
    b_id = pl.program_id(0)
    chips = kv_ref.shape[0]
    rows, tok = q0_ref.shape[1], q0_ref.shape[2]
    e = kv_ref.shape[3] // 2
    reps = rows // e
    blk = 2 * tok

    def heads_to_lanes(first_ref, second_ref):
        full = jnp.concatenate([first_ref[0], second_ref[0]], axis=1)
        return jnp.concatenate([full[i * e:(i + 1) * e] for i in range(reps)], axis=1)

    head_cols = [slice(i * blk, (i + 1) * blk) for i in range(reps)]

    def kv_block(i):
        return jnp.concatenate([kv_ref[chip - i, 0, 0], kv_ref[chip - i, 1, 0]], axis=1)

    def scores(i):
        qt = heads_to_lanes(q0_ref, q1_ref)
        q_pad = jnp.concatenate([qt, jnp.zeros_like(qt)], axis=0)
        kvt = kv_block(i).T
        kvt_ref[i] = kvt
        tops = []
        for cols in head_cols:
            t = dot(kvt, q_pad[:, cols])
            if i == 0:
                r = lax.broadcasted_iota(jnp.int32, (blk, blk), 0)
                c = lax.broadcasted_iota(jnp.int32, (blk, blk), 1)
                shift = (1 - 2 * core) * tok
                k_pos = jnp.where(r < tok, r, r - tok + shift)
                q_pos = jnp.where(c < tok, c, c - tok + shift)
                t = jnp.where(k_pos <= q_pos, t, MASK_VALUE)
            s_ref[i, :, cols] = t
            tops.append(jnp.max(t, axis=0, keepdims=True))
        return jnp.concatenate(tops, axis=1) * LOG2E

    def accumulate(i, m):
        v_t = kv_block(i)[e:2 * e]
        sums, outs = [], []
        for cols in head_cols:
            p = jnp.exp2(s_ref[i, :, cols] * LOG2E - m[:, cols])
            sums.append(jnp.sum(p, axis=0, keepdims=True))
            outs.append(dot(v_t, p.astype(BF16)))
        return jnp.concatenate(sums, axis=1), jnp.concatenate(outs, axis=1)

    ml_ref[0:1] = scores(0)
    ml_ref[1:2] = jnp.zeros_like(ml_ref[1:2])
    acc_ref[...] = jnp.zeros_like(acc_ref)

    for i in range(1, chips):
        @pl.when(i <= chip)
        def _(i=i):
            m = ml_ref[0:1]
            add_l, add_o = accumulate(i - 1, m)
            m_new = jnp.maximum(m, scores(i))
            alpha = jnp.exp2(m - m_new)
            acc_ref[...] = (acc_ref[...] + add_o) * alpha
            ml_ref[1:2] = (ml_ref[1:2] + add_l) * alpha
            ml_ref[0:1] = m_new

    m = ml_ref[0:1]
    add_l, add_o = accumulate(chip, m)
    l = ml_ref[1:2] + add_l
    o_t = (acc_ref[...] + add_o) * (1.0 / l)
    dot_t = heads_to_lanes(do0_ref, do1_ref)
    ml_ref[1:2] = jnp.sum(o_t * dot_t.astype(F32), axis=0, keepdims=True)
    ml_ref[0:1] = m + jnp.log2(l)
    o_b = o_t.astype(BF16)
    o_full = jnp.concatenate([o_b[:, cols] for cols in head_cols], axis=0)
    odd = lax.rem(b_id, 2)
    lhs_ref[odd, rows:2 * rows] = o_full
    own_ref[0, 0] = o_full[:, :tok]
    par_ref[0, 0] = o_full[:, tok:]
    acc_ref[...] = jnp.zeros_like(acc_ref)

    def score_grads(i):
        dot_t = heads_to_lanes(do0_ref, do1_ref)
        do_pad = jnp.concatenate([jnp.zeros_like(dot_t), dot_t], axis=0)
        kvt = kvt_ref[i]
        for cols in head_cols:
            p = jnp.exp2(s_ref[i, :, cols] * LOG2E - ml_ref[0:1, cols])
            dp = dot(kvt, do_pad[:, cols])
            p_ref[i, :, cols] = p.astype(BF16)
            ds_ref[i, :, cols] = (p * (dp - ml_ref[1:2, cols])).astype(BF16)

    def input_grads(i):
        qt = heads_to_lanes(q0_ref, q1_ref)
        dot_t = heads_to_lanes(do0_ref, do1_ref)
        k_t = kv_block(i)[0:e]
        dv = dot(dot_t, p_ref[i], NT)
        dk = dot(qt, ds_ref[i], NT)
        send_ref[chip - i, 0:2 * e, pl.ds(pl.multiple_of(b_id * blk, blk), blk)] = jnp.concatenate([dk, dv], axis=0).astype(BF16)
        acc_ref[...] += dot(k_t, ds_ref[i])

    score_grads(0)
    for i in range(1, chips):
        @pl.when(i <= chip)
        def _(i=i):
            input_grads(i - 1)
            score_grads(i)

    input_grads(chip)

    def zero_step(j, carry):
        send_ref[j, 0:2 * e, pl.ds(pl.multiple_of(b_id * blk, blk), blk)] = jnp.zeros((2 * e, blk), BF16)
        return carry

    lax.fori_loop(chip + 1, chips, zero_step, 0)

    cos = jnp.concatenate([cos_ref[0], cos_ref[1]], axis=1)
    sin = jnp.concatenate([sin_ref[0], sin_ref[1]], axis=1)
    dq_rows = []
    for cols in head_cols:
        dq = (acc_ref[:, cols] * (e ** -0.5)).astype(BF16).astype(F32)
        dq_rows.append(rope_rows(dq, cos, sin, -1.0).astype(BF16))
    dq_full = jnp.concatenate(dq_rows, axis=0)
    own_ref[1, 0] = dq_full[:, :tok]
    par_ref[1, 0] = dq_full[:, tok:]

    d = h0_ref.shape[2]
    step = 512
    lhs_ref[odd, 0:rows] = dq_full

    def weight_grads(first):
        for c in range(0, d, step):
            cs = slice(c, c + step)
            for r, (a_ref, b_ref) in enumerate(((h0_ref, h1_ref), (g0_ref, g1_ref))):
                rs = slice(r * rows, (r + 1) * rows)
                lhs = jnp.concatenate([lhs_ref[0, rs], lhs_ref[1, rs]], axis=1)
                rhs = jnp.concatenate([a_ref[0, :, cs], b_ref[0, :, cs], a_ref[1, :, cs], b_ref[1, :, cs]], axis=0)
                if first:
                    gacc_ref[rs, cs] = dot(lhs, rhs)
                else:
                    gacc_ref[rs, cs] += dot(lhs, rhs)

    pl.when(b_id == 1)(lambda: weight_grads(True))
    pl.when((odd == 1) & (b_id > 1))(lambda: weight_grads(False))

    @pl.when(b_id == pl.num_programs(0) - 1)
    def _():
        for j in range(chips):
            n = rows // chips
            base = 2 * e if len(sends) == 1 else 0
            g_send_ref[j, base:base + n] = gacc_ref[j * n:(j + 1) * n].astype(BF16)
            g_send_ref[j, base + n:base + 2 * n] = gacc_ref[rows + j * n:rows + (j + 1) * n].astype(BF16)


def kv_grad_kernel(*refs, stages):
    recv = refs[:stages]
    h0_ref, h1_ref, cos_ref, sin_ref, own_ref, par_ref, send_ref, gacc_ref = refs[stages:]
    nb, tok, d = h0_ref.shape
    e2 = own_ref.shape[1] // stages
    e = e2 // 2
    side = jnp.concatenate([cos_ref[0], cos_ref[1]], axis=1), jnp.concatenate([sin_ref[0], sin_ref[1]], axis=1)
    cos, sin = (jnp.concatenate([t] * nb, axis=1) for t in side)
    parts = []
    for r in recv:
        total = r[0].astype(F32)
        for j in range(1, r.shape[0]):
            total = total + r[j].astype(F32)
        total = total.astype(BF16).astype(F32)
        parts.append(jnp.concatenate([rope_rows(total[0:e], cos, sin, -1.0), total[e:2 * e]], axis=0).astype(BF16))
    gf = jnp.concatenate(parts, axis=0)
    for b in range(nb):
        own_ref[b] = gf[:, 2 * b * tok:(2 * b + 1) * tok]
        par_ref[b] = gf[:, (2 * b + 1) * tok:(2 * b + 2) * tok]

    def weight_grads(first):
        step = 512
        for c in range(0, d, step):
            cs = slice(c, c + step)
            hh = jnp.concatenate([r[b, :, cs] for b in range(nb) for r in (h0_ref, h1_ref)], axis=0)
            if first:
                gacc_ref[:, cs] = dot(gf, hh)
            else:
                gacc_ref[:, cs] += dot(gf, hh)

    pl.when(pl.program_id(0) == 0)(lambda: weight_grads(True))
    pl.when(pl.program_id(0) > 0)(lambda: weight_grads(False))

    @pl.when(pl.program_id(0) == pl.num_programs(0) - 1)
    def _():
        n = send_ref.shape[1]
        for j in range(send_ref.shape[0]):
            send_ref[j] = gacc_ref[j * n:(j + 1) * n].astype(BF16)


def out_kernel(ids, x_ref, w_ref, *refs, stages):
    core = ids[1]
    o_refs, (y_ref, lhs_ref) = refs[:-2], refs[-2:]
    nb, tok, d = x_ref.shape
    rows = o_refs[0].shape[2]
    half = stages * rows
    for side in range(2):
        base = (core if side == 0 else 1 - core) * half
        for s in range(stages):
            for b in range(nb):
                lhs_ref[b * tok:(b + 1) * tok, pl.ds(pl.multiple_of(base + s * rows, rows), rows)] = o_refs[side * stages + s][0, b].T
    lhs = lhs_ref[...]
    step = 512
    for c in range(0, d, step):
        prod = dot(lhs, w_ref[:, c:c + step])
        y_ref[:, :, c:c + step] = (x_ref[:, :, c:c + step].astype(F32) + prod.reshape(nb, tok, step)).astype(BF16)


def norm_grad_kernel(ids, x_ref, go_ref, g_ref, w_ref, kv0_ref, kv1_ref, *refs, stages):
    core = ids[1]
    q_refs = refs[:2 * stages]
    gh_ref, gn_ref, lhs_ref, tot_ref = refs[2 * stages:]
    nb, tok, d = x_ref.shape
    rows = q_refs[0].shape[2]
    half = stages * rows
    e2 = kv0_ref.shape[1] // stages
    e = e2 // 2
    kv_half = stages * e
    for side in range(2):
        who = core if side == 0 else 1 - core
        kv_ref = kv0_ref if side == 0 else kv1_ref
        for b in range(nb):
            ts = slice(b * tok, (b + 1) * tok)
            for s in range(stages):
                lhs_ref[ts, pl.ds(pl.multiple_of(who * half + s * rows, rows), rows)] = q_refs[side * stages + s][0, b].T
            ks = jnp.concatenate([kv_ref[b, i * e2:i * e2 + e] for i in range(stages)], axis=0)
            vs = jnp.concatenate([kv_ref[b, i * e2 + e:(i + 1) * e2] for i in range(stages)], axis=0)
            base = 2 * half
            lhs_ref[ts, pl.ds(pl.multiple_of(base + who * kv_half, kv_half), kv_half)] = ks.T
            base = base + 2 * kv_half
            lhs_ref[ts, pl.ds(pl.multiple_of(base + who * kv_half, kv_half), kv_half)] = vs.T
    lhs = lhs_ref[...]
    step = 256
    for c in range(0, d, step):
        tot_ref[:, c:c + step] = dot(lhs, w_ref[c:c + step, :], NT)

    @pl.when(pl.program_id(0) == 0)
    def _():
        gn_ref[...] = jnp.zeros_like(gn_ref)

    g = g_ref[...].astype(F32)
    for b in range(nb):
        total = tot_ref[b * tok:(b + 1) * tok]
        x = x_ref[b].astype(F32)
        inv = lax.rsqrt(jnp.mean(x * x, axis=-1, keepdims=True) + NORM_EPS)
        unit = x * inv
        gu = total * g
        mean_dot = jnp.mean(gu * unit, axis=-1, keepdims=True)
        gh_ref[b] = (go_ref[b].astype(F32) + inv * (gu - unit * mean_dot)).astype(BF16)
        gn_ref[...] += jnp.sum((total * unit).reshape(tok // 8, 8, d), axis=0)


def transpose_to(out_ref, blk):
    for c in range(0, blk.shape[1], 256):
        out_ref[c:c + 256, :] = blk[:, c:c + 256].astype(F32).T


def assemble_main_kernel(*refs, stages, n_q):
    ins, (wq_ref, wo_ref) = refs[:stages], refs[stages:]
    for s in range(stages):
        @pl.when(pl.program_id(1) == s)
        def _(ref=ins[s]):
            chips, _, n, d = ref.shape
            transpose_to(wq_ref, ref[:, 0, 0:n_q].reshape(chips * n_q, d))
            wo_ref[...] = ref[:, 0, n_q:n].astype(F32)


def assemble_tail_kernel(in_ref, _, out_ref):
    chips, _, n, d = in_ref.shape
    transpose_to(out_ref, in_ref[:, 0].reshape(chips * n, d))


def solution(mesh):
    chips = mesh.shape['sp'] // CORES
    mesh2 = Mesh(mesh.devices.reshape(mesh.shape['dp'], chips, CORES), ('dp', 'x', 'core'))
    swap = [(i, CORES - 1 - i) for i in range(CORES)]

    def device_step(hidden, norm_w, w_qkv, w_out, long_factor, grad_out):
        n_batch, tok, d = hidden.shape
        n_heads, e = w_out.shape[0], w_out.shape[1]
        kv_heads = (w_qkv.shape[1] // e - n_heads) // 2
        reps = n_heads // kv_heads
        stages = kv_heads // CORES
        rows = reps * e
        q_half = stages * rows
        kv_half = stages * e
        e2 = 2 * e
        half_rot = long_factor.shape[0]
        chip = lax.axis_index('x')
        core = lax.axis_index('core')
        ids = jnp.stack([chip, core]).astype(jnp.int32)
        tiles = 2
        nb = n_batch // tiles

        x_par = lax.ppermute(hidden, 'core', swap)
        go_par = lax.ppermute(grad_out, 'core', swap)
        w_o = w_out.reshape(n_heads * e, d)
        norm2 = norm_w.reshape(1, d)

        exponent = jnp.arange(half_rot, dtype=F32) / half_rot
        inv_freq = 1.0 / (long_factor * jnp.power(ROPE_BASE, exponent))
        sides = jnp.stack([core, 1 - core])
        positions = ((chip * CORES + sides)[:, None] * tok + jnp.arange(tok)[None, :]).astype(F32)
        angles = inv_freq[None, :, None] * positions[:, None, :]
        cos_t, sin_t = jnp.cos(angles) * ROPE_GAIN, jnp.sin(angles) * ROPE_GAIN

        tok_spec = pl.BlockSpec((nb, tok, d), lambda i, _: (i, 0, 0))
        rot_spec = pl.BlockSpec((half_rot, tok), lambda i, _: (0, 0))

        def kv_proj(x, side, filled):
            kb = 2 * q_half // kv_half
            kt = 4
            kn = n_batch // kt
            x_spec = pl.BlockSpec((kn, tok, d), lambda i, _: (i, 0, 0))
            any_spec = pl.BlockSpec(memory_space=pl.ANY)
            return pl.pallas_call(
                drop_scalar(kv_proj_kernel),
                out_shape=[jax.ShapeDtypeStruct((n_batch, tok, d), BF16)]
                + [jax.ShapeDtypeStruct((2, n_batch, e2, tok), BF16)] * stages,
                grid_spec=pltpu.PrefetchScalarGridSpec(
                    num_scalar_prefetch=1, grid=(kt,),
                    in_specs=[x_spec, pl.BlockSpec((1, d), lambda i, _: (0, 0)),
                              pl.BlockSpec((d, kv_half), lambda i, c: (0, kb + c[1])),
                              pl.BlockSpec((d, kv_half), lambda i, c: (0, kb + CORES + c[1])), rot_spec, rot_spec]
                    + [any_spec] * len(filled),
                    out_specs=[x_spec] + [pl.BlockSpec((1, kn, e2, tok), lambda i, _: (side, i, 0, 0))] * stages),
                input_output_aliases={7 + i: 1 + i for i in range(len(filled))},
                compiler_params=params(), name='kv_proj',
                cost_estimate=cost(2 * n_batch * tok * d * 2 * kv_half, 3 * n_batch * tok * d * 2),
            )(ids, x, norm2, w_qkv, w_qkv, cos_t[side], sin_t[side], *filled)

        first = lambda i: jnp.minimum(i, tiles - 1)
        second = lambda i: jnp.maximum(i - tiles, 0)
        own_spec = pl.BlockSpec((nb, tok, d), lambda i, _: (first(i), 0, 0))
        par_spec = pl.BlockSpec((nb, tok, d), lambda i, _: (second(i), 0, 0))
        own_out = pl.BlockSpec((nb, q_half, tok), lambda i, _: (first(i), 0, 0))
        par_out = pl.BlockSpec((nb, q_half, tok), lambda i, _: (second(i), 0, 0))
        both_rot = pl.BlockSpec((2, half_rot, tok), lambda i, _: (0, 0, 0))
        q_shapes = (jax.ShapeDtypeStruct((n_batch, q_half, tok), BF16), jax.ShapeDtypeStruct((n_batch, q_half, tok), BF16))

        def q_proj(h0, h1):
            return pl.pallas_call(
                drop_scalar(q_proj_kernel), out_shape=q_shapes,
                grid_spec=pltpu.PrefetchScalarGridSpec(
                    num_scalar_prefetch=1, grid=(2 * tiles,),
                    in_specs=[own_spec, par_spec, pl.BlockSpec((d, q_half), lambda i, c: (0, c[1])), both_rot, both_rot],
                    out_specs=(own_out, par_out)),
                compiler_params=params(), name='q_proj',
                cost_estimate=cost(4 * n_batch * tok * d * q_half, 6 * n_batch * tok * d * 2),
            )(ids, h0, h1, w_qkv, cos_t, sin_t)

        def do_proj(g0, g1):
            return pl.pallas_call(
                drop_scalar(do_proj_kernel), out_shape=q_shapes,
                grid_spec=pltpu.PrefetchScalarGridSpec(
                    num_scalar_prefetch=1, grid=(2 * tiles,),
                    in_specs=[own_spec, par_spec, pl.BlockSpec((q_half, d), lambda i, c: (c[1], 0))],
                    out_specs=(own_out, par_out)),
                compiler_params=params(), name='do_proj',
                cost_estimate=cost(4 * n_batch * tok * d * q_half, 6 * n_batch * tok * d * 2),
            )(ids, g0, g1, w_o)

        h_own, *kv_sides = kv_proj(hidden, 0, [])
        h_par, *kv_sides = kv_proj(x_par, 1, kv_sides)
        gathered = []
        for s in range(stages):
            gathered.append(lax.all_gather(kv_sides[s], 'x'))
        q_own, q_par = q_proj(h_own, h_par)
        do_own, do_par = do_proj(grad_out, go_par)

        def attention(s):
            blk = 2 * tok
            n_g = 2 * rows // chips
            parts = [e2, n_g] if s == stages - 1 else [e2 + n_g]
            q_spec = pl.BlockSpec((1, rows, tok), lambda b, _: (b, s, 0))
            t_spec = pl.BlockSpec((2, tok, d), lambda b, _: (b // 2, 0, 0))
            r_spec = pl.BlockSpec((2, half_rot, tok), lambda b, _: (0, 0, 0))
            o_spec = pl.BlockSpec((2, 1, rows, tok), lambda b, _: (0, b, 0, 0))
            return pl.pallas_call(
                attn_kernel,
                out_shape=[jax.ShapeDtypeStruct((2, n_batch, rows, tok), BF16)] * 2
                + [jax.ShapeDtypeStruct((chips, n, d), BF16) for n in parts],
                grid_spec=pltpu.PrefetchScalarGridSpec(
                    num_scalar_prefetch=1, grid=(n_batch,),
                    in_specs=[q_spec, q_spec, q_spec, q_spec,
                              pl.BlockSpec((chips, 2, 1, e2, tok), lambda b, _: (0, 0, b, 0, 0)),
                              t_spec, t_spec, t_spec, t_spec, r_spec, r_spec],
                    out_specs=[o_spec, o_spec] + [pl.BlockSpec((chips, n, d), lambda b, _: (0, 0, 0)) for n in parts],
                    scratch_shapes=[pltpu.VMEM((chips, blk, reps * blk), F32), pltpu.VMEM((chips, blk, reps * blk), BF16),
                                    pltpu.VMEM((chips, blk, reps * blk), BF16), pltpu.VMEM((e, reps * blk), F32),
                                    pltpu.VMEM((8, reps * blk), F32),
                                    pltpu.VMEM((chips, blk, e2), BF16), pltpu.VMEM((2, 2 * rows, blk), BF16),
                                    pltpu.VMEM((2 * rows, d), F32)]),
                compiler_params=params(),
                cost_estimate=cost(4e10, 3e7, 3e7),
            )(ids, q_own, q_par, do_own, do_par, gathered[s], h_own, h_par, grad_out, go_par, cos_t, sin_t)

        own, par, recv = [], [], []
        for s in range(stages):
            own_s, par_s, *sends = attention(s)
            own.append(own_s)
            par.append(lax.ppermute(par_s, 'core', swap))
            recv.append(lax.all_to_all(sends[0], 'x', 0, 0, tiled=True))

        g_send, recv[-1] = lax.optimization_barrier((sends[1], recv[-1]))
        recv_g = lax.all_to_all(g_send, 'x', 0, 0, tiled=True)
        n_w = 2 * rows // chips
        shards = [jnp.sum(r.astype(F32), axis=0).astype(BF16) for r in [r[:, e2:] for r in recv[:-1]] + [recv_g]]

        gb = 2
        gf_spec = pl.BlockSpec((gb, stages * e2, tok), lambda b: (b, 0, 0))
        kv_own_g, kv_par_g, send_kv = pl.pallas_call(
            functools.partial(kv_grad_kernel, stages=stages),
            out_shape=[jax.ShapeDtypeStruct((n_batch, stages * e2, tok), BF16)] * 2
            + [jax.ShapeDtypeStruct((chips, stages * e2 // chips, d), BF16)],
            grid=(n_batch // gb,),
            in_specs=[pl.BlockSpec((chips, e2, 2 * tok * gb), lambda b: (0, 0, b))] * stages
            + [pl.BlockSpec((gb, tok, d), lambda b: (b, 0, 0))] * 2 + [pl.BlockSpec((2, half_rot, tok), lambda b: (0, 0, 0))] * 2,
            out_specs=[gf_spec, gf_spec, pl.BlockSpec((chips, stages * e2 // chips, d), lambda b: (0, 0, 0))],
            scratch_shapes=[pltpu.VMEM((stages * e2, d), F32)],
            compiler_params=params(), name='kv_grad',
            cost_estimate=cost(2 * 2 * n_batch * tok * d * stages * e2, 3e7),
        )(*recv, h_own, h_par, cos_t, sin_t)
        kv_other_g = lax.ppermute(kv_par_g, 'core', swap)
        recv_kv = lax.all_to_all(send_kv, 'x', 0, 0, tiled=True)
        shard_kv = jnp.sum(recv_kv.astype(F32), axis=0).astype(BF16)

        nb2 = 2
        t2_spec = pl.BlockSpec((nb2, tok, d), lambda b, _: (b, 0, 0))
        block_out = pl.pallas_call(
            functools.partial(out_kernel, stages=stages),
            out_shape=jax.ShapeDtypeStruct((n_batch, tok, d), BF16),
            grid_spec=pltpu.PrefetchScalarGridSpec(
                num_scalar_prefetch=1, grid=(n_batch // nb2,),
                in_specs=[t2_spec, pl.BlockSpec((n_heads * e, d), lambda b, _: (0, 0))]
                + [pl.BlockSpec((1, nb2, rows, tok), lambda b, _: (0, b, 0, 0))] * (2 * stages),
                out_specs=t2_spec, scratch_shapes=[pltpu.VMEM((nb2 * tok, n_heads * e), BF16)]),
            compiler_params=params(), name='out_proj',
            cost_estimate=cost(2 * n_batch * tok * d * n_heads * e, 3e7),
        )(ids, hidden, w_o, *own, *par)

        nb2 = nb
        t2_spec = pl.BlockSpec((nb2, tok, d), lambda b, _: (b, 0, 0))
        grad_hidden, gn = pl.pallas_call(
            functools.partial(norm_grad_kernel, stages=stages),
            out_shape=(jax.ShapeDtypeStruct((n_batch, tok, d), BF16), jax.ShapeDtypeStruct((8, d), F32)),
            grid_spec=pltpu.PrefetchScalarGridSpec(
                num_scalar_prefetch=1, grid=(n_batch // nb2,),
                in_specs=[t2_spec, t2_spec, pl.BlockSpec((1, d), lambda b, _: (0, 0)),
                          pl.BlockSpec(w_qkv.shape, lambda b, _: (0, 0))]
                + [pl.BlockSpec((nb2, stages * e2, tok), lambda b, _: (b, 0, 0))] * 2
                + [pl.BlockSpec((1, nb2, rows, tok), lambda b, _: (1, b, 0, 0))] * (2 * stages),
                out_specs=(t2_spec, pl.BlockSpec((8, d), lambda b, _: (0, 0))),
                scratch_shapes=[pltpu.VMEM((nb2 * tok, w_qkv.shape[1]), BF16), pltpu.VMEM((nb2 * tok, d), F32)]),
            compiler_params=params(), name='norm_grad',
            cost_estimate=cost(2 * n_batch * tok * d * w_qkv.shape[1], 4e7),
        )(ids, hidden, grad_out, norm2, w_qkv, kv_own_g, kv_other_g, *own, *par)

        gn_row = jnp.sum(gn, axis=0, keepdims=True)
        gn_hi = gn_row.astype(BF16)
        gn_lo = (gn_row - gn_hi.astype(F32)).astype(BF16)
        pad = jnp.zeros((14, d), BF16)
        tail = lax.all_gather(jnp.concatenate([shard_kv, gn_hi, gn_lo, pad], axis=0), ('x', 'core'))
        tail = tail.reshape(chips, CORES, -1, d)
        n_kv = shard_kv.shape[0]
        n_q = rows // chips
        main = [lax.all_gather(s, ('x', 'core')).reshape(chips, CORES, n_w, d) for s in shards]
        w_cols, grad_w_out = pl.pallas_call(
            functools.partial(assemble_main_kernel, stages=stages, n_q=n_q),
            out_shape=(jax.ShapeDtypeStruct(w_qkv.shape, F32), jax.ShapeDtypeStruct((n_heads, e, d), F32)),
            grid=(CORES, stages),
            in_specs=[pl.BlockSpec((chips, 1, n_w, d), lambda p, s: (0, p, 0, 0))] * stages,
            out_specs=(pl.BlockSpec((d, rows), lambda p, s: (0, p * stages + s)),
                       pl.BlockSpec((reps, e, d), lambda p, s: (p * stages + s, 0, 0))),
            compiler_params=params(2), name='assemble_main', cost_estimate=cost(2e9, 6e7),
        )(*main)
        kcol = 2 * q_half // kv_half
        grad_w_qkv = pl.pallas_call(
            assemble_tail_kernel,
            out_shape=jax.ShapeDtypeStruct(w_qkv.shape, F32),
            grid=(CORES, 2),
            in_specs=[pl.BlockSpec((chips, 1, e, d), lambda p, k: (0, p, k, 0)), pl.BlockSpec(memory_space=pl.ANY)],
            out_specs=pl.BlockSpec((d, kv_half), lambda p, k: (0, kcol + k * CORES + p)),
            input_output_aliases={1: 0},
            compiler_params=params(2), name='assemble_tail', cost_estimate=cost(1e9, 2e7),
        )(tail, w_cols)
        gn_all = tail[:, :, n_kv:n_kv + 2].astype(F32)
        grad_norm_w = jnp.sum(gn_all, axis=(0, 1, 2))
        return block_out, grad_hidden, grad_w_qkv, grad_w_out, grad_norm_w

    tok_spec = P('dp', ('x', 'core'), None)
    return jax.shard_map(device_step, mesh=mesh2,
                         in_specs=(tok_spec, P(), P(), P(), P(), tok_spec),
                         out_specs=(tok_spec, tok_spec, P('dp', None), P('dp', None, None), P('dp')),
                         check_vma=False)
```

```python
import functools
import math

import jax
import jax.numpy as jnp
from jax import lax
from jax.experimental import pallas as pl
from jax.experimental.pallas import tpu as pltpu
from jax.sharding import Mesh, PartitionSpec as P


NORM_EPS = 1e-5
ROPE_BASE = 10000.0
ROPE_GAIN = math.sqrt(1.0 + math.log(32.0) / math.log(4096.0))
MASK_VALUE = -1e30
LOG2E = math.log2(math.e)
CORES = 2
PAIR = 2
BF16 = jnp.bfloat16
F32 = jnp.float32
VMEM_LIMIT = 60 * 1024 * 1024

NN = (((1,), (0,)), ((), ()))
NT = (((1,), (1,)), ((), ()))


cat_rows = functools.partial(jnp.concatenate, axis=0)
cat_lanes = functools.partial(jnp.concatenate, axis=1)
column_max = functools.partial(jnp.max, axis=0, keepdims=True)
column_sum = functools.partial(jnp.sum, axis=0, keepdims=True)
row_mean = functools.partial(jnp.mean, axis=-1, keepdims=True)


def whole(*shape):
    return pl.BlockSpec(shape, lambda *_: (0,) * len(shape))


def along(axis, *shape):
    return pl.BlockSpec(shape, lambda i, *_: tuple(i if n == axis else 0 for n in range(len(shape))))


def dot(a, b, dims=NN):
    return lax.dot_general(a, b, dims, preferred_element_type=F32)


def cost(flops, nbytes, trans=0):
    return pl.CostEstimate(flops=int(flops), bytes_accessed=int(nbytes), transcendentals=int(trans))


def params(n_axes=1):
    return pltpu.CompilerParams(dimension_semantics=("arbitrary",) * n_axes, vmem_limit_bytes=VMEM_LIMIT)


def rope_rows(block, cos, sin, direction):
    half = cos.shape[0]
    a, b = block[:half], block[half:PAIR * half]
    s = sin * direction
    return cat_rows([a * cos - b * s, b * cos + a * s])


def kv_proj_kernel(x_ref, g_ref, wk_ref, wv_ref, cos_ref, sin_ref, *refs):
    nb, tok, d = x_ref.shape
    stages = (wk_ref.shape[1] // (PAIR * cos_ref.shape[0]))
    h_ref, kv_refs = refs[-stages - 1], refs[-stages:]
    e2 = kv_refs[0].shape[2]
    e = e2 // 2
    x = x_ref[:].reshape(nb * tok, d).astype(F32)
    inv = lax.rsqrt(row_mean(x * x) + NORM_EPS)
    h = (x * inv * g_ref[:].astype(F32)).astype(BF16)
    h_ref[:] = h.reshape(nb, tok, d)
    cos, sin = cos_ref[:], sin_ref[:]
    k = dot(h, wk_ref[:]).T
    v = dot(h, wv_ref[:]).T
    for i in range(stages):
        for b in range(nb):
            kv_refs[i][0, b, 0:e] = rope_rows(k[i * e:(i + 1) * e, b * tok:(b + 1) * tok], cos, sin, 1.0).astype(BF16)
            kv_refs[i][0, b, e:PAIR * e] = v[i * e:(i + 1) * e, b * tok:(b + 1) * tok].astype(BF16)


def q_proj_kernel(h0_ref, h1_ref, w_ref, cos_ref, sin_ref, q0_ref, q1_ref):
    nb, tok, d = h0_ref.shape
    e = PAIR * cos_ref.shape[1]
    rows = w_ref.shape[1]
    scale = e ** -0.5
    step = 4 * e

    def run(h_ref, q_ref, side):
        h = h_ref[:].reshape(nb * tok, d)
        cos, sin = cos_ref[side], sin_ref[side]
        for r in range(0, rows, step):
            blk = dot(h, w_ref[:, r:r + step]).T
            for i in range(0, step, e):
                for b in range(nb):
                    q_ref[b, r + i:r + i + e] = (rope_rows(blk[i:i + e, b * tok:(b + 1) * tok], cos, sin, 1.0).astype(BF16)
                                                 * scale).astype(BF16)

    half = pl.num_programs(0) // 2
    pl.when(pl.program_id(0) < half)(lambda: run(h0_ref, q0_ref, 0))
    pl.when(pl.program_id(0) >= half)(lambda: run(h1_ref, q1_ref, 1))


def do_proj_kernel(g0_ref, g1_ref, w_ref, o0_ref, o1_ref):
    nb, tok, d = g0_ref.shape
    rows = w_ref.shape[0]
    step = 512

    def run(g_ref, o_ref):
        g = g_ref[:].reshape(nb * tok, d)
        for r in range(0, rows, step):
            blk = dot(w_ref[r:r + step], g, NT)
            for b in range(nb):
                o_ref[b, r:r + step] = blk[:, b * tok:(b + 1) * tok].astype(BF16)

    half = pl.num_programs(0) // 2
    pl.when(pl.program_id(0) < half)(lambda: run(g0_ref, o0_ref))
    pl.when(pl.program_id(0) >= half)(lambda: run(g1_ref, o1_ref))


def drop_scalar(kernel):
    def wrapped(_, *refs):
        kernel(*refs)

    return wrapped


def ring_peers(chips):
    chip, core = lax.axis_index('x'), lax.axis_index('core')
    return chip, lax.rem(chip + 1, chips), lax.rem(chip + chips - 1, chips), lax.rem(chip + 2, chips), core, 1 - core


def ring_barrier(chips):
    _, right, left, _, _, mate = ring_peers(chips)
    sem = pltpu.get_barrier_semaphore()
    for who in ({'x': right}, {'x': left}, {'core': mate}):
        pl.semaphore_signal(sem, inc=1, device_id=who, device_id_type=pl.DeviceIdType.MESH)
    pl.semaphore_wait(sem, 3)


class RingSum:
    @staticmethod
    def scratch(chips, rows, d):
        half = rows // 2
        return [pltpu.VMEM((2, half, d), BF16), pltpu.VMEM((2, half, d), BF16), pltpu.VMEM((rows, d), BF16),
                pltpu.VMEM((2, rows, d), BF16), pltpu.SemaphoreType.DMA((6,)), pltpu.SemaphoreType.DMA((6,)),
                pltpu.SemaphoreType.DMA((3,))]

    def __init__(self, send_ref, total_ref, mid, buf, own, recv, s_sem, r_sem, l_sem):
        chips, rows, _ = send_ref.shape
        half = rows // 2
        chip, right, left, far, _, _ = ring_peers(chips)
        top, low = pl.ds(0, half), pl.ds(half, half)

        def remote(n, src, dst, who):
            return pltpu.make_async_remote_copy(src_ref=src, dst_ref=dst, send_sem=s_sem.at[n], recv_sem=r_sem.at[n],
                                                device_id={'x': who}, device_id_type=pl.DeviceIdType.MESH)

        self.first = [remote(0, send_ref.at[far, top], mid.at[0], right), remote(1, send_ref.at[far, low], mid.at[1], left),
                      remote(2, send_ref.at[left, top], recv.at[1, top], left),
                      remote(3, send_ref.at[right, low], recv.at[0, low], right)]
        self.second = [remote(4, buf.at[0], recv.at[0, top], right), remote(5, buf.at[1], recv.at[1, low], left)]
        self.local = [pltpu.make_async_copy(send_ref.at[right, top], buf.at[0], l_sem.at[0]),
                      pltpu.make_async_copy(send_ref.at[left, low], buf.at[1], l_sem.at[1]),
                      pltpu.make_async_copy(send_ref.at[chip], own, l_sem.at[2])]
        self.mid, self.buf, self.own, self.recv, self.total_ref = mid, buf, own, recv, total_ref

    def start(self):
        for c in self.first[:2] + self.local:
            c.start()

    def start_direct(self):
        for c in self.first[2:]:
            c.start()

    def merge(self):
        for i in range(2):
            self.local[i].wait()
            self.first[i].wait_recv()
            self.buf[i] = (self.buf[i].astype(F32) + self.mid[i].astype(F32)).astype(BF16)

    def send(self):
        for c in self.second:
            c.start()

    def finish(self):
        self.local[2].wait()
        for c in self.first[2:] + self.second:
            c.wait_recv()
        self.total_ref[:] = (self.own[:].astype(F32) + self.recv[0].astype(F32) + self.recv[1].astype(F32)).astype(BF16)
        for c in self.first + self.second:
            c.wait_send()


class RingGather:
    @staticmethod
    def scratch():
        return [pltpu.SemaphoreType.DMA((8,)), pltpu.SemaphoreType.DMA((8,)), pltpu.SemaphoreType.DMA((1,))]

    def __init__(self, block_ref, out_ref, s_sem, r_sem, l_sem):
        chips, rows = out_ref.shape[1], out_ref.shape[2]
        chip, right, left, far, core, mate = ring_peers(chips)
        top, low = pl.ds(0, rows // 2), pl.ds(rows // 2, rows // 2)

        def remote(n, src, dst, who):
            return pltpu.make_async_remote_copy(src_ref=src, dst_ref=dst, send_sem=s_sem.at[n], recv_sem=r_sem.at[n],
                                                device_id=who, device_id_type=pl.DeviceIdType.MESH)

        mine = out_ref.at[core]
        self.local = pltpu.make_async_copy(block_ref, mine.at[chip], l_sem.at[0])
        self.first = [remote(0, block_ref, mine.at[chip], {'x': right}), remote(1, block_ref, mine.at[chip], {'x': left})]
        self.second = [remote(2, mine.at[left, top], mine.at[left, top], {'x': right}),
                       remote(3, mine.at[right, low], mine.at[right, low], {'x': left})]
        self.mate = [remote(4, block_ref, mine.at[chip], {'core': mate})] + [
            remote(5 + i, mine.at[j], mine.at[j], {'core': mate}) for i, j in enumerate((left, right, far))]

    def start(self):
        for c in [self.local, *self.first, self.mate[0]]:
            c.start()

    def forward(self):
        for c in self.first:
            c.wait_recv()
        for c in self.second + self.mate[1:3]:
            c.start()

    def last(self):
        for c in self.second:
            c.wait_recv()
        self.mate[3].start()

    def finish(self):
        self.local.wait()
        for c in self.mate:
            c.wait_recv()
        for c in self.first + self.second + self.mate:
            c.wait_send()


def run_at(step, n, *actions):
    @pl.when(step == n)
    def _():
        for a in actions:
            a()


def host_rings(ring_sum, gather, step, plan, chips):
    if ring_sum is None and gather is None:
        return
    direct, merge, forward = plan
    run_at(step, 0, lambda: ring_barrier(chips), *([ring_sum.start] if ring_sum else []), *([gather.start] if gather else []))
    if ring_sum:
        run_at(step, direct, ring_sum.start_direct)
        run_at(step, merge + 1, ring_sum.send)
    if gather:
        run_at(step, forward, gather.forward)


def finish_rings(ring_sum, gather, step, plan, final):
    if ring_sum:
        run_at(step, plan[1], ring_sum.merge)
    last = ([gather.last] if gather else []) + ([ring_sum.finish] if ring_sum else []) + ([gather.finish] if gather else [])
    if last:
        run_at(step, final, *last)


def comm_params(cid, n_axes=1):
    return pltpu.CompilerParams(dimension_semantics=("arbitrary",) * n_axes, vmem_limit_bytes=VMEM_LIMIT,
                                collective_id=cid, has_side_effects=True)


def attn_kernel(q0_ref, q1_ref, do0_ref, do1_ref, kv_ref, h0_ref, h1_ref, g0_ref, g1_ref, cos_ref, sin_ref, *refs,
                has_sum, has_gather):
    refs = list(refs)
    ring_sum = gather = None
    prev_ref = refs.pop(0) if has_sum else None
    shard_ref = refs.pop(0) if has_gather else None
    own_ref, par_ref, send_ref = refs[:3]
    refs = refs[3:]
    total_ref = refs.pop(0) if has_sum else None
    all_ref = refs.pop(0) if has_gather else None
    s_ref, p_ref, ds_ref, acc_ref, ml_ref, kvt_ref, lhs_ref, gacc_ref = refs[:8]
    refs = refs[8:]
    if has_sum:
        ring_sum = RingSum(prev_ref, total_ref, *refs[:7])
        refs = refs[7:]
    if has_gather:
        gather = RingGather(shard_ref, all_ref, *refs)
    g_send_ref = send_ref
    chip, core = lax.axis_index('x'), lax.axis_index('core')
    b_id = pl.program_id(0)
    plan = (2, 3, 4)
    host_rings(ring_sum, gather, b_id, plan, kv_ref.shape[0])
    chips = kv_ref.shape[0]
    rows, tok = q0_ref.shape[1], q0_ref.shape[2]
    e = kv_ref.shape[3] // 2
    reps = rows // e
    blk = PAIR * tok

    def heads_to_lanes(first_ref, second_ref):
        full = cat_lanes([first_ref[0], second_ref[0]])
        return cat_lanes([full[i * e:(i + 1) * e] for i in range(reps)])

    head_cols = [slice(i * blk, (i + 1) * blk) for i in range(reps)]

    def kv_block(i):
        return cat_lanes([kv_ref[chip - i, 0, 0], kv_ref[chip - i, 1, 0]])

    def scores(i):
        qt = heads_to_lanes(q0_ref, q1_ref)
        q_pad = cat_rows([qt, jnp.zeros_like(qt)])
        kvt = kv_block(i).T
        kvt_ref[i] = kvt
        tops = []
        for cols in head_cols:
            t = dot(kvt, q_pad[:, cols])
            if i == 0:
                r = lax.broadcasted_iota(jnp.int32, (blk, blk), 0)
                c = lax.broadcasted_iota(jnp.int32, (blk, blk), 1)
                shift = (1 - PAIR * core) * tok
                k_pos = jnp.where(r < tok, r, r - tok + shift)
                q_pos = jnp.where(c < tok, c, c - tok + shift)
                t = jnp.where(k_pos <= q_pos, t, MASK_VALUE)
            s_ref[i, :, cols] = t
            tops.append(column_max(t))
        return cat_lanes(tops) * LOG2E

    def accumulate(i, m):
        v_t = kv_block(i)[e:PAIR * e]
        sums, outs = [], []
        for cols in head_cols:
            p = jnp.exp2(s_ref[i, :, cols] * LOG2E - m[:, cols])
            sums.append(column_sum(p))
            outs.append(dot(v_t, p.astype(BF16)))
        return cat_lanes(sums), cat_lanes(outs)

    ml_ref[0:1] = scores(0)
    ml_ref[1:2] = jnp.zeros_like(ml_ref[1:2])
    acc_ref[:] = jnp.zeros_like(acc_ref)

    for i in range(1, chips):
        @pl.when(i <= chip)
        def _(i=i):
            m = ml_ref[0:1]
            add_l, add_o = accumulate(i - 1, m)
            m_new = jnp.maximum(m, scores(i))
            alpha = jnp.exp2(m - m_new)
            acc_ref[:] = (acc_ref[:] + add_o) * alpha
            ml_ref[1:2] = (ml_ref[1:2] + add_l) * alpha
            ml_ref[0:1] = m_new

    m = ml_ref[0:1]
    add_l, add_o = accumulate(chip, m)
    l = ml_ref[1:2] + add_l
    o_t = (acc_ref[:] + add_o) * (1.0 / l)
    dot_t = heads_to_lanes(do0_ref, do1_ref)
    ml_ref[1:2] = column_sum(o_t * dot_t.astype(F32))
    ml_ref[0:1] = m + jnp.log2(l)
    o_b = o_t.astype(BF16)
    o_full = cat_rows([o_b[:, cols] for cols in head_cols])
    odd = lax.rem(b_id, 2)
    lhs_ref[odd, rows:PAIR * rows] = o_full
    own_ref[0, 0] = o_full[:, :tok]
    par_ref[0, 0] = o_full[:, tok:]
    acc_ref[:] = jnp.zeros_like(acc_ref)

    def score_grads(i):
        dot_t = heads_to_lanes(do0_ref, do1_ref)
        do_pad = cat_rows([jnp.zeros_like(dot_t), dot_t])
        kvt = kvt_ref[i]
        for cols in head_cols:
            p = jnp.exp2(s_ref[i, :, cols] * LOG2E - ml_ref[0:1, cols])
            dp = dot(kvt, do_pad[:, cols])
            p_ref[i, :, cols] = p.astype(BF16)
            ds_ref[i, :, cols] = (p * (dp - ml_ref[1:2, cols])).astype(BF16)

    def input_grads(i):
        qt = heads_to_lanes(q0_ref, q1_ref)
        dot_t = heads_to_lanes(do0_ref, do1_ref)
        k_t = kv_block(i)[0:e]
        dv = dot(dot_t, p_ref[i], NT)
        dk = dot(qt, ds_ref[i], NT)
        send_ref[chip - i, 0:PAIR * e, pl.ds(pl.multiple_of(b_id * blk, blk), blk)] = cat_rows([dk, dv]).astype(BF16)
        acc_ref[:] += dot(k_t, ds_ref[i])

    score_grads(0)
    for i in range(1, chips):
        @pl.when(i <= chip)
        def _(i=i):
            input_grads(i - 1)
            score_grads(i)

    input_grads(chip)

    def zero_step(j, carry):
        send_ref[j, 0:PAIR * e, pl.ds(pl.multiple_of(b_id * blk, blk), blk)] = jnp.zeros((PAIR * e, blk), BF16)
        return carry

    lax.fori_loop(chip + 1, chips, zero_step, 0)

    cos = cat_lanes([cos_ref[0], cos_ref[1]])
    sin = cat_lanes([sin_ref[0], sin_ref[1]])
    dq_rows = []
    for cols in head_cols:
        dq = (acc_ref[:, cols] * (e ** -0.5)).astype(BF16).astype(F32)
        dq_rows.append(rope_rows(dq, cos, sin, -1.0).astype(BF16))
    dq_full = cat_rows(dq_rows)
    own_ref[1, 0] = dq_full[:, :tok]
    par_ref[1, 0] = dq_full[:, tok:]

    d = h0_ref.shape[2]
    step = 512
    lhs_ref[odd, 0:rows] = dq_full

    def weight_grads(first):
        for c in range(0, d, step):
            cs = slice(c, c + step)
            for r, (a_ref, b_ref) in enumerate(((h0_ref, h1_ref), (g0_ref, g1_ref))):
                rs = slice(r * rows, (r + 1) * rows)
                lhs = cat_lanes([lhs_ref[0, rs], lhs_ref[1, rs]])
                rhs = cat_rows([a_ref[0, :, cs], b_ref[0, :, cs], a_ref[1, :, cs], b_ref[1, :, cs]])
                if first:
                    gacc_ref[rs, cs] = dot(lhs, rhs)
                else:
                    gacc_ref[rs, cs] += dot(lhs, rhs)

    pl.when(b_id == 1)(lambda: weight_grads(True))
    pl.when((odd == 1) & (b_id > 1))(lambda: weight_grads(False))

    @pl.when(b_id == pl.num_programs(0) - 1)
    def _():
        for j in range(chips):
            n = rows // chips
            base = PAIR * e
            g_send_ref[j, base:base + n] = gacc_ref[j * n:(j + 1) * n].astype(BF16)
            g_send_ref[j, base + n:base + PAIR * n] = gacc_ref[rows + j * n:rows + (j + 1) * n].astype(BF16)

    finish_rings(ring_sum, gather, b_id, plan, pl.num_programs(0) - 1)


def kv_grad_kernel(*refs, stages):
    recv = refs[:stages]
    h0_ref, h1_ref, cos_ref, sin_ref, shard_ref, own_ref, par_ref, send_ref, all_ref, gacc_ref = refs[stages:stages + 10]
    gather = RingGather(shard_ref, all_ref, *refs[stages + 10:])
    plan = (0, 0, 3)
    host_rings(None, gather, pl.program_id(0), plan, all_ref.shape[1])
    nb, tok, d = h0_ref.shape
    e2 = own_ref.shape[1] // stages
    e = e2 // 2
    side = cat_lanes([cos_ref[0], cos_ref[1]]), cat_lanes([sin_ref[0], sin_ref[1]])
    cos, sin = (cat_lanes([t] * nb) for t in side)
    parts = []
    for r in recv:
        total = r[:].astype(F32)
        parts.append(cat_rows([rope_rows(total[0:e], cos, sin, -1.0), total[e:PAIR * e]]).astype(BF16))
    gf = cat_rows(parts)
    for b in range(nb):
        own_ref[b] = gf[:, PAIR * b * tok:(PAIR * b + 1) * tok]
        par_ref[b] = gf[:, (PAIR * b + 1) * tok:(PAIR * b + 2) * tok]

    def weight_grads(first):
        step = 512
        for c in range(0, d, step):
            cs = slice(c, c + step)
            hh = cat_rows([r[b, :, cs] for b in range(nb) for r in (h0_ref, h1_ref)])
            if first:
                gacc_ref[:, cs] = dot(gf, hh)
            else:
                gacc_ref[:, cs] += dot(gf, hh)

    pl.when(pl.program_id(0) == 0)(lambda: weight_grads(True))
    pl.when(pl.program_id(0) > 0)(lambda: weight_grads(False))

    @pl.when(pl.program_id(0) == pl.num_programs(0) - 1)
    def _():
        n = send_ref.shape[1]
        for j in range(send_ref.shape[0]):
            send_ref[j] = gacc_ref[j * n:(j + 1) * n].astype(BF16)

    finish_rings(None, gather, pl.program_id(0), plan, pl.num_programs(0) - 1)


def out_kernel(x_ref, w_ref, prev_ref, *refs, stages):
    core = lax.axis_index('core')
    o_refs, (y_ref, total_ref, lhs_ref) = refs[:PAIR * stages], refs[PAIR * stages:PAIR * stages + 3]
    ring_sum = RingSum(prev_ref, total_ref, *refs[PAIR * stages + 3:])
    plan = (1, 2, 0)
    host_rings(ring_sum, None, pl.program_id(0), plan, prev_ref.shape[0])
    nb, tok, d = x_ref.shape
    rows = o_refs[0].shape[2]
    half = stages * rows
    for side in range(2):
        base = (core if side == 0 else 1 - core) * half
        for s in range(stages):
            for b in range(nb):
                lhs_ref[b * tok:(b + 1) * tok, pl.ds(pl.multiple_of(base + s * rows, rows), rows)] = o_refs[side * stages + s][0, b].T
    lhs = lhs_ref[:]
    step = 512
    for c in range(0, d, step):
        prod = dot(lhs, w_ref[:, c:c + step])
        y_ref[:, :, c:c + step] = (x_ref[:, :, c:c + step].astype(F32) + prod.reshape(nb, tok, step)).astype(BF16)

    finish_rings(ring_sum, None, pl.program_id(0), plan, pl.num_programs(0) - 1)


def norm_grad_kernel(x_ref, go_ref, g_ref, w_ref, kv0_ref, kv1_ref, prev_ref, shard_ref, *refs, stages):
    core = lax.axis_index('core')
    q_refs = refs[:PAIR * stages]
    gh_ref, gn_ref, total_ref, all_ref, lhs_ref, tot_ref = refs[PAIR * stages:PAIR * stages + 6]
    ring_sum = RingSum(prev_ref, total_ref, *refs[PAIR * stages + 6:PAIR * stages + 13])
    gather = RingGather(shard_ref, all_ref, *refs[PAIR * stages + 13:])
    plan = (1, 0, 2)
    host_rings(ring_sum, gather, pl.program_id(0), plan, prev_ref.shape[0])
    nb, tok, d = x_ref.shape
    rows = q_refs[0].shape[2]
    half = stages * rows
    e2 = kv0_ref.shape[1] // stages
    e = e2 // 2
    kv_half = stages * e
    for side in range(2):
        who = core if side == 0 else 1 - core
        kv_ref = kv0_ref if side == 0 else kv1_ref
        for b in range(nb):
            ts = slice(b * tok, (b + 1) * tok)
            for s in range(stages):
                lhs_ref[ts, pl.ds(pl.multiple_of(who * half + s * rows, rows), rows)] = q_refs[side * stages + s][0, b].T
            ks = cat_rows([kv_ref[b, i * e2:i * e2 + e] for i in range(stages)])
            vs = cat_rows([kv_ref[b, i * e2 + e:(i + 1) * e2] for i in range(stages)])
            base = PAIR * half
            lhs_ref[ts, pl.ds(pl.multiple_of(base + who * kv_half, kv_half), kv_half)] = ks.T
            base = base + PAIR * kv_half
            lhs_ref[ts, pl.ds(pl.multiple_of(base + who * kv_half, kv_half), kv_half)] = vs.T
    lhs = lhs_ref[:]
    step = 256
    for c in range(0, d, step):
        tot_ref[:, c:c + step] = dot(lhs, w_ref[c:c + step, :], NT)

    @pl.when(pl.program_id(0) == 0)
    def _():
        gn_ref[:] = jnp.zeros_like(gn_ref)

    g = g_ref[:].astype(F32)
    for b in range(nb):
        total = tot_ref[b * tok:(b + 1) * tok]
        x = x_ref[b].astype(F32)
        inv = lax.rsqrt(row_mean(x * x) + NORM_EPS)
        unit = x * inv
        gu = total * g
        mean_dot = row_mean(gu * unit)
        gh_ref[b] = (go_ref[b].astype(F32) + inv * (gu - unit * mean_dot)).astype(BF16)
        gn_ref[:] += jnp.sum((total * unit).reshape(tok // 8, 8, d), axis=0)

    finish_rings(ring_sum, gather, pl.program_id(0), plan, pl.num_programs(0) - 1)


def transpose_to(out_ref, blk):
    for c in range(0, blk.shape[1], 256):
        out_ref[c:c + 256, :] = blk[:, c:c + 256].astype(F32).T


def assemble_main_kernel(*refs, stages, n_q):
    ins, (y_ref, gh_ref, wq_ref, wo_ref, y_out, gh_out) = refs[:stages], refs[stages:]
    y_out[:] = y_ref[:]
    gh_out[:] = gh_ref[:]
    for s in range(stages):
        @pl.when(pl.program_id(1) == s)
        def _(ref=ins[s]):
            _, chips, n, d = ref.shape
            transpose_to(wq_ref, ref[0, :, 0:n_q].reshape(chips * n_q, d))
            wo_ref[:] = ref[0, :, n_q:n].astype(F32)


def assemble_tail_kernel(in_ref, _, out_ref):
    chips, _, n, d = in_ref.shape
    transpose_to(out_ref, in_ref[:, 0].reshape(chips * n, d))


def solution(mesh):
    chips = mesh.shape['sp'] // CORES
    mesh2 = Mesh(mesh.devices.reshape(mesh.shape['dp'], chips, CORES), ('dp', 'x', 'core'))
    swap = [(i, CORES - 1 - i) for i in range(CORES)]

    def device_step(hidden, norm_w, w_qkv, w_out, long_factor, grad_out):
        n_batch, tok, d = hidden.shape
        n_heads, e = w_out.shape[0], w_out.shape[1]
        kv_heads = (w_qkv.shape[1] // e - n_heads) // 2
        reps = n_heads // kv_heads
        stages = kv_heads // CORES
        rows = reps * e
        q_half = stages * rows
        kv_half = stages * e
        e2 = PAIR * e
        half_rot = long_factor.shape[0]
        chip = lax.axis_index('x')
        core = lax.axis_index('core')
        ids = jnp.stack([chip, core]).astype(jnp.int32)
        tiles = 2
        nb = n_batch // tiles

        x_par = lax.ppermute(hidden, 'core', swap)
        go_par = lax.ppermute(grad_out, 'core', swap)
        w_o = w_out.reshape(n_heads * e, d)
        norm2 = norm_w.reshape(1, d)

        exponent = jnp.arange(half_rot, dtype=F32) / half_rot
        inv_freq = 1.0 / (long_factor * jnp.power(ROPE_BASE, exponent))
        sides = jnp.stack([core, 1 - core])
        positions = ((chip * CORES + sides)[:, None] * tok + jnp.arange(tok)[None, :]).astype(F32)
        angles = inv_freq[None, :, None] * positions[:, None, :]
        cos_t, sin_t = jnp.cos(angles) * ROPE_GAIN, jnp.sin(angles) * ROPE_GAIN

        tok_spec = along(0, nb, tok, d)
        rot_spec = whole(half_rot, tok)

        def kv_proj(x, side, filled):
            kb = PAIR * q_half // kv_half
            kt = 4
            kn = n_batch // kt
            x_spec = along(0, kn, tok, d)
            any_spec = pl.BlockSpec(memory_space=pl.ANY)
            return pl.pallas_call(
                drop_scalar(kv_proj_kernel),
                out_shape=[jax.ShapeDtypeStruct((n_batch, tok, d), BF16)]
                + [jax.ShapeDtypeStruct((2, n_batch, e2, tok), BF16)] * stages,
                grid_spec=pltpu.PrefetchScalarGridSpec(
                    num_scalar_prefetch=1, grid=(kt,),
                    in_specs=[x_spec, whole(1, d),
                              pl.BlockSpec((d, kv_half), lambda i, c: (0, kb + c[1])),
                              pl.BlockSpec((d, kv_half), lambda i, c: (0, kb + CORES + c[1])), rot_spec, rot_spec]
                    + [any_spec] * len(filled),
                    out_specs=[x_spec] + [pl.BlockSpec((1, kn, e2, tok), lambda i, _: (side, i, 0, 0))] * stages),
                input_output_aliases={7 + i: 1 + i for i in range(len(filled))},
                compiler_params=params(), name='kv_proj',
                cost_estimate=cost(PAIR * n_batch * tok * d * PAIR * kv_half, 3 * n_batch * tok * d * 2),
            )(ids, x, norm2, w_qkv, w_qkv, cos_t[side], sin_t[side], *filled)

        first = lambda i: jnp.minimum(i, tiles - 1)
        second = lambda i: jnp.maximum(i - tiles, 0)
        own_spec = pl.BlockSpec((nb, tok, d), lambda i, _: (first(i), 0, 0))
        par_spec = pl.BlockSpec((nb, tok, d), lambda i, _: (second(i), 0, 0))
        own_out = pl.BlockSpec((nb, q_half, tok), lambda i, _: (first(i), 0, 0))
        par_out = pl.BlockSpec((nb, q_half, tok), lambda i, _: (second(i), 0, 0))
        both_rot = whole(2, half_rot, tok)
        q_shapes = (jax.ShapeDtypeStruct((n_batch, q_half, tok), BF16), jax.ShapeDtypeStruct((n_batch, q_half, tok), BF16))

        def q_proj(h0, h1):
            return pl.pallas_call(
                drop_scalar(q_proj_kernel), out_shape=q_shapes,
                grid_spec=pltpu.PrefetchScalarGridSpec(
                    num_scalar_prefetch=1, grid=(PAIR * tiles,),
                    in_specs=[own_spec, par_spec, pl.BlockSpec((d, q_half), lambda i, c: (0, c[1])), both_rot, both_rot],
                    out_specs=(own_out, par_out)),
                compiler_params=params(), name='q_proj',
                cost_estimate=cost(4 * n_batch * tok * d * q_half, 6 * n_batch * tok * d * 2),
            )(ids, h0, h1, w_qkv, cos_t, sin_t)

        def do_proj(g0, g1):
            return pl.pallas_call(
                drop_scalar(do_proj_kernel), out_shape=q_shapes,
                grid_spec=pltpu.PrefetchScalarGridSpec(
                    num_scalar_prefetch=1, grid=(PAIR * tiles,),
                    in_specs=[own_spec, par_spec, pl.BlockSpec((q_half, d), lambda i, c: (c[1], 0))],
                    out_specs=(own_out, par_out)),
                compiler_params=params(), name='do_proj',
                cost_estimate=cost(4 * n_batch * tok * d * q_half, 6 * n_batch * tok * d * 2),
            )(ids, g0, g1, w_o)

        h_own, *kv_sides = kv_proj(hidden, 0, [])
        h_par, *kv_sides = kv_proj(x_par, 1, kv_sides)
        gathered = []
        for s in range(stages):
            gathered.append(lax.all_gather(kv_sides[s], 'x'))
        q_own, q_par = q_proj(h_own, h_par)
        do_own, do_par = do_proj(grad_out, go_par)

        n_g = PAIR * rows // chips
        n_s = e2 + n_g
        hbm = pl.BlockSpec(memory_space=pl.ANY)
        shard_spec = lambda n: whole(n, d)

        def gathered_shape(n):
            return jax.ShapeDtypeStruct((CORES, chips, n, d), BF16)

        def attention(s, prev, shard):
            blk = PAIR * tok
            has_sum, has_gather = prev is not None, shard is not None
            q_spec = pl.BlockSpec((1, rows, tok), lambda b: (b, s, 0))
            t_spec = pl.BlockSpec((2, tok, d), lambda b: (b // 2, 0, 0))
            r_spec = whole(2, half_rot, tok)
            o_spec = along(1, 2, 1, rows, tok)
            return pl.pallas_call(
                functools.partial(attn_kernel, has_sum=has_sum, has_gather=has_gather),
                out_shape=[jax.ShapeDtypeStruct((2, n_batch, rows, tok), BF16)] * 2
                + [jax.ShapeDtypeStruct((chips, n_s, d), BF16)]
                + [jax.ShapeDtypeStruct((n_s, d), BF16)] * has_sum + [gathered_shape(n_g)] * has_gather,
                grid=(n_batch,),
                in_specs=[q_spec, q_spec, q_spec, q_spec, along(2, chips, 2, 1, e2, tok),
                          t_spec, t_spec, t_spec, t_spec, r_spec, r_spec]
                + [hbm] * has_sum + [shard_spec(n_g)] * has_gather,
                out_specs=[o_spec, o_spec, whole(chips, n_s, d)]
                + [shard_spec(n_s)] * has_sum + [hbm] * has_gather,
                scratch_shapes=[pltpu.VMEM((chips, blk, reps * blk), F32), pltpu.VMEM((chips, blk, reps * blk), BF16),
                                pltpu.VMEM((chips, blk, reps * blk), BF16), pltpu.VMEM((e, reps * blk), F32),
                                pltpu.VMEM((8, reps * blk), F32),
                                pltpu.VMEM((chips, blk, e2), BF16), pltpu.VMEM((2, PAIR * rows, blk), BF16),
                                pltpu.VMEM((PAIR * rows, d), F32)]
                + (RingSum.scratch(chips, n_s, d) if has_sum else []) + (RingGather.scratch() if has_gather else []),
                compiler_params=comm_params(s) if has_sum else params(),
                cost_estimate=cost(4e10, 3e7, 3e7),
            )(q_own, q_par, do_own, do_par, gathered[s], h_own, h_par, grad_out, go_par, cos_t, sin_t,
              *([prev] if has_sum else []), *([shard] if has_gather else []))

        own, par, totals, main = [], [], [], []
        prev = None
        for s in range(stages):
            shard = totals[s - 2][e2:] if s >= 2 else None
            outs = attention(s, prev, shard)
            own.append(outs[0])
            par.append(lax.ppermute(outs[1], 'core', swap))
            prev = outs[2]
            totals += outs[3:4]
            main += outs[4:5]

        nb2 = 2
        t2_spec = along(0, nb2, tok, d)
        block_out, total = pl.pallas_call(
            functools.partial(out_kernel, stages=stages),
            out_shape=[jax.ShapeDtypeStruct((n_batch, tok, d), BF16), jax.ShapeDtypeStruct((n_s, d), BF16)],
            grid=(n_batch // nb2,),
            in_specs=[t2_spec, whole(n_heads * e, d), hbm]
            + [along(1, 1, nb2, rows, tok)] * (PAIR * stages),
            out_specs=[t2_spec, shard_spec(n_s)],
            scratch_shapes=[pltpu.VMEM((nb2 * tok, n_heads * e), BF16)] + RingSum.scratch(chips, n_s, d),
            compiler_params=comm_params(stages), name='out_proj',
            cost_estimate=cost(PAIR * n_batch * tok * d * n_heads * e, 3e7),
        )(hidden, w_o, prev, *own, *par)
        totals.append(total)

        gb = 2
        gf_spec = along(0, gb, stages * e2, tok)
        n_kv = stages * e2 // chips
        kv_own_g, kv_par_g, send_kv, main_2 = pl.pallas_call(
            functools.partial(kv_grad_kernel, stages=stages),
            out_shape=[jax.ShapeDtypeStruct((n_batch, stages * e2, tok), BF16)] * 2
            + [jax.ShapeDtypeStruct((chips, n_kv, d), BF16), gathered_shape(n_g)],
            grid=(n_batch // gb,),
            in_specs=[along(1, e2, PAIR * tok * gb)] * stages
            + [along(0, gb, tok, d)] * 2 + [whole(2, half_rot, tok)] * 2
            + [shard_spec(n_g)],
            out_specs=[gf_spec, gf_spec, whole(chips, n_kv, d), hbm],
            scratch_shapes=[pltpu.VMEM((stages * e2, d), F32)] + RingGather.scratch(),
            compiler_params=comm_params(stages + 1), name='kv_grad',
            cost_estimate=cost(PAIR * PAIR * n_batch * tok * d * stages * e2, 3e7),
        )(*totals, h_own, h_par, cos_t, sin_t, totals[-2][e2:])
        main.append(main_2)
        kv_other_g = lax.ppermute(kv_par_g, 'core', swap)

        nb3 = 2
        t3_spec = along(0, nb3, tok, d)
        grad_hidden, gn, shard_kv, main_3 = pl.pallas_call(
            functools.partial(norm_grad_kernel, stages=stages),
            out_shape=[jax.ShapeDtypeStruct((n_batch, tok, d), BF16), jax.ShapeDtypeStruct((8, d), F32),
                       jax.ShapeDtypeStruct((n_kv, d), BF16), gathered_shape(n_g)],
            grid=(n_batch // nb3,),
            in_specs=[t3_spec, t3_spec, whole(1, d), whole(*w_qkv.shape)]
            + [along(0, nb3, stages * e2, tok)] * 2 + [hbm, shard_spec(n_g)]
            + [pl.BlockSpec((1, nb3, rows, tok), lambda b: (1, b, 0, 0))] * (PAIR * stages),
            out_specs=[t3_spec, whole(8, d), shard_spec(n_kv), hbm],
            scratch_shapes=[pltpu.VMEM((nb3 * tok, w_qkv.shape[1]), BF16), pltpu.VMEM((nb3 * tok, d), F32)]
            + RingSum.scratch(chips, n_kv, d) + RingGather.scratch(),
            compiler_params=comm_params(stages + 2), name='norm_grad',
            cost_estimate=cost(PAIR * n_batch * tok * d * w_qkv.shape[1], 4e7),
        )(hidden, grad_out, norm2, w_qkv, kv_own_g, kv_other_g, send_kv, totals[-1][e2:], *own, *par)
        main.append(main_3)

        gn_row = jnp.sum(gn, axis=0, keepdims=True)
        gn_hi = gn_row.astype(BF16)
        gn_lo = (gn_row - gn_hi.astype(F32)).astype(BF16)
        n_t = n_kv + 16
        tail_block = cat_rows([shard_kv, gn_hi, gn_lo, jnp.zeros((n_t - n_kv - 2, d), BF16)])
        tail = lax.all_gather(tail_block, ('x', 'core')).reshape(chips, CORES, n_t, d)
        n_q = rows // chips
        b_spec = pl.BlockSpec((n_batch // (CORES * stages), tok, d), lambda p, s: (p * stages + s, 0, 0))
        w_cols, grad_w_out, block_out, grad_hidden = pl.pallas_call(
            functools.partial(assemble_main_kernel, stages=stages, n_q=n_q),
            out_shape=[jax.ShapeDtypeStruct(w_qkv.shape, F32), jax.ShapeDtypeStruct((n_heads, e, d), F32)]
            + [jax.ShapeDtypeStruct((n_batch, tok, d), BF16)] * PAIR,
            grid=(CORES, stages),
            in_specs=[along(0, 1, chips, n_g, d)] * stages + [b_spec] * PAIR,
            out_specs=[pl.BlockSpec((d, rows), lambda p, s: (0, p * stages + s)),
                       pl.BlockSpec((reps, e, d), lambda p, s: (p * stages + s, 0, 0)), b_spec, b_spec],
            compiler_params=params(2), name='assemble_main', cost_estimate=cost(2e9, 6e7),
        )(*main, block_out, grad_hidden)
        kcol = PAIR * q_half // kv_half
        grad_w_qkv = pl.pallas_call(
            assemble_tail_kernel,
            out_shape=jax.ShapeDtypeStruct(w_qkv.shape, F32),
            grid=(CORES, 2),
            in_specs=[pl.BlockSpec((chips, 1, e, d), lambda p, k: (0, p, k, 0)), pl.BlockSpec(memory_space=pl.ANY)],
            out_specs=pl.BlockSpec((d, kv_half), lambda p, k: (0, kcol + k * CORES + p)),
            input_output_aliases={1: 0},
            compiler_params=params(2), name='assemble_tail', cost_estimate=cost(1e9, 2e7),
        )(tail, w_cols)
        gn_all = tail[:, :, n_kv:n_kv + 2].astype(F32)
        grad_norm_w = jnp.sum(gn_all, axis=(0, 1, 2))
        return block_out, grad_hidden, grad_w_qkv, grad_w_out, grad_norm_w

    tok_spec = P('dp', ('x', 'core'), None)
    return jax.shard_map(device_step, mesh=mesh2,
                         in_specs=(tok_spec, P(), P(), P(), P(), tok_spec),
                         out_specs=(tok_spec, tok_spec, P('dp', None), P('dp', None, None), P('dp')),
                         check_vma=False)
```

```python
import functools
import math

import jax
import jax.numpy as jnp
from jax import lax
from jax.experimental import pallas as pl
from jax.experimental.pallas import tpu as pltpu
from jax.sharding import Mesh, PartitionSpec as P


NORM_EPS = 1e-5
ROPE_BASE = 10000.0
ROPE_GAIN = math.sqrt(1.0 + math.log(32.0) / math.log(4096.0))
MASK_VALUE = -1e30
LOG2E = math.log2(math.e)
CORES = 2
PAIR = 2
BF16 = jnp.bfloat16
F32 = jnp.float32
VMEM_LIMIT = 60 * 1024 * 1024

NN = (((1,), (0,)), ((), ()))
NT = (((1,), (1,)), ((), ()))


cat_rows = functools.partial(jnp.concatenate, axis=0)
cat_lanes = functools.partial(jnp.concatenate, axis=1)
column_max = functools.partial(jnp.max, axis=0, keepdims=True)
column_sum = functools.partial(jnp.sum, axis=0, keepdims=True)
row_mean = functools.partial(jnp.mean, axis=-1, keepdims=True)


def whole(*shape):
    return pl.BlockSpec(shape, lambda *_: (0,) * len(shape))


def along(axis, *shape):
    return pl.BlockSpec(shape, lambda i, *_: tuple(i if n == axis else 0 for n in range(len(shape))))


def dot(a, b, dims=NN):
    return lax.dot_general(a, b, dims, preferred_element_type=F32)


def cost(flops, nbytes, trans=0):
    return pl.CostEstimate(flops=int(flops), bytes_accessed=int(nbytes), transcendentals=int(trans))


def params(n_axes=1):
    return pltpu.CompilerParams(dimension_semantics=("arbitrary",) * n_axes, vmem_limit_bytes=VMEM_LIMIT)


def rope_rows(block, cos, sin, direction):
    half = cos.shape[0]
    a, b = block[:half], block[half:PAIR * half]
    s = sin * direction
    return cat_rows([a * cos - b * s, b * cos + a * s])


def kv_proj_kernel(x_ref, g_ref, wk_ref, wv_ref, cos_ref, sin_ref, *refs):
    nb, tok, d = x_ref.shape
    stages = (wk_ref.shape[1] // (PAIR * cos_ref.shape[0]))
    h_ref, kv_refs = refs[-stages - 1], refs[-stages:]
    e2 = kv_refs[0].shape[2]
    e = e2 // 2
    x = x_ref[:].reshape(nb * tok, d).astype(F32)
    inv = lax.rsqrt(row_mean(x * x) + NORM_EPS)
    h = (x * inv * g_ref[:].astype(F32)).astype(BF16)
    h_ref[:] = h.reshape(nb, tok, d)
    cos, sin = cos_ref[:], sin_ref[:]
    k = dot(h, wk_ref[:]).T
    v = dot(h, wv_ref[:]).T
    for i in range(stages):
        for b in range(nb):
            kv_refs[i][0, b, 0:e] = rope_rows(k[i * e:(i + 1) * e, b * tok:(b + 1) * tok], cos, sin, 1.0).astype(BF16)
            kv_refs[i][0, b, e:PAIR * e] = v[i * e:(i + 1) * e, b * tok:(b + 1) * tok].astype(BF16)


def q_proj_kernel(h0_ref, h1_ref, w_ref, cos_ref, sin_ref, q0_ref, q1_ref):
    nb, tok, d = h0_ref.shape
    e = PAIR * cos_ref.shape[1]
    rows = w_ref.shape[1]
    scale = e ** -0.5
    step = 4 * e

    def run(h_ref, q_ref, side):
        h = h_ref[:].reshape(nb * tok, d)
        cos, sin = cos_ref[side], sin_ref[side]
        for r in range(0, rows, step):
            blk = dot(h, w_ref[:, r:r + step]).T
            for i in range(0, step, e):
                for b in range(nb):
                    q_ref[b, r + i:r + i + e] = (rope_rows(blk[i:i + e, b * tok:(b + 1) * tok], cos, sin, 1.0).astype(BF16)
                                                 * scale).astype(BF16)

    half = pl.num_programs(0) // 2
    pl.when(pl.program_id(0) < half)(lambda: run(h0_ref, q0_ref, 0))
    pl.when(pl.program_id(0) >= half)(lambda: run(h1_ref, q1_ref, 1))


def do_proj_kernel(g0_ref, g1_ref, w_ref, o0_ref, o1_ref):
    nb, tok, d = g0_ref.shape
    rows = w_ref.shape[0]
    step = 512

    def run(g_ref, o_ref):
        g = g_ref[:].reshape(nb * tok, d)
        for r in range(0, rows, step):
            blk = dot(w_ref[r:r + step], g, NT)
            for b in range(nb):
                o_ref[b, r:r + step] = blk[:, b * tok:(b + 1) * tok].astype(BF16)

    half = pl.num_programs(0) // 2
    pl.when(pl.program_id(0) < half)(lambda: run(g0_ref, o0_ref))
    pl.when(pl.program_id(0) >= half)(lambda: run(g1_ref, o1_ref))


def drop_scalar(kernel):
    def wrapped(_, *refs):
        kernel(*refs)

    return wrapped


def ring_peers(chips):
    chip, core = lax.axis_index('x'), lax.axis_index('core')
    return chip, lax.rem(chip + 1, chips), lax.rem(chip + chips - 1, chips), lax.rem(chip + 2, chips), core, 1 - core


def ring_barrier(chips):
    _, right, left, _, _, _ = ring_peers(chips)
    sem = pltpu.get_barrier_semaphore()
    for who in (right, left):
        pl.semaphore_signal(sem, inc=1, device_id={'x': who}, device_id_type=pl.DeviceIdType.MESH)
    pl.semaphore_wait(sem, 2)


class RingSum:
    @staticmethod
    def scratch(rows, d):
        half = rows // 2
        return [pltpu.VMEM((PAIR, half, d), BF16), pltpu.VMEM((PAIR, half, d), BF16), pltpu.VMEM((rows, d), BF16),
                pltpu.VMEM((PAIR, rows, d), BF16), pltpu.SemaphoreType.DMA((6,)), pltpu.SemaphoreType.DMA((6,)),
                pltpu.SemaphoreType.DMA((3,))]

    def __init__(self, send_ref, totals, plan, base, mid, buf, own, recv, s_sem, r_sem, l_sem):
        self.chips = chips = send_ref.shape[0]
        rows = own.shape[0]
        half = rows // 2
        chip, right, left, far, _, _ = ring_peers(chips)
        top, low = pl.ds(0, half), pl.ds(half, half)
        from_top, from_low = pl.ds(base, half), pl.ds(base + half, half)

        def remote(n, src, dst, who):
            return pltpu.make_async_remote_copy(src_ref=src, dst_ref=dst, send_sem=s_sem.at[n], recv_sem=r_sem.at[n],
                                                device_id={'x': who}, device_id_type=pl.DeviceIdType.MESH)

        self.far = [remote(0, send_ref.at[far, from_top], mid.at[0], right),
                    remote(1, send_ref.at[far, from_low], mid.at[1], left)]
        self.direct = [remote(2, send_ref.at[left, from_top], recv.at[1, top], left),
                       remote(3, send_ref.at[right, from_low], recv.at[0, low], right)]
        self.second = [remote(4, buf.at[0], recv.at[0, top], right), remote(5, buf.at[1], recv.at[1, low], left)]
        self.local = [pltpu.make_async_copy(send_ref.at[right, from_top], buf.at[0], l_sem.at[0]),
                      pltpu.make_async_copy(send_ref.at[left, from_low], buf.at[1], l_sem.at[1]),
                      pltpu.make_async_copy(send_ref.at[chip, pl.ds(base, rows)], own, l_sem.at[2])]
        self.mid, self.buf, self.own, self.recv, self.totals = mid, buf, own, recv, totals
        self.plan = plan

    def start(self):
        ring_barrier(self.chips)
        for c in self.far + self.local:
            c.start()

    def start_direct(self):
        for c in self.direct:
            c.start()

    def merge(self):
        for far, local, buf, mid in zip(self.far, self.local, (self.buf.at[0], self.buf.at[1]), (self.mid.at[0], self.mid.at[1])):
            local.wait()
            far.wait_recv()
            buf[:] = (buf[:].astype(F32) + mid[:].astype(F32)).astype(BF16)

    def send(self):
        for c in self.second:
            c.start()

    def finish(self):
        self.local[-1].wait()
        for c in self.direct + self.second:
            c.wait_recv()
        row = 0
        for ref in self.totals:
            r = slice(row, row + ref.shape[0])
            ref[:] = (self.own[r].astype(F32) + self.recv[0, r].astype(F32) + self.recv[1, r].astype(F32)).astype(BF16)
            row += ref.shape[0]
        for c in self.far + self.direct + self.second:
            c.wait_send()

    def ahead(self, step):
        direct, merge = self.plan
        run_at(step, 0, self.start)
        run_at(step, direct, self.start_direct)
        run_at(step, merge + 1, self.send)

    def behind(self, step, final):
        run_at(step, self.plan[1], self.merge)
        run_at(step, final, self.finish)


def run_at(step, n, *actions):
    @pl.when(step == n)
    def _():
        for a in actions:
            a()


def comm_params(cid, n_axes=1):
    return pltpu.CompilerParams(dimension_semantics=("arbitrary",) * n_axes, vmem_limit_bytes=VMEM_LIMIT,
                                collective_id=cid, has_side_effects=True)


def attn_kernel(q0_ref, q1_ref, do0_ref, do1_ref, kv_ref, h0_ref, h1_ref, g0_ref, g1_ref, cos_ref, sin_ref, *refs,
                has_sum):
    refs = list(refs)
    prev_ref = refs.pop(0) if has_sum else None
    own_ref, par_ref, send_ref = refs[:3]
    refs = refs[3:]
    totals = [refs.pop(0), refs.pop(0)] if has_sum else []
    s_ref, p_ref, ds_ref, acc_ref, ml_ref, kvt_ref, lhs_ref, gacc_ref = refs[:8]
    chip, core = lax.axis_index('x'), lax.axis_index('core')
    b_id = pl.program_id(0)
    if has_sum:
        ring_sum = RingSum(prev_ref, totals, (2, 3), 0, *refs[8:])
        ring_sum.ahead(b_id)
    chips = kv_ref.shape[0]
    rows, tok = q0_ref.shape[1], q0_ref.shape[2]
    e = kv_ref.shape[3] // 2
    reps = rows // e
    blk = PAIR * tok

    def heads_to_lanes(first_ref, second_ref):
        full = cat_lanes([first_ref[0], second_ref[0]])
        return cat_lanes([full[i * e:(i + 1) * e] for i in range(reps)])

    head_cols = [slice(i * blk, (i + 1) * blk) for i in range(reps)]

    def kv_block(i):
        return cat_lanes([kv_ref[chip - i, 0, 0], kv_ref[chip - i, 1, 0]])

    def scores(i):
        qt = heads_to_lanes(q0_ref, q1_ref)
        q_pad = cat_rows([qt, jnp.zeros_like(qt)])
        kvt = kv_block(i).T
        kvt_ref[i] = kvt
        tops = []
        for cols in head_cols:
            t = dot(kvt, q_pad[:, cols])
            if i == 0:
                r = lax.broadcasted_iota(jnp.int32, (blk, blk), 0)
                c = lax.broadcasted_iota(jnp.int32, (blk, blk), 1)
                shift = (1 - PAIR * core) * tok
                k_pos = jnp.where(r < tok, r, r - tok + shift)
                q_pos = jnp.where(c < tok, c, c - tok + shift)
                t = jnp.where(k_pos <= q_pos, t, MASK_VALUE)
            s_ref[i, :, cols] = t
            tops.append(column_max(t))
        return cat_lanes(tops) * LOG2E

    def accumulate(i, m):
        v_t = kv_block(i)[e:PAIR * e]
        sums, outs = [], []
        for cols in head_cols:
            p = jnp.exp2(s_ref[i, :, cols] * LOG2E - m[:, cols])
            sums.append(column_sum(p))
            outs.append(dot(v_t, p.astype(BF16)))
        return cat_lanes(sums), cat_lanes(outs)

    ml_ref[0:1] = scores(0)
    ml_ref[1:2] = jnp.zeros_like(ml_ref[1:2])
    acc_ref[:] = jnp.zeros_like(acc_ref)

    for i in range(1, chips):
        @pl.when(i <= chip)
        def _(i=i):
            m = ml_ref[0:1]
            add_l, add_o = accumulate(i - 1, m)
            m_new = jnp.maximum(m, scores(i))
            alpha = jnp.exp2(m - m_new)
            acc_ref[:] = (acc_ref[:] + add_o) * alpha
            ml_ref[1:2] = (ml_ref[1:2] + add_l) * alpha
            ml_ref[0:1] = m_new

    m = ml_ref[0:1]
    add_l, add_o = accumulate(chip, m)
    l = ml_ref[1:2] + add_l
    o_t = (acc_ref[:] + add_o) * (1.0 / l)
    dot_t = heads_to_lanes(do0_ref, do1_ref)
    ml_ref[1:2] = column_sum(o_t * dot_t.astype(F32))
    ml_ref[0:1] = m + jnp.log2(l)
    o_b = o_t.astype(BF16)
    o_full = cat_rows([o_b[:, cols] for cols in head_cols])
    odd = lax.rem(b_id, 2)
    lhs_ref[odd, rows:PAIR * rows] = o_full
    own_ref[0, 0] = o_full[:, :tok]
    par_ref[0, 0] = o_full[:, tok:]
    acc_ref[:] = jnp.zeros_like(acc_ref)

    def score_grads(i):
        dot_t = heads_to_lanes(do0_ref, do1_ref)
        do_pad = cat_rows([jnp.zeros_like(dot_t), dot_t])
        kvt = kvt_ref[i]
        for cols in head_cols:
            p = jnp.exp2(s_ref[i, :, cols] * LOG2E - ml_ref[0:1, cols])
            dp = dot(kvt, do_pad[:, cols])
            p_ref[i, :, cols] = p.astype(BF16)
            ds_ref[i, :, cols] = (p * (dp - ml_ref[1:2, cols])).astype(BF16)

    def input_grads(i):
        qt = heads_to_lanes(q0_ref, q1_ref)
        dot_t = heads_to_lanes(do0_ref, do1_ref)
        k_t = kv_block(i)[0:e]
        dv = dot(dot_t, p_ref[i], NT)
        dk = dot(qt, ds_ref[i], NT)
        send_ref[chip - i, 0:PAIR * e, pl.ds(pl.multiple_of(b_id * blk, blk), blk)] = cat_rows([dk, dv]).astype(BF16)
        acc_ref[:] += dot(k_t, ds_ref[i])

    score_grads(0)
    for i in range(1, chips):
        @pl.when(i <= chip)
        def _(i=i):
            input_grads(i - 1)
            score_grads(i)

    input_grads(chip)

    def zero_step(j, carry):
        send_ref[j, 0:PAIR * e, pl.ds(pl.multiple_of(b_id * blk, blk), blk)] = jnp.zeros((PAIR * e, blk), BF16)
        return carry

    lax.fori_loop(chip + 1, chips, zero_step, 0)

    cos = cat_lanes([cos_ref[0], cos_ref[1]])
    sin = cat_lanes([sin_ref[0], sin_ref[1]])
    dq_rows = []
    for cols in head_cols:
        dq = (acc_ref[:, cols] * (e ** -0.5)).astype(BF16).astype(F32)
        dq_rows.append(rope_rows(dq, cos, sin, -1.0).astype(BF16))
    dq_full = cat_rows(dq_rows)
    own_ref[1, 0] = dq_full[:, :tok]
    par_ref[1, 0] = dq_full[:, tok:]

    d = h0_ref.shape[2]
    step = 512
    lhs_ref[odd, 0:rows] = dq_full

    def weight_grads(first):
        for c in range(0, d, step):
            cs = slice(c, c + step)
            for r, (a_ref, b_ref) in enumerate(((h0_ref, h1_ref), (g0_ref, g1_ref))):
                rs = slice(r * rows, (r + 1) * rows)
                lhs = cat_lanes([lhs_ref[0, rs], lhs_ref[1, rs]])
                rhs = cat_rows([a_ref[0, :, cs], b_ref[0, :, cs], a_ref[1, :, cs], b_ref[1, :, cs]])
                if first:
                    gacc_ref[rs, cs] = dot(lhs, rhs)
                else:
                    gacc_ref[rs, cs] += dot(lhs, rhs)

    pl.when(b_id == 1)(lambda: weight_grads(True))
    pl.when((odd == 1) & (b_id > 1))(lambda: weight_grads(False))

    @pl.when(b_id == pl.num_programs(0) - 1)
    def _():
        for j in range(chips):
            n = rows // chips
            base = PAIR * e
            send_ref[j, base:base + n] = gacc_ref[j * n:(j + 1) * n].astype(BF16)
            send_ref[j, base + n:base + PAIR * n] = gacc_ref[rows + j * n:rows + (j + 1) * n].astype(BF16)

    if has_sum:
        ring_sum.behind(b_id, pl.num_programs(0) - 1)


def kv_grad_kernel(*refs, stages):
    recv = refs[:stages]
    h0_ref, h1_ref, cos_ref, sin_ref, prev_ref, own_ref, par_ref, send_ref, shard_ref, gacc_ref = refs[stages:stages + 10]
    ring_sum = RingSum(prev_ref, [shard_ref], (1, 2), own_ref.shape[1] // stages, *refs[stages + 10:])
    ring_sum.ahead(pl.program_id(0))
    nb, tok, d = h0_ref.shape
    e2 = own_ref.shape[1] // stages
    e = e2 // 2
    side = cat_lanes([cos_ref[0], cos_ref[1]]), cat_lanes([sin_ref[0], sin_ref[1]])
    cos, sin = (cat_lanes([t] * nb) for t in side)
    parts = []
    for r in recv:
        total = r[:].astype(F32)
        parts.append(cat_rows([rope_rows(total[0:e], cos, sin, -1.0), total[e:PAIR * e]]).astype(BF16))
    gf = cat_rows(parts)
    for b in range(nb):
        own_ref[b] = gf[:, PAIR * b * tok:(PAIR * b + 1) * tok]
        par_ref[b] = gf[:, (PAIR * b + 1) * tok:(PAIR * b + 2) * tok]

    def weight_grads(first):
        step = 512
        for c in range(0, d, step):
            cs = slice(c, c + step)
            hh = cat_rows([r[b, :, cs] for b in range(nb) for r in (h0_ref, h1_ref)])
            if first:
                gacc_ref[:, cs] = dot(gf, hh)
            else:
                gacc_ref[:, cs] += dot(gf, hh)

    pl.when(pl.program_id(0) == 0)(lambda: weight_grads(True))
    pl.when(pl.program_id(0) > 0)(lambda: weight_grads(False))

    @pl.when(pl.program_id(0) == pl.num_programs(0) - 1)
    def _():
        n = send_ref.shape[1]
        for j in range(send_ref.shape[0]):
            send_ref[j] = gacc_ref[j * n:(j + 1) * n].astype(BF16)

    ring_sum.behind(pl.program_id(0), pl.num_programs(0) - 1)


def out_kernel(x_ref, w_ref, prev_ref, *refs, stages):
    core = lax.axis_index('core')
    o_refs, (y_ref, total_ref, lhs_ref) = refs[:PAIR * stages], refs[PAIR * stages:PAIR * stages + 3]
    ring_sum = RingSum(prev_ref, [total_ref], (1, 2), 0, *refs[PAIR * stages + 3:])
    ring_sum.ahead(pl.program_id(0))
    nb, tok, d = x_ref.shape
    rows = o_refs[0].shape[2]
    half = stages * rows
    for side in range(2):
        base = (core if side == 0 else 1 - core) * half
        for s in range(stages):
            for b in range(nb):
                lhs_ref[b * tok:(b + 1) * tok, pl.ds(pl.multiple_of(base + s * rows, rows), rows)] = o_refs[side * stages + s][0, b].T
    lhs = lhs_ref[:]
    step = 512
    for c in range(0, d, step):
        prod = dot(lhs, w_ref[:, c:c + step])
        y_ref[:, :, c:c + step] = (x_ref[:, :, c:c + step].astype(F32) + prod.reshape(nb, tok, step)).astype(BF16)

    ring_sum.behind(pl.program_id(0), pl.num_programs(0) - 1)


def norm_grad_kernel(x_ref, go_ref, g_ref, w_ref, kv0_ref, kv1_ref, prev_ref, *refs, stages):
    core = lax.axis_index('core')
    q_refs = refs[:PAIR * stages]
    gh_ref, gn_ref, total_ref, lhs_ref, tot_ref = refs[PAIR * stages:PAIR * stages + 5]
    ring_sum = RingSum(prev_ref, [total_ref], (1, 1), 0, *refs[PAIR * stages + 5:])
    ring_sum.ahead(pl.program_id(0))
    nb, tok, d = x_ref.shape
    rows = q_refs[0].shape[2]
    half = stages * rows
    e2 = kv0_ref.shape[1] // stages
    e = e2 // 2
    kv_half = stages * e
    for side in range(2):
        who = core if side == 0 else 1 - core
        kv_ref = kv0_ref if side == 0 else kv1_ref
        for b in range(nb):
            ts = slice(b * tok, (b + 1) * tok)
            for s in range(stages):
                lhs_ref[ts, pl.ds(pl.multiple_of(who * half + s * rows, rows), rows)] = q_refs[side * stages + s][0, b].T
            ks = cat_rows([kv_ref[b, i * e2:i * e2 + e] for i in range(stages)])
            vs = cat_rows([kv_ref[b, i * e2 + e:(i + 1) * e2] for i in range(stages)])
            base = PAIR * half
            lhs_ref[ts, pl.ds(pl.multiple_of(base + who * kv_half, kv_half), kv_half)] = ks.T
            base = base + PAIR * kv_half
            lhs_ref[ts, pl.ds(pl.multiple_of(base + who * kv_half, kv_half), kv_half)] = vs.T
    lhs = lhs_ref[:]
    step = 256
    for c in range(0, d, step):
        tot_ref[:, c:c + step] = dot(lhs, w_ref[c:c + step, :], NT)

    @pl.when(pl.program_id(0) == 0)
    def _():
        gn_ref[:] = jnp.zeros_like(gn_ref)

    g = g_ref[:].astype(F32)
    for b in range(nb):
        total = tot_ref[b * tok:(b + 1) * tok]
        x = x_ref[b].astype(F32)
        inv = lax.rsqrt(row_mean(x * x) + NORM_EPS)
        unit = x * inv
        gu = total * g
        mean_dot = row_mean(gu * unit)
        gh_ref[b] = (go_ref[b].astype(F32) + inv * (gu - unit * mean_dot)).astype(BF16)
        gn_ref[:] += jnp.sum((total * unit).reshape(tok // 8, 8, d), axis=0)

    ring_sum.behind(pl.program_id(0), pl.num_programs(0) - 1)


def transpose_to(out_ref, blk):
    for c in range(0, blk.shape[1], 256):
        out_ref[c:c + 256, :] = blk[:, c:c + 256].astype(F32).T


def assemble_main_kernel(*refs, stages, n_q):
    ins, (y_ref, gh_ref, wq_ref, wo_ref, y_out, gh_out) = refs[:stages], refs[stages:]
    y_out[:] = y_ref[:]
    gh_out[:] = gh_ref[:]
    for s in range(stages):
        @pl.when(pl.program_id(1) == s)
        def _(ref=ins[s]):
            chips, _, n, d = ref.shape
            transpose_to(wq_ref, ref[:, 0, 0:n_q].reshape(chips * n_q, d))
            wo_ref[:] = ref[:, 0, n_q:n].astype(F32)


def assemble_tail_kernel(in_ref, _, out_ref):
    chips, _, n, d = in_ref.shape
    transpose_to(out_ref, in_ref[:, 0].reshape(chips * n, d))


def solution(mesh):
    chips = mesh.shape['sp'] // CORES
    mesh2 = Mesh(mesh.devices.reshape(mesh.shape['dp'], chips, CORES), ('dp', 'x', 'core'))
    swap = [(i, CORES - 1 - i) for i in range(CORES)]

    def device_step(hidden, norm_w, w_qkv, w_out, long_factor, grad_out):
        n_batch, tok, d = hidden.shape
        n_heads, e = w_out.shape[0], w_out.shape[1]
        kv_heads = (w_qkv.shape[1] // e - n_heads) // 2
        reps = n_heads // kv_heads
        stages = kv_heads // CORES
        rows = reps * e
        q_half = stages * rows
        kv_half = stages * e
        e2 = PAIR * e
        half_rot = long_factor.shape[0]
        chip = lax.axis_index('x')
        core = lax.axis_index('core')
        ids = jnp.stack([chip, core]).astype(jnp.int32)
        tiles = 2
        nb = n_batch // tiles

        x_par = lax.ppermute(hidden, 'core', swap)
        go_par = lax.ppermute(grad_out, 'core', swap)
        w_o = w_out.reshape(n_heads * e, d)
        norm2 = norm_w.reshape(1, d)

        exponent = jnp.arange(half_rot, dtype=F32) / half_rot
        inv_freq = 1.0 / (long_factor * jnp.power(ROPE_BASE, exponent))
        sides = jnp.stack([core, 1 - core])
        positions = ((chip * CORES + sides)[:, None] * tok + jnp.arange(tok)[None, :]).astype(F32)
        angles = inv_freq[None, :, None] * positions[:, None, :]
        cos_t, sin_t = jnp.cos(angles) * ROPE_GAIN, jnp.sin(angles) * ROPE_GAIN

        tok_spec = along(0, nb, tok, d)
        rot_spec = whole(half_rot, tok)

        def kv_proj(x, side, filled):
            kb = PAIR * q_half // kv_half
            kt = 4
            kn = n_batch // kt
            x_spec = along(0, kn, tok, d)
            any_spec = pl.BlockSpec(memory_space=pl.ANY)
            return pl.pallas_call(
                drop_scalar(kv_proj_kernel),
                out_shape=[jax.ShapeDtypeStruct((n_batch, tok, d), BF16)]
                + [jax.ShapeDtypeStruct((2, n_batch, e2, tok), BF16)] * stages,
                grid_spec=pltpu.PrefetchScalarGridSpec(
                    num_scalar_prefetch=1, grid=(kt,),
                    in_specs=[x_spec, whole(1, d),
                              pl.BlockSpec((d, kv_half), lambda i, c: (0, kb + c[1])),
                              pl.BlockSpec((d, kv_half), lambda i, c: (0, kb + CORES + c[1])), rot_spec, rot_spec]
                    + [any_spec] * len(filled),
                    out_specs=[x_spec] + [pl.BlockSpec((1, kn, e2, tok), lambda i, _: (side, i, 0, 0))] * stages),
                input_output_aliases={7 + i: 1 + i for i in range(len(filled))},
                compiler_params=params(), name='kv_proj',
                cost_estimate=cost(PAIR * n_batch * tok * d * PAIR * kv_half, 3 * n_batch * tok * d * 2),
            )(ids, x, norm2, w_qkv, w_qkv, cos_t[side], sin_t[side], *filled)

        first = lambda i: jnp.minimum(i, tiles - 1)
        second = lambda i: jnp.maximum(i - tiles, 0)
        own_spec = pl.BlockSpec((nb, tok, d), lambda i, _: (first(i), 0, 0))
        par_spec = pl.BlockSpec((nb, tok, d), lambda i, _: (second(i), 0, 0))
        own_out = pl.BlockSpec((nb, q_half, tok), lambda i, _: (first(i), 0, 0))
        par_out = pl.BlockSpec((nb, q_half, tok), lambda i, _: (second(i), 0, 0))
        both_rot = whole(2, half_rot, tok)
        q_shapes = (jax.ShapeDtypeStruct((n_batch, q_half, tok), BF16), jax.ShapeDtypeStruct((n_batch, q_half, tok), BF16))

        def q_proj(h0, h1):
            return pl.pallas_call(
                drop_scalar(q_proj_kernel), out_shape=q_shapes,
                grid_spec=pltpu.PrefetchScalarGridSpec(
                    num_scalar_prefetch=1, grid=(PAIR * tiles,),
                    in_specs=[own_spec, par_spec, pl.BlockSpec((d, q_half), lambda i, c: (0, c[1])), both_rot, both_rot],
                    out_specs=(own_out, par_out)),
                compiler_params=params(), name='q_proj',
                cost_estimate=cost(4 * n_batch * tok * d * q_half, 6 * n_batch * tok * d * 2),
            )(ids, h0, h1, w_qkv, cos_t, sin_t)

        def do_proj(g0, g1):
            return pl.pallas_call(
                drop_scalar(do_proj_kernel), out_shape=q_shapes,
                grid_spec=pltpu.PrefetchScalarGridSpec(
                    num_scalar_prefetch=1, grid=(PAIR * tiles,),
                    in_specs=[own_spec, par_spec, pl.BlockSpec((q_half, d), lambda i, c: (c[1], 0))],
                    out_specs=(own_out, par_out)),
                compiler_params=params(), name='do_proj',
                cost_estimate=cost(4 * n_batch * tok * d * q_half, 6 * n_batch * tok * d * 2),
            )(ids, g0, g1, w_o)

        h_own, *kv_sides = kv_proj(hidden, 0, [])
        h_par, *kv_sides = kv_proj(x_par, 1, kv_sides)
        gathered = []
        for s in range(stages):
            gathered.append(lax.all_gather(kv_sides[s], 'x'))
        q_own, q_par = q_proj(h_own, h_par)
        do_own, do_par = do_proj(grad_out, go_par)

        n_g = PAIR * rows // chips
        n_s = e2 + n_g
        hbm = pl.BlockSpec(memory_space=pl.ANY)
        shard_spec = lambda n: whole(n, d)

        def gather_shard(shard):
            return lax.all_gather(shard, ('x', 'core')).reshape(chips, CORES, *shard.shape)

        def attention(s, prev):
            blk = PAIR * tok
            has_sum = prev is not None
            q_spec = pl.BlockSpec((1, rows, tok), lambda b: (b, s, 0))
            t_spec = pl.BlockSpec((2, tok, d), lambda b: (b // 2, 0, 0))
            r_spec = whole(2, half_rot, tok)
            o_spec = along(1, 2, 1, rows, tok)
            return pl.pallas_call(
                functools.partial(attn_kernel, has_sum=has_sum),
                out_shape=[jax.ShapeDtypeStruct((2, n_batch, rows, tok), BF16)] * 2
                + [jax.ShapeDtypeStruct((chips, n_s, d), BF16)]
                + [jax.ShapeDtypeStruct((n, d), BF16) for n in (e2, n_g)] * has_sum,
                grid=(n_batch,),
                in_specs=[q_spec, q_spec, q_spec, q_spec, along(2, chips, 2, 1, e2, tok),
                          t_spec, t_spec, t_spec, t_spec, r_spec, r_spec]
                + [hbm] * has_sum,
                out_specs=[o_spec, o_spec, whole(chips, n_s, d)]
                + [shard_spec(e2), shard_spec(n_g)] * has_sum,
                scratch_shapes=[pltpu.VMEM((chips, blk, reps * blk), F32), pltpu.VMEM((chips, blk, reps * blk), BF16),
                                pltpu.VMEM((chips, blk, reps * blk), BF16), pltpu.VMEM((e, reps * blk), F32),
                                pltpu.VMEM((8, reps * blk), F32),
                                pltpu.VMEM((chips, blk, e2), BF16), pltpu.VMEM((2, PAIR * rows, blk), BF16),
                                pltpu.VMEM((PAIR * rows, d), F32)]
                + RingSum.scratch(n_s, d) * has_sum,
                compiler_params=comm_params(s) if has_sum else params(),
                cost_estimate=cost(4e10, 3e7, 3e7),
            )(q_own, q_par, do_own, do_par, gathered[s], h_own, h_par, grad_out, go_par, cos_t, sin_t,
              *([prev] * has_sum))

        own, par, totals, main = [], [], [], []
        prev = None
        for s in range(stages):
            own_s, par_s, send, *sums = attention(s, prev)
            own.append(own_s)
            par.append(lax.ppermute(par_s, 'core', swap))
            prev = send
            totals += sums[:1]
            main += [gather_shard(g) for g in sums[1:]]

        nb2 = 2
        t2_spec = along(0, nb2, tok, d)
        block_out, total = pl.pallas_call(
            functools.partial(out_kernel, stages=stages),
            out_shape=[jax.ShapeDtypeStruct((n_batch, tok, d), BF16), jax.ShapeDtypeStruct((e2, d), BF16)],
            grid=(n_batch // nb2,),
            in_specs=[t2_spec, whole(n_heads * e, d), hbm]
            + [along(1, 1, nb2, rows, tok)] * (PAIR * stages),
            out_specs=[t2_spec, shard_spec(e2)],
            scratch_shapes=[pltpu.VMEM((nb2 * tok, n_heads * e), BF16)] + RingSum.scratch(e2, d),
            compiler_params=comm_params(stages), name='out_proj',
            cost_estimate=cost(PAIR * n_batch * tok * d * n_heads * e, 3e7),
        )(hidden, w_o, prev, *own, *par)
        totals.append(total)

        gb = 2
        gf_spec = along(0, gb, stages * e2, tok)
        n_kv = stages * e2 // chips
        kv_own_g, kv_par_g, send_kv, shard = pl.pallas_call(
            functools.partial(kv_grad_kernel, stages=stages),
            out_shape=[jax.ShapeDtypeStruct((n_batch, stages * e2, tok), BF16)] * 2
            + [jax.ShapeDtypeStruct((chips, n_kv, d), BF16), jax.ShapeDtypeStruct((n_g, d), BF16)],
            grid=(n_batch // gb,),
            in_specs=[along(1, e2, PAIR * tok * gb)] * stages
            + [along(0, gb, tok, d)] * 2 + [whole(2, half_rot, tok)] * 2
            + [hbm],
            out_specs=[gf_spec, gf_spec, whole(chips, n_kv, d), shard_spec(n_g)],
            scratch_shapes=[pltpu.VMEM((stages * e2, d), F32)] + RingSum.scratch(n_g, d),
            compiler_params=comm_params(stages + 1), name='kv_grad',
            cost_estimate=cost(PAIR * PAIR * n_batch * tok * d * stages * e2, 3e7),
        )(*totals, h_own, h_par, cos_t, sin_t, prev)
        main.append(gather_shard(shard))
        kv_other_g = lax.ppermute(kv_par_g, 'core', swap)

        nb3 = 2
        t3_spec = along(0, nb3, tok, d)
        grad_hidden, gn, shard_kv = pl.pallas_call(
            functools.partial(norm_grad_kernel, stages=stages),
            out_shape=[jax.ShapeDtypeStruct((n_batch, tok, d), BF16), jax.ShapeDtypeStruct((8, d), F32),
                       jax.ShapeDtypeStruct((n_kv, d), BF16)],
            grid=(n_batch // nb3,),
            in_specs=[t3_spec, t3_spec, whole(1, d), whole(*w_qkv.shape)]
            + [along(0, nb3, stages * e2, tok)] * 2 + [hbm]
            + [pl.BlockSpec((1, nb3, rows, tok), lambda b: (1, b, 0, 0))] * (PAIR * stages),
            out_specs=[t3_spec, whole(8, d), shard_spec(n_kv)],
            scratch_shapes=[pltpu.VMEM((nb3 * tok, w_qkv.shape[1]), BF16), pltpu.VMEM((nb3 * tok, d), F32)]
            + RingSum.scratch(n_kv, d),
            compiler_params=comm_params(stages + 2), name='norm_grad',
            cost_estimate=cost(PAIR * n_batch * tok * d * w_qkv.shape[1], 4e7),
        )(hidden, grad_out, norm2, w_qkv, kv_own_g, kv_other_g, send_kv, *own, *par)

        gn_row = jnp.sum(gn, axis=0, keepdims=True)
        gn_hi = gn_row.astype(BF16)
        gn_lo = (gn_row - gn_hi.astype(F32)).astype(BF16)
        n_t = n_kv + 16
        tail_block = cat_rows([shard_kv, gn_hi, gn_lo, jnp.zeros((n_t - n_kv - 2, d), BF16)])
        tail = gather_shard(tail_block)
        n_q = rows // chips
        b_spec = pl.BlockSpec((n_batch // (CORES * stages), tok, d), lambda p, s: (p * stages + s, 0, 0))
        w_cols, grad_w_out, block_out, grad_hidden = pl.pallas_call(
            functools.partial(assemble_main_kernel, stages=stages, n_q=n_q),
            out_shape=[jax.ShapeDtypeStruct(w_qkv.shape, F32), jax.ShapeDtypeStruct((n_heads, e, d), F32)]
            + [jax.ShapeDtypeStruct((n_batch, tok, d), BF16)] * PAIR,
            grid=(CORES, stages),
            in_specs=[along(1, chips, 1, n_g, d)] * stages + [b_spec] * PAIR,
            out_specs=[pl.BlockSpec((d, rows), lambda p, s: (0, p * stages + s)),
                       pl.BlockSpec((reps, e, d), lambda p, s: (p * stages + s, 0, 0)), b_spec, b_spec],
            compiler_params=params(2), name='assemble_main', cost_estimate=cost(2e9, 6e7),
        )(*main, block_out, grad_hidden)
        kcol = PAIR * q_half // kv_half
        grad_w_qkv = pl.pallas_call(
            assemble_tail_kernel,
            out_shape=jax.ShapeDtypeStruct(w_qkv.shape, F32),
            grid=(CORES, 2),
            in_specs=[pl.BlockSpec((chips, 1, e, d), lambda p, k: (0, p, k, 0)), pl.BlockSpec(memory_space=pl.ANY)],
            out_specs=pl.BlockSpec((d, kv_half), lambda p, k: (0, kcol + k * CORES + p)),
            input_output_aliases={1: 0},
            compiler_params=params(2), name='assemble_tail', cost_estimate=cost(1e9, 2e7),
        )(tail, w_cols)
        gn_all = tail[:, :, n_kv:n_kv + 2].astype(F32)
        grad_norm_w = jnp.sum(gn_all, axis=(0, 1, 2))
        return block_out, grad_hidden, grad_w_qkv, grad_w_out, grad_norm_w

    tok_spec = P('dp', ('x', 'core'), None)
    return jax.shard_map(device_step, mesh=mesh2,
                         in_specs=(tok_spec, P(), P(), P(), P(), tok_spec),
                         out_specs=(tok_spec, tok_spec, P('dp', None), P('dp', None, None), P('dp')),
                         check_vma=False)
```

```python
import functools
import math

import jax
import jax.numpy as jnp
from jax import lax
from jax.experimental import pallas as pl
from jax.experimental.pallas import tpu as pltpu
from jax.sharding import Mesh, PartitionSpec as P


NORM_EPS = 1e-5
ROPE_BASE = 10000.0
ROPE_GAIN = math.sqrt(1.0 + math.log(32.0) / math.log(4096.0))
MASK_VALUE = -1e30
LOG2E = math.log2(math.e)
CORES = 2
PAIR = 2
BF16 = jnp.bfloat16
F32 = jnp.float32
VMEM_LIMIT = 60 * 1024 * 1024

NN = (((1,), (0,)), ((), ()))
NT = (((1,), (1,)), ((), ()))


cat_rows = functools.partial(jnp.concatenate, axis=0)
cat_lanes = functools.partial(jnp.concatenate, axis=1)
column_max = functools.partial(jnp.max, axis=0, keepdims=True)
column_sum = functools.partial(jnp.sum, axis=0, keepdims=True)
row_mean = functools.partial(jnp.mean, axis=-1, keepdims=True)


def whole(*shape):
    return pl.BlockSpec(shape, lambda *_: (0,) * len(shape))


def along(axis, *shape):
    return pl.BlockSpec(shape, lambda i, *_: tuple(i if n == axis else 0 for n in range(len(shape))))


def dot(a, b, dims=NN):
    return lax.dot_general(a, b, dims, preferred_element_type=F32)


def cost(flops, nbytes, trans=0):
    return pl.CostEstimate(flops=int(flops), bytes_accessed=int(nbytes), transcendentals=int(trans))


def params(n_axes=1):
    return pltpu.CompilerParams(dimension_semantics=("arbitrary",) * n_axes, vmem_limit_bytes=VMEM_LIMIT)


def rope_rows(block, cos, sin, direction):
    half = cos.shape[0]
    a, b = block[:half], block[half:PAIR * half]
    s = sin * direction
    return cat_rows([a * cos - b * s, b * cos + a * s])


def kv_proj_kernel(x_ref, g_ref, wk_ref, wv_ref, cos_ref, sin_ref, *refs):
    nb, tok, d = x_ref.shape
    stages = (wk_ref.shape[1] // (PAIR * cos_ref.shape[0]))
    h_ref, first_ref, rest_ref = refs[-3:]
    kv_refs = [first_ref] + [rest_ref.at[i] for i in range(stages - 1)]
    e2 = first_ref.shape[2]
    e = e2 // 2
    x = x_ref[:].reshape(nb * tok, d).astype(F32)
    inv = lax.rsqrt(row_mean(x * x) + NORM_EPS)
    h = (x * inv * g_ref[:].astype(F32)).astype(BF16)
    h_ref[:] = h.reshape(nb, tok, d)
    cos, sin = cos_ref[:], sin_ref[:]
    k = dot(h, wk_ref[:]).T
    v = dot(h, wv_ref[:]).T
    for i in range(stages):
        for b in range(nb):
            kv_refs[i][0, b, 0:e] = rope_rows(k[i * e:(i + 1) * e, b * tok:(b + 1) * tok], cos, sin, 1.0).astype(BF16)
            kv_refs[i][0, b, e:PAIR * e] = v[i * e:(i + 1) * e, b * tok:(b + 1) * tok].astype(BF16)


def q_proj_kernel(h0_ref, h1_ref, w_ref, cos_ref, sin_ref, q0_ref, q1_ref):
    nb, tok, d = h0_ref.shape
    e = PAIR * cos_ref.shape[1]
    rows = w_ref.shape[1]
    scale = e ** -0.5
    step = 4 * e

    def run(h_ref, q_ref, side):
        h = h_ref[:].reshape(nb * tok, d)
        cos, sin = cos_ref[side], sin_ref[side]
        for r in range(0, rows, step):
            blk = dot(h, w_ref[:, r:r + step]).T
            for i in range(0, step, e):
                for b in range(nb):
                    q_ref[b, r + i:r + i + e] = (rope_rows(blk[i:i + e, b * tok:(b + 1) * tok], cos, sin, 1.0).astype(BF16)
                                                 * scale).astype(BF16)

    half = pl.num_programs(0) // 2
    pl.when(pl.program_id(0) < half)(lambda: run(h0_ref, q0_ref, 0))
    pl.when(pl.program_id(0) >= half)(lambda: run(h1_ref, q1_ref, 1))


def do_proj_kernel(g0_ref, g1_ref, w_ref, o0_ref, o1_ref):
    nb, tok, d = g0_ref.shape
    rows = w_ref.shape[0]
    step = 512

    def run(g_ref, o_ref):
        g = g_ref[:].reshape(nb * tok, d)
        for r in range(0, rows, step):
            blk = dot(w_ref[r:r + step], g, NT)
            for b in range(nb):
                o_ref[b, r:r + step] = blk[:, b * tok:(b + 1) * tok].astype(BF16)

    half = pl.num_programs(0) // 2
    pl.when(pl.program_id(0) < half)(lambda: run(g0_ref, o0_ref))
    pl.when(pl.program_id(0) >= half)(lambda: run(g1_ref, o1_ref))


def drop_scalar(kernel):
    def wrapped(_, *refs):
        kernel(*refs)

    return wrapped


def ring_peers(chips):
    chip, core = lax.axis_index('x'), lax.axis_index('core')
    return chip, lax.rem(chip + 1, chips), lax.rem(chip + chips - 1, chips), lax.rem(chip + 2, chips), core, 1 - core


def ring_barrier(chips):
    _, right, left, _, _, _ = ring_peers(chips)
    sem = pltpu.get_barrier_semaphore()
    for who in (right, left):
        pl.semaphore_signal(sem, inc=1, device_id={'x': who}, device_id_type=pl.DeviceIdType.MESH)
    pl.semaphore_wait(sem, 2)


class RingSum:
    @staticmethod
    def scratch(rows, d):
        half = rows // 2
        return [pltpu.VMEM((PAIR, half, d), BF16), pltpu.VMEM((PAIR, half, d), BF16), pltpu.VMEM((rows, d), BF16),
                pltpu.VMEM((PAIR, rows, d), BF16), pltpu.SemaphoreType.DMA((6,)), pltpu.SemaphoreType.DMA((6,)),
                pltpu.SemaphoreType.DMA((3,))]

    def __init__(self, send_ref, totals, plan, base, mid, buf, own, recv, s_sem, r_sem, l_sem):
        self.chips = chips = send_ref.shape[0]
        rows = own.shape[0]
        half = rows // 2
        chip, right, left, far, _, _ = ring_peers(chips)
        top, low = pl.ds(0, half), pl.ds(half, half)
        from_top, from_low = pl.ds(base, half), pl.ds(base + half, half)

        def remote(n, src, dst, who):
            return pltpu.make_async_remote_copy(src_ref=src, dst_ref=dst, send_sem=s_sem.at[n], recv_sem=r_sem.at[n],
                                                device_id={'x': who}, device_id_type=pl.DeviceIdType.MESH)

        self.far = [remote(0, send_ref.at[far, from_top], mid.at[0], right),
                    remote(1, send_ref.at[far, from_low], mid.at[1], left)]
        self.direct = [remote(2, send_ref.at[left, from_top], recv.at[1, top], left),
                       remote(3, send_ref.at[right, from_low], recv.at[0, low], right)]
        self.second = [remote(4, buf.at[0], recv.at[0, top], right), remote(5, buf.at[1], recv.at[1, low], left)]
        self.local = [pltpu.make_async_copy(send_ref.at[right, from_top], buf.at[0], l_sem.at[0]),
                      pltpu.make_async_copy(send_ref.at[left, from_low], buf.at[1], l_sem.at[1]),
                      pltpu.make_async_copy(send_ref.at[chip, pl.ds(base, rows)], own, l_sem.at[2])]
        self.mid, self.buf, self.own, self.recv, self.totals = mid, buf, own, recv, totals
        self.plan = plan

    def start(self):
        ring_barrier(self.chips)
        for c in self.far + self.local:
            c.start()

    def start_direct(self):
        for c in self.direct:
            c.start()

    def merge(self):
        for far, local, buf, mid in zip(self.far, self.local, (self.buf.at[0], self.buf.at[1]), (self.mid.at[0], self.mid.at[1])):
            local.wait()
            far.wait_recv()
            buf[:] = (buf[:].astype(F32) + mid[:].astype(F32)).astype(BF16)

    def send(self):
        for c in self.second:
            c.start()

    def finish(self):
        self.local[-1].wait()
        for c in self.direct + self.second:
            c.wait_recv()
        row = 0
        for ref in self.totals:
            r = slice(row, row + ref.shape[0])
            ref[:] = (self.own[r].astype(F32) + self.recv[0, r].astype(F32) + self.recv[1, r].astype(F32)).astype(BF16)
            row += ref.shape[0]
        for c in self.far + self.direct + self.second:
            c.wait_send()

    def ahead(self, step):
        direct, merge = self.plan
        run_at(step, 0, self.start)
        run_at(step, direct, self.start_direct)
        run_at(step, merge + 1, self.send)

    def behind(self, step, final):
        run_at(step, self.plan[1], self.merge)
        run_at(step, final, self.finish)


def run_at(step, n, *actions):
    @pl.when(step == n)
    def _():
        for a in actions:
            a()


def comm_params(cid, n_axes=1):
    return pltpu.CompilerParams(dimension_semantics=("arbitrary",) * n_axes, vmem_limit_bytes=VMEM_LIMIT,
                                collective_id=cid, has_side_effects=True)


def attn_kernel(q0_ref, q1_ref, do0_ref, do1_ref, kv_ref, h0_ref, h1_ref, g0_ref, g1_ref, cos_ref, sin_ref, *refs,
                has_sum):
    refs = list(refs)
    prev_ref = refs.pop(0) if has_sum else None
    own_ref, par_ref, send_ref = refs[:3]
    refs = refs[3:]
    totals = [refs.pop(0), refs.pop(0)] if has_sum else []
    s_ref, p_ref, ds_ref, acc_ref, ml_ref, kvt_ref, lhs_ref, gacc_ref = refs[:8]
    chip, core = lax.axis_index('x'), lax.axis_index('core')
    b_id = pl.program_id(0)
    if has_sum:
        ring_sum = RingSum(prev_ref, totals, (2, 3), 0, *refs[8:])
        ring_sum.ahead(b_id)
    chips = kv_ref.shape[0]
    rows, tok = q0_ref.shape[1], q0_ref.shape[2]
    e = kv_ref.shape[3] // 2
    reps = rows // e
    blk = PAIR * tok

    def heads_to_lanes(first_ref, second_ref):
        full = cat_lanes([first_ref[0], second_ref[0]])
        return cat_lanes([full[i * e:(i + 1) * e] for i in range(reps)])

    head_cols = [slice(i * blk, (i + 1) * blk) for i in range(reps)]

    def kv_block(i):
        return cat_lanes([kv_ref[chip - i, 0, 0], kv_ref[chip - i, 1, 0]])

    def scores(i):
        qt = heads_to_lanes(q0_ref, q1_ref)
        q_pad = cat_rows([qt, jnp.zeros_like(qt)])
        kvt = kv_block(i).T
        kvt_ref[i] = kvt
        tops = []
        for cols in head_cols:
            t = dot(kvt, q_pad[:, cols])
            if i == 0:
                r = lax.broadcasted_iota(jnp.int32, (blk, blk), 0)
                c = lax.broadcasted_iota(jnp.int32, (blk, blk), 1)
                shift = (1 - PAIR * core) * tok
                k_pos = jnp.where(r < tok, r, r - tok + shift)
                q_pos = jnp.where(c < tok, c, c - tok + shift)
                t = jnp.where(k_pos <= q_pos, t, MASK_VALUE)
            s_ref[i, :, cols] = t
            tops.append(column_max(t))
        return cat_lanes(tops) * LOG2E

    def accumulate(i, m):
        v_t = kv_block(i)[e:PAIR * e]
        sums, outs = [], []
        for cols in head_cols:
            p = jnp.exp2(s_ref[i, :, cols] * LOG2E - m[:, cols])
            sums.append(column_sum(p))
            outs.append(dot(v_t, p.astype(BF16)))
        return cat_lanes(sums), cat_lanes(outs)

    ml_ref[0:1] = scores(0)
    ml_ref[1:2] = jnp.zeros_like(ml_ref[1:2])
    acc_ref[:] = jnp.zeros_like(acc_ref)

    for i in range(1, chips):
        @pl.when(i <= chip)
        def _(i=i):
            m = ml_ref[0:1]
            add_l, add_o = accumulate(i - 1, m)
            m_new = jnp.maximum(m, scores(i))
            alpha = jnp.exp2(m - m_new)
            acc_ref[:] = (acc_ref[:] + add_o) * alpha
            ml_ref[1:2] = (ml_ref[1:2] + add_l) * alpha
            ml_ref[0:1] = m_new

    m = ml_ref[0:1]
    add_l, add_o = accumulate(chip, m)
    l = ml_ref[1:2] + add_l
    o_t = (acc_ref[:] + add_o) * (1.0 / l)
    dot_t = heads_to_lanes(do0_ref, do1_ref)
    ml_ref[1:2] = column_sum(o_t * dot_t.astype(F32))
    ml_ref[0:1] = m + jnp.log2(l)
    o_b = o_t.astype(BF16)
    o_full = cat_rows([o_b[:, cols] for cols in head_cols])
    odd = lax.rem(b_id, 2)
    lhs_ref[odd, rows:PAIR * rows] = o_full
    own_ref[0, 0] = o_full[:, :tok]
    par_ref[0, 0] = o_full[:, tok:]
    acc_ref[:] = jnp.zeros_like(acc_ref)

    def score_grads(i):
        dot_t = heads_to_lanes(do0_ref, do1_ref)
        do_pad = cat_rows([jnp.zeros_like(dot_t), dot_t])
        kvt = kvt_ref[i]
        for cols in head_cols:
            p = jnp.exp2(s_ref[i, :, cols] * LOG2E - ml_ref[0:1, cols])
            dp = dot(kvt, do_pad[:, cols])
            p_ref[i, :, cols] = p.astype(BF16)
            ds_ref[i, :, cols] = (p * (dp - ml_ref[1:2, cols])).astype(BF16)

    def input_grads(i):
        qt = heads_to_lanes(q0_ref, q1_ref)
        dot_t = heads_to_lanes(do0_ref, do1_ref)
        k_t = kv_block(i)[0:e]
        dv = dot(dot_t, p_ref[i], NT)
        dk = dot(qt, ds_ref[i], NT)
        send_ref[chip - i, 0:PAIR * e, pl.ds(pl.multiple_of(b_id * blk, blk), blk)] = cat_rows([dk, dv]).astype(BF16)
        acc_ref[:] += dot(k_t, ds_ref[i])

    score_grads(0)
    for i in range(1, chips):
        @pl.when(i <= chip)
        def _(i=i):
            input_grads(i - 1)
            score_grads(i)

    input_grads(chip)

    def zero_step(j, carry):
        send_ref[j, 0:PAIR * e, pl.ds(pl.multiple_of(b_id * blk, blk), blk)] = jnp.zeros((PAIR * e, blk), BF16)
        return carry

    lax.fori_loop(chip + 1, chips, zero_step, 0)

    cos = cat_lanes([cos_ref[0], cos_ref[1]])
    sin = cat_lanes([sin_ref[0], sin_ref[1]])
    dq_rows = []
    for cols in head_cols:
        dq = (acc_ref[:, cols] * (e ** -0.5)).astype(BF16).astype(F32)
        dq_rows.append(rope_rows(dq, cos, sin, -1.0).astype(BF16))
    dq_full = cat_rows(dq_rows)
    own_ref[1, 0] = dq_full[:, :tok]
    par_ref[1, 0] = dq_full[:, tok:]

    d = h0_ref.shape[2]
    step = 512
    lhs_ref[odd, 0:rows] = dq_full

    def weight_grads(first):
        for c in range(0, d, step):
            cs = slice(c, c + step)
            for r, (a_ref, b_ref) in enumerate(((h0_ref, h1_ref), (g0_ref, g1_ref))):
                rs = slice(r * rows, (r + 1) * rows)
                lhs = cat_lanes([lhs_ref[0, rs], lhs_ref[1, rs]])
                rhs = cat_rows([a_ref[0, :, cs], b_ref[0, :, cs], a_ref[1, :, cs], b_ref[1, :, cs]])
                if first:
                    gacc_ref[rs, cs] = dot(lhs, rhs)
                else:
                    gacc_ref[rs, cs] += dot(lhs, rhs)

    pl.when(b_id == 1)(lambda: weight_grads(True))
    pl.when((odd == 1) & (b_id > 1))(lambda: weight_grads(False))

    @pl.when(b_id == pl.num_programs(0) - 1)
    def _():
        for j in range(chips):
            n = rows // chips
            base = PAIR * e
            send_ref[j, base:base + n] = gacc_ref[j * n:(j + 1) * n].astype(BF16)
            send_ref[j, base + n:base + PAIR * n] = gacc_ref[rows + j * n:rows + (j + 1) * n].astype(BF16)

    if has_sum:
        ring_sum.behind(b_id, pl.num_programs(0) - 1)


def kv_grad_kernel(*refs, stages):
    recv = refs[:stages]
    h0_ref, h1_ref, cos_ref, sin_ref, prev_ref, own_ref, par_ref, send_ref, shard_ref, gacc_ref = refs[stages:stages + 10]
    ring_sum = RingSum(prev_ref, [shard_ref], (1, 2), own_ref.shape[1] // stages, *refs[stages + 10:])
    ring_sum.ahead(pl.program_id(0))
    nb, tok, d = h0_ref.shape
    e2 = own_ref.shape[1] // stages
    e = e2 // 2
    side = cat_lanes([cos_ref[0], cos_ref[1]]), cat_lanes([sin_ref[0], sin_ref[1]])
    cos, sin = (cat_lanes([t] * nb) for t in side)
    parts = []
    for r in recv:
        total = r[:].astype(F32)
        parts.append(cat_rows([rope_rows(total[0:e], cos, sin, -1.0), total[e:PAIR * e]]).astype(BF16))
    gf = cat_rows(parts)
    for b in range(nb):
        own_ref[b] = gf[:, PAIR * b * tok:(PAIR * b + 1) * tok]
        par_ref[b] = gf[:, (PAIR * b + 1) * tok:(PAIR * b + 2) * tok]

    def weight_grads(first):
        step = 512
        for c in range(0, d, step):
            cs = slice(c, c + step)
            hh = cat_rows([r[b, :, cs] for b in range(nb) for r in (h0_ref, h1_ref)])
            if first:
                gacc_ref[:, cs] = dot(gf, hh)
            else:
                gacc_ref[:, cs] += dot(gf, hh)

    pl.when(pl.program_id(0) == 0)(lambda: weight_grads(True))
    pl.when(pl.program_id(0) > 0)(lambda: weight_grads(False))

    @pl.when(pl.program_id(0) == pl.num_programs(0) - 1)
    def _():
        n = send_ref.shape[1]
        for j in range(send_ref.shape[0]):
            send_ref[j] = gacc_ref[j * n:(j + 1) * n].astype(BF16)

    ring_sum.behind(pl.program_id(0), pl.num_programs(0) - 1)


def out_kernel(x_ref, w_ref, prev_ref, *refs, stages):
    core = lax.axis_index('core')
    o_refs, (y_ref, total_ref, lhs_ref) = refs[:PAIR * stages], refs[PAIR * stages:PAIR * stages + 3]
    ring_sum = RingSum(prev_ref, [total_ref], (1, 2), 0, *refs[PAIR * stages + 3:])
    ring_sum.ahead(pl.program_id(0))
    nb, tok, d = x_ref.shape
    rows = o_refs[0].shape[2]
    half = stages * rows
    for side in range(2):
        base = (core if side == 0 else 1 - core) * half
        for s in range(stages):
            for b in range(nb):
                lhs_ref[b * tok:(b + 1) * tok, pl.ds(pl.multiple_of(base + s * rows, rows), rows)] = o_refs[side * stages + s][0, b].T
    lhs = lhs_ref[:]
    step = 512
    for c in range(0, d, step):
        prod = dot(lhs, w_ref[:, c:c + step])
        y_ref[:, :, c:c + step] = (x_ref[:, :, c:c + step].astype(F32) + prod.reshape(nb, tok, step)).astype(BF16)

    ring_sum.behind(pl.program_id(0), pl.num_programs(0) - 1)


def norm_grad_kernel(x_ref, go_ref, g_ref, w_ref, kv0_ref, kv1_ref, prev_ref, *refs, stages):
    core = lax.axis_index('core')
    q_refs = refs[:PAIR * stages]
    gh_ref, tail_ref, lhs_ref, tot_ref, gn_ref = refs[PAIR * stages:PAIR * stages + 5]
    n_kv = prev_ref.shape[1]
    ring_sum = RingSum(prev_ref, [tail_ref.at[pl.ds(0, n_kv)]], (1, 1), 0, *refs[PAIR * stages + 5:])
    ring_sum.ahead(pl.program_id(0))
    nb, tok, d = x_ref.shape
    rows = q_refs[0].shape[2]
    half = stages * rows
    e2 = kv0_ref.shape[1] // stages
    e = e2 // 2
    kv_half = stages * e
    for side in range(2):
        who = core if side == 0 else 1 - core
        kv_ref = kv0_ref if side == 0 else kv1_ref
        for b in range(nb):
            ts = slice(b * tok, (b + 1) * tok)
            for s in range(stages):
                lhs_ref[ts, pl.ds(pl.multiple_of(who * half + s * rows, rows), rows)] = q_refs[side * stages + s][0, b].T
            ks = cat_rows([kv_ref[b, i * e2:i * e2 + e] for i in range(stages)])
            vs = cat_rows([kv_ref[b, i * e2 + e:(i + 1) * e2] for i in range(stages)])
            base = PAIR * half
            lhs_ref[ts, pl.ds(pl.multiple_of(base + who * kv_half, kv_half), kv_half)] = ks.T
            base = base + PAIR * kv_half
            lhs_ref[ts, pl.ds(pl.multiple_of(base + who * kv_half, kv_half), kv_half)] = vs.T
    lhs = lhs_ref[:]
    step = 256
    for c in range(0, d, step):
        tot_ref[:, c:c + step] = dot(lhs, w_ref[c:c + step, :], NT)

    @pl.when(pl.program_id(0) == 0)
    def _():
        gn_ref[:] = jnp.zeros_like(gn_ref)

    g = g_ref[:].astype(F32)
    for b in range(nb):
        total = tot_ref[b * tok:(b + 1) * tok]
        x = x_ref[b].astype(F32)
        inv = lax.rsqrt(row_mean(x * x) + NORM_EPS)
        unit = x * inv
        gu = total * g
        mean_dot = row_mean(gu * unit)
        gh_ref[b] = (go_ref[b].astype(F32) + inv * (gu - unit * mean_dot)).astype(BF16)
        gn_ref[:] += jnp.sum((total * unit).reshape(tok // 8, 8, d), axis=0)

    @pl.when(pl.program_id(0) == pl.num_programs(0) - 1)
    def _():
        extra = tail_ref.shape[0] - n_kv
        total = column_sum(gn_ref[:])
        high = total.astype(BF16).astype(F32)
        row = lax.broadcasted_iota(jnp.int32, (extra, d), 0)
        tail_ref[n_kv:] = jnp.where(row == 0, high, jnp.where(row == 1, total - high, 0.0)).astype(BF16)

    ring_sum.behind(pl.program_id(0), pl.num_programs(0) - 1)


def transpose_to(out_ref, blk):
    for c in range(0, blk.shape[1], 256):
        out_ref[c:c + 256, :] = blk[:, c:c + 256].astype(F32).T


def assemble_main_kernel(*refs, stages, n_q):
    ins, (y_ref, gh_ref, wq_ref, wo_ref, y_out, gh_out) = refs[:stages], refs[stages:]
    y_out[:] = y_ref[:]
    gh_out[:] = gh_ref[:]
    for s in range(stages):
        @pl.when(pl.program_id(1) == s)
        def _(ref=ins[s]):
            chips, _, n, d = ref.shape
            transpose_to(wq_ref, ref[:, 0, 0:n_q].reshape(chips * n_q, d))
            wo_ref[:] = ref[:, 0, n_q:n].astype(F32)


def assemble_tail_kernel(in_ref, gn_ref, _, out_ref, norm_ref):
    norm_ref[:] = jnp.sum(gn_ref[:].astype(F32), axis=(0, 1, 2)).reshape(norm_ref.shape)
    chips, _, n, d = in_ref.shape
    transpose_to(out_ref, in_ref[:, 0].reshape(chips * n, d))


def solution(mesh):
    chips = mesh.shape['sp'] // CORES
    mesh2 = Mesh(mesh.devices.reshape(mesh.shape['dp'], chips, CORES), ('dp', 'x', 'core'))
    swap = [(i, CORES - 1 - i) for i in range(CORES)]

    def device_step(hidden, norm_w, w_qkv, w_out, long_factor, grad_out):
        n_batch, tok, d = hidden.shape
        n_heads, e = w_out.shape[0], w_out.shape[1]
        kv_heads = (w_qkv.shape[1] // e - n_heads) // 2
        reps = n_heads // kv_heads
        stages = kv_heads // CORES
        rows = reps * e
        q_half = stages * rows
        kv_half = stages * e
        e2 = PAIR * e
        half_rot = long_factor.shape[0]
        chip = lax.axis_index('x')
        core = lax.axis_index('core')
        ids = jnp.stack([chip, core]).astype(jnp.int32)
        tiles = 2
        nb = n_batch // tiles

        x_par = lax.ppermute(hidden, 'core', swap)
        go_par = lax.ppermute(grad_out, 'core', swap)
        w_o = w_out.reshape(n_heads * e, d)
        norm2 = norm_w.reshape(1, d)

        exponent = jnp.arange(half_rot, dtype=F32) / half_rot
        inv_freq = 1.0 / (long_factor * jnp.power(ROPE_BASE, exponent))
        sides = jnp.stack([core, 1 - core])
        positions = ((chip * CORES + sides)[:, None] * tok + jnp.arange(tok)[None, :]).astype(F32)
        angles = inv_freq[None, :, None] * positions[:, None, :]
        cos_t, sin_t = jnp.cos(angles) * ROPE_GAIN, jnp.sin(angles) * ROPE_GAIN

        tok_spec = along(0, nb, tok, d)
        rot_spec = whole(half_rot, tok)

        def kv_proj(x, side, filled):
            kb = PAIR * q_half // kv_half
            kt = 4
            kn = n_batch // kt
            x_spec = along(0, kn, tok, d)
            any_spec = pl.BlockSpec(memory_space=pl.ANY)
            return pl.pallas_call(
                drop_scalar(kv_proj_kernel),
                out_shape=[jax.ShapeDtypeStruct((n_batch, tok, d), BF16)]
                + [jax.ShapeDtypeStruct((2, n_batch, e2, tok), BF16), jax.ShapeDtypeStruct((stages - 1, 2, n_batch, e2, tok), BF16)],
                grid_spec=pltpu.PrefetchScalarGridSpec(
                    num_scalar_prefetch=1, grid=(kt,),
                    in_specs=[x_spec, whole(1, d),
                              pl.BlockSpec((d, kv_half), lambda i, c: (0, kb + c[1])),
                              pl.BlockSpec((d, kv_half), lambda i, c: (0, kb + CORES + c[1])), rot_spec, rot_spec]
                    + [any_spec] * len(filled),
                    out_specs=[x_spec, pl.BlockSpec((1, kn, e2, tok), lambda i, _: (side, i, 0, 0)),
                               pl.BlockSpec((stages - 1, 1, kn, e2, tok), lambda i, _: (0, side, i, 0, 0))]),
                input_output_aliases={7 + i: 1 + i for i in range(len(filled))},
                compiler_params=params(), name='kv_proj',
                cost_estimate=cost(PAIR * n_batch * tok * d * PAIR * kv_half, 3 * n_batch * tok * d * 2),
            )(ids, x, norm2, w_qkv, w_qkv, cos_t[side], sin_t[side], *filled)

        first = lambda i: jnp.minimum(i, tiles - 1)
        second = lambda i: jnp.maximum(i - tiles, 0)
        own_spec = pl.BlockSpec((nb, tok, d), lambda i, _: (first(i), 0, 0))
        par_spec = pl.BlockSpec((nb, tok, d), lambda i, _: (second(i), 0, 0))
        own_out = pl.BlockSpec((nb, q_half, tok), lambda i, _: (first(i), 0, 0))
        par_out = pl.BlockSpec((nb, q_half, tok), lambda i, _: (second(i), 0, 0))
        both_rot = whole(2, half_rot, tok)
        q_shapes = (jax.ShapeDtypeStruct((n_batch, q_half, tok), BF16), jax.ShapeDtypeStruct((n_batch, q_half, tok), BF16))

        def q_proj(h0, h1):
            return pl.pallas_call(
                drop_scalar(q_proj_kernel), out_shape=q_shapes,
                grid_spec=pltpu.PrefetchScalarGridSpec(
                    num_scalar_prefetch=1, grid=(PAIR * tiles,),
                    in_specs=[own_spec, par_spec, pl.BlockSpec((d, q_half), lambda i, c: (0, c[1])), both_rot, both_rot],
                    out_specs=(own_out, par_out)),
                compiler_params=params(), name='q_proj',
                cost_estimate=cost(4 * n_batch * tok * d * q_half, 6 * n_batch * tok * d * 2),
            )(ids, h0, h1, w_qkv, cos_t, sin_t)

        def do_proj(g0, g1):
            return pl.pallas_call(
                drop_scalar(do_proj_kernel), out_shape=q_shapes,
                grid_spec=pltpu.PrefetchScalarGridSpec(
                    num_scalar_prefetch=1, grid=(PAIR * tiles,),
                    in_specs=[own_spec, par_spec, pl.BlockSpec((q_half, d), lambda i, c: (c[1], 0))],
                    out_specs=(own_out, par_out)),
                compiler_params=params(), name='do_proj',
                cost_estimate=cost(4 * n_batch * tok * d * q_half, 6 * n_batch * tok * d * 2),
            )(ids, g0, g1, w_o)

        h_own, *kv_sides = kv_proj(hidden, 0, [])
        h_par, *kv_sides = kv_proj(x_par, 1, kv_sides)
        gathered = [lax.all_gather(kv, 'x') for kv in kv_sides]
        q_own, q_par = q_proj(h_own, h_par)
        do_own, do_par = do_proj(grad_out, go_par)

        n_g = PAIR * rows // chips
        n_s = e2 + n_g
        hbm = pl.BlockSpec(memory_space=pl.ANY)
        shard_spec = lambda n: whole(n, d)

        def gather_shard(shard):
            return lax.all_gather(shard, ('x', 'core')).reshape(chips, CORES, *shard.shape)

        def attention(s, prev):
            blk = PAIR * tok
            has_sum = prev is not None
            if s == 0:
                kv_spec = along(2, chips, 2, 1, e2, tok)
            else:
                kv_spec = pl.BlockSpec((chips, None, 2, 1, e2, tok), lambda b: (0, s - 1, 0, b, 0, 0))
            q_spec = pl.BlockSpec((1, rows, tok), lambda b: (b, s, 0))
            t_spec = pl.BlockSpec((2, tok, d), lambda b: (b // 2, 0, 0))
            r_spec = whole(2, half_rot, tok)
            o_spec = along(1, 2, 1, rows, tok)
            return pl.pallas_call(
                functools.partial(attn_kernel, has_sum=has_sum),
                out_shape=[jax.ShapeDtypeStruct((2, n_batch, rows, tok), BF16)] * 2
                + [jax.ShapeDtypeStruct((chips, n_s, d), BF16)]
                + [jax.ShapeDtypeStruct((n, d), BF16) for n in (e2, n_g)] * has_sum,
                grid=(n_batch,),
                in_specs=[q_spec, q_spec, q_spec, q_spec, kv_spec,
                          t_spec, t_spec, t_spec, t_spec, r_spec, r_spec]
                + [hbm] * has_sum,
                out_specs=[o_spec, o_spec, whole(chips, n_s, d)]
                + [shard_spec(e2), shard_spec(n_g)] * has_sum,
                scratch_shapes=[pltpu.VMEM((chips, blk, reps * blk), F32), pltpu.VMEM((chips, blk, reps * blk), BF16),
                                pltpu.VMEM((chips, blk, reps * blk), BF16), pltpu.VMEM((e, reps * blk), F32),
                                pltpu.VMEM((8, reps * blk), F32),
                                pltpu.VMEM((chips, blk, e2), BF16), pltpu.VMEM((2, PAIR * rows, blk), BF16),
                                pltpu.VMEM((PAIR * rows, d), F32)]
                + RingSum.scratch(n_s, d) * has_sum,
                compiler_params=comm_params(s) if has_sum else params(),
                cost_estimate=cost(4e10, 3e7, 3e7),
            )(q_own, q_par, do_own, do_par, gathered[min(s, 1)], h_own, h_par, grad_out, go_par, cos_t, sin_t,
              *([prev] * has_sum))

        own, par, totals, main = [], [], [], []
        prev = None
        for s in range(stages):
            own_s, par_s, send, *sums = attention(s, prev)
            own.append(own_s)
            par.append(lax.ppermute(par_s, 'core', swap))
            prev = send
            totals += sums[:1]
            main += [gather_shard(g) for g in sums[1:]]

        nb2 = 2
        t2_spec = along(0, nb2, tok, d)
        block_out, total = pl.pallas_call(
            functools.partial(out_kernel, stages=stages),
            out_shape=[jax.ShapeDtypeStruct((n_batch, tok, d), BF16), jax.ShapeDtypeStruct((e2, d), BF16)],
            grid=(n_batch // nb2,),
            in_specs=[t2_spec, whole(n_heads * e, d), hbm]
            + [along(1, 1, nb2, rows, tok)] * (PAIR * stages),
            out_specs=[t2_spec, shard_spec(e2)],
            scratch_shapes=[pltpu.VMEM((nb2 * tok, n_heads * e), BF16)] + RingSum.scratch(e2, d),
            compiler_params=comm_params(stages), name='out_proj',
            cost_estimate=cost(PAIR * n_batch * tok * d * n_heads * e, 3e7),
        )(hidden, w_o, prev, *own, *par)
        totals.append(total)

        gb = 2
        gf_spec = along(0, gb, stages * e2, tok)
        n_kv = stages * e2 // chips
        kv_own_g, kv_par_g, send_kv, shard = pl.pallas_call(
            functools.partial(kv_grad_kernel, stages=stages),
            out_shape=[jax.ShapeDtypeStruct((n_batch, stages * e2, tok), BF16)] * 2
            + [jax.ShapeDtypeStruct((chips, n_kv, d), BF16), jax.ShapeDtypeStruct((n_g, d), BF16)],
            grid=(n_batch // gb,),
            in_specs=[along(1, e2, PAIR * tok * gb)] * stages
            + [along(0, gb, tok, d)] * 2 + [whole(2, half_rot, tok)] * 2
            + [hbm],
            out_specs=[gf_spec, gf_spec, whole(chips, n_kv, d), shard_spec(n_g)],
            scratch_shapes=[pltpu.VMEM((stages * e2, d), F32)] + RingSum.scratch(n_g, d),
            compiler_params=comm_params(stages + 1), name='kv_grad',
            cost_estimate=cost(PAIR * PAIR * n_batch * tok * d * stages * e2, 3e7),
        )(*totals, h_own, h_par, cos_t, sin_t, prev)
        main.append(gather_shard(shard))
        kv_other_g = lax.ppermute(kv_par_g, 'core', swap)

        nb3 = 2
        t3_spec = along(0, nb3, tok, d)
        n_t = n_kv + 16
        grad_hidden, tail_block = pl.pallas_call(
            functools.partial(norm_grad_kernel, stages=stages),
            out_shape=[jax.ShapeDtypeStruct((n_batch, tok, d), BF16), jax.ShapeDtypeStruct((n_t, d), BF16)],
            grid=(n_batch // nb3,),
            in_specs=[t3_spec, t3_spec, whole(1, d), whole(*w_qkv.shape)]
            + [along(0, nb3, stages * e2, tok)] * 2 + [hbm]
            + [pl.BlockSpec((1, nb3, rows, tok), lambda b: (1, b, 0, 0))] * (PAIR * stages),
            out_specs=[t3_spec, shard_spec(n_t)],
            scratch_shapes=[pltpu.VMEM((nb3 * tok, w_qkv.shape[1]), BF16), pltpu.VMEM((nb3 * tok, d), F32), pltpu.VMEM((8, d), F32)]
            + RingSum.scratch(n_kv, d),
            compiler_params=comm_params(stages + 2), name='norm_grad',
            cost_estimate=cost(PAIR * n_batch * tok * d * w_qkv.shape[1], 4e7),
        )(hidden, grad_out, norm2, w_qkv, kv_own_g, kv_other_g, send_kv, *own, *par)

        tail = gather_shard(tail_block)
        n_q = rows // chips
        b_spec = pl.BlockSpec((n_batch // (CORES * stages), tok, d), lambda p, s: (p * stages + s, 0, 0))
        w_cols, grad_w_out, block_out, grad_hidden = pl.pallas_call(
            functools.partial(assemble_main_kernel, stages=stages, n_q=n_q),
            out_shape=[jax.ShapeDtypeStruct(w_qkv.shape, F32), jax.ShapeDtypeStruct((n_heads, e, d), F32)]
            + [jax.ShapeDtypeStruct((n_batch, tok, d), BF16)] * PAIR,
            grid=(CORES, stages),
            in_specs=[along(1, chips, 1, n_g, d)] * stages + [b_spec] * PAIR,
            out_specs=[pl.BlockSpec((d, rows), lambda p, s: (0, p * stages + s)),
                       pl.BlockSpec((reps, e, d), lambda p, s: (p * stages + s, 0, 0)), b_spec, b_spec],
            compiler_params=params(2), name='assemble_main', cost_estimate=cost(2e9, 6e7),
        )(*main, block_out, grad_hidden)
        kcol = PAIR * q_half // kv_half
        extra = n_t - n_kv
        grad_w_qkv, grad_norm_w = pl.pallas_call(
            assemble_tail_kernel,
            out_shape=[jax.ShapeDtypeStruct(w_qkv.shape, F32), jax.ShapeDtypeStruct((1, d), F32)],
            grid=(CORES, PAIR),
            in_specs=[pl.BlockSpec((chips, 1, e, d), lambda p, k: (0, p, k, 0)),
                      pl.BlockSpec((chips, CORES, extra, d), lambda p, k: (0, 0, n_kv // extra, 0)),
                      pl.BlockSpec(memory_space=pl.ANY)],
            out_specs=[pl.BlockSpec((d, kv_half), lambda p, k: (0, kcol + k * CORES + p)), whole(1, d)],
            input_output_aliases={2: 0},
            compiler_params=params(2), name='assemble_tail', cost_estimate=cost(1e9, 2e7),
        )(tail, tail, w_cols)
        grad_norm_w = grad_norm_w.reshape(d)
        return block_out, grad_hidden, grad_w_qkv, grad_w_out, grad_norm_w

    tok_spec = P('dp', ('x', 'core'), None)
    return jax.shard_map(device_step, mesh=mesh2,
                         in_specs=(tok_spec, P(), P(), P(), P(), tok_spec),
                         out_specs=(tok_spec, tok_spec, P('dp', None), P('dp', None, None), P('dp')),
                         check_vma=False)
```

```python
import functools
import math

import jax
import jax.numpy as jnp
from jax import lax
from jax.experimental import pallas as pl
from jax.experimental.pallas import tpu as pltpu
from jax.sharding import Mesh, PartitionSpec as P


NORM_EPS = 1e-5
ROPE_BASE = 10000.0
ROPE_GAIN = math.sqrt(1.0 + math.log(32.0) / math.log(4096.0))
MASK_VALUE = -1e30
LOG2E = math.log2(math.e)
CORES = 2
PAIR = 2
BF16 = jnp.bfloat16
F32 = jnp.float32
VMEM_LIMIT = 60 * 1024 * 1024

NN = (((1,), (0,)), ((), ()))
NT = (((1,), (1,)), ((), ()))


cat_rows = functools.partial(jnp.concatenate, axis=0)
cat_lanes = functools.partial(jnp.concatenate, axis=1)
column_max = functools.partial(jnp.max, axis=0, keepdims=True)
column_sum = functools.partial(jnp.sum, axis=0, keepdims=True)
row_mean = functools.partial(jnp.mean, axis=-1, keepdims=True)


def whole(*shape):
    return pl.BlockSpec(shape, lambda *_: (0,) * len(shape))


def along(axis, *shape):
    return pl.BlockSpec(shape, lambda i, *_: tuple(i if n == axis else 0 for n in range(len(shape))))


def dot(a, b, dims=NN):
    return lax.dot_general(a, b, dims, preferred_element_type=F32)


def cost(flops, nbytes, trans=0):
    return pl.CostEstimate(flops=int(flops), bytes_accessed=int(nbytes), transcendentals=int(trans))


def params(n_axes=1):
    return pltpu.CompilerParams(dimension_semantics=("arbitrary",) * n_axes, vmem_limit_bytes=VMEM_LIMIT)


def rope_rows(block, cos, sin, direction):
    half = cos.shape[0]
    a, b = block[:half], block[half:PAIR * half]
    s = sin * direction
    return cat_rows([a * cos - b * s, b * cos + a * s])


def kv_proj_kernel(x_ref, g_ref, wk_ref, wv_ref, cos_ref, sin_ref, *refs):
    nb, tok, d = x_ref.shape
    stages = (wk_ref.shape[1] // (PAIR * cos_ref.shape[0]))
    h_ref, first_ref, second_ref, rest_ref = refs[-4:]
    kv_refs = [first_ref, second_ref] + [rest_ref.at[i] for i in range(stages - 2)]
    e2 = first_ref.shape[2]
    e = e2 // 2
    x = x_ref[:].reshape(nb * tok, d).astype(F32)
    inv = lax.rsqrt(row_mean(x * x) + NORM_EPS)
    h = (x * inv * g_ref[:].astype(F32)).astype(BF16)
    h_ref[:] = h.reshape(nb, tok, d)
    cos, sin = cos_ref[:], sin_ref[:]
    k = dot(h, wk_ref[:]).T
    v = dot(h, wv_ref[:]).T
    for i in range(stages):
        for b in range(nb):
            kv_refs[i][0, b, 0:e] = rope_rows(k[i * e:(i + 1) * e, b * tok:(b + 1) * tok], cos, sin, 1.0).astype(BF16)
            kv_refs[i][0, b, e:PAIR * e] = v[i * e:(i + 1) * e, b * tok:(b + 1) * tok].astype(BF16)


def q_do_proj_kernel(h0_ref, h1_ref, g0_ref, g1_ref, wq_ref, wo_ref, cos_ref, sin_ref, q0_ref, q1_ref, do0_ref, do1_ref):
    nb, tok, d = h0_ref.shape
    e = PAIR * cos_ref.shape[1]
    rows = wo_ref.shape[0]
    scale = e ** -0.5
    step = 4 * e

    def run(h_ref, g_ref, q_ref, do_ref, side):
        h = h_ref[:].reshape(nb * tok, d)
        g = g_ref[:].reshape(nb * tok, d)
        cos, sin = cos_ref[side], sin_ref[side]
        for r in range(0, rows, step):
            blk = dot(h, wq_ref[:, r:r + step]).T
            for i in range(0, step, e):
                for b in range(nb):
                    q_ref[b, r + i:r + i + e] = (rope_rows(blk[i:i + e, b * tok:(b + 1) * tok], cos, sin, 1.0).astype(BF16)
                                                 * scale).astype(BF16)
        for r in range(0, rows, 512):
            blk = dot(wo_ref[r:r + 512], g, NT)
            for b in range(nb):
                do_ref[b, r:r + 512] = blk[:, b * tok:(b + 1) * tok].astype(BF16)

    half = pl.num_programs(0) // 2
    pl.when(pl.program_id(0) < half)(lambda: run(h0_ref, g0_ref, q0_ref, do0_ref, 0))
    pl.when(pl.program_id(0) >= half)(lambda: run(h1_ref, g1_ref, q1_ref, do1_ref, 1))


def drop_scalar(kernel):
    def wrapped(_, *refs):
        kernel(*refs)

    return wrapped


def ring_peers(chips):
    chip, core = lax.axis_index('x'), lax.axis_index('core')
    return chip, lax.rem(chip + 1, chips), lax.rem(chip + chips - 1, chips), lax.rem(chip + 2, chips), core, 1 - core


def ring_barrier(chips):
    _, right, left, _, _, _ = ring_peers(chips)
    sem = pltpu.get_barrier_semaphore()
    for who in (right, left):
        pl.semaphore_signal(sem, inc=1, device_id={'x': who}, device_id_type=pl.DeviceIdType.MESH)
    pl.semaphore_wait(sem, 2)


class RingSum:
    @staticmethod
    def scratch(rows, d):
        half = rows // 2
        return [pltpu.VMEM((PAIR, half, d), BF16), pltpu.VMEM((PAIR, half, d), BF16), pltpu.VMEM((rows, d), BF16),
                pltpu.VMEM((PAIR, rows, d), BF16), pltpu.SemaphoreType.DMA((6,)), pltpu.SemaphoreType.DMA((6,)),
                pltpu.SemaphoreType.DMA((3,))]

    def __init__(self, send_ref, totals, plan, base, mid, buf, own, recv, s_sem, r_sem, l_sem):
        self.chips = chips = send_ref.shape[0]
        rows = own.shape[0]
        half = rows // 2
        chip, right, left, far, _, _ = ring_peers(chips)
        top, low = pl.ds(0, half), pl.ds(half, half)
        from_top, from_low = pl.ds(base, half), pl.ds(base + half, half)

        def remote(n, src, dst, who):
            return pltpu.make_async_remote_copy(src_ref=src, dst_ref=dst, send_sem=s_sem.at[n], recv_sem=r_sem.at[n],
                                                device_id={'x': who}, device_id_type=pl.DeviceIdType.MESH)

        self.far = [remote(0, send_ref.at[far, from_top], mid.at[0], right),
                    remote(1, send_ref.at[far, from_low], mid.at[1], left)]
        self.direct = [remote(2, send_ref.at[left, from_top], recv.at[1, top], left),
                       remote(3, send_ref.at[right, from_low], recv.at[0, low], right)]
        self.second = [remote(4, buf.at[0], recv.at[0, top], right), remote(5, buf.at[1], recv.at[1, low], left)]
        self.local = [pltpu.make_async_copy(send_ref.at[right, from_top], buf.at[0], l_sem.at[0]),
                      pltpu.make_async_copy(send_ref.at[left, from_low], buf.at[1], l_sem.at[1]),
                      pltpu.make_async_copy(send_ref.at[chip, pl.ds(base, rows)], own, l_sem.at[2])]
        self.mid, self.buf, self.own, self.recv, self.totals = mid, buf, own, recv, totals
        self.plan = plan

    def start(self):
        ring_barrier(self.chips)
        for c in self.far + self.local:
            c.start()

    def start_direct(self):
        for c in self.direct:
            c.start()

    def merge(self):
        for far, local, buf, mid in zip(self.far, self.local, (self.buf.at[0], self.buf.at[1]), (self.mid.at[0], self.mid.at[1])):
            local.wait()
            far.wait_recv()
            buf[:] = (buf[:].astype(F32) + mid[:].astype(F32)).astype(BF16)

    def send(self):
        for c in self.second:
            c.start()

    def finish(self):
        self.local[-1].wait()
        for c in self.direct + self.second:
            c.wait_recv()
        row = 0
        for ref in self.totals:
            r = slice(row, row + ref.shape[0])
            ref[:] = (self.own[r].astype(F32) + self.recv[0, r].astype(F32) + self.recv[1, r].astype(F32)).astype(BF16)
            row += ref.shape[0]
        for c in self.far + self.direct + self.second:
            c.wait_send()

    def ahead(self, step):
        direct, merge = self.plan
        run_at(step, 0, self.start)
        run_at(step, direct, self.start_direct)
        run_at(step, merge + 1, self.send)

    def behind(self, step, final):
        run_at(step, self.plan[1], self.merge)
        run_at(step, final, self.finish)


def run_at(step, n, *actions):
    @pl.when(step == n)
    def _():
        for a in actions:
            a()


def comm_params(cid, n_axes=1):
    return pltpu.CompilerParams(dimension_semantics=("arbitrary",) * n_axes, vmem_limit_bytes=VMEM_LIMIT,
                                collective_id=cid, has_side_effects=True)


def attn_kernel(q0_ref, q1_ref, do0_ref, do1_ref, kv_ref, h0_ref, h1_ref, g0_ref, g1_ref, cos_ref, sin_ref, *refs,
                has_sum):
    refs = list(refs)
    prev_ref = refs.pop(0) if has_sum else None
    own_ref, par_ref, send_ref = refs[:3]
    refs = refs[3:]
    totals = [refs.pop(0), refs.pop(0)] if has_sum else []
    s_ref, p_ref, ds_ref, acc_ref, ml_ref, kvt_ref, lhs_ref, gacc_ref = refs[:8]
    chip, core = lax.axis_index('x'), lax.axis_index('core')
    b_id = pl.program_id(0)
    if has_sum:
        ring_sum = RingSum(prev_ref, totals, (2, 3), 0, *refs[8:])
        ring_sum.ahead(b_id)
    chips = kv_ref.shape[0]
    rows, tok = q0_ref.shape[1], q0_ref.shape[2]
    e = kv_ref.shape[3] // 2
    reps = rows // e
    blk = PAIR * tok

    def heads_to_lanes(first_ref, second_ref):
        full = cat_lanes([first_ref[0], second_ref[0]])
        return cat_lanes([full[i * e:(i + 1) * e] for i in range(reps)])

    head_cols = [slice(i * blk, (i + 1) * blk) for i in range(reps)]

    def kv_block(i):
        return cat_lanes([kv_ref[chip - i, 0, 0], kv_ref[chip - i, 1, 0]])

    def scores(i):
        qt = heads_to_lanes(q0_ref, q1_ref)
        q_pad = cat_rows([qt, jnp.zeros_like(qt)])
        kvt = kv_block(i).T
        kvt_ref[i] = kvt
        tops = []
        for cols in head_cols:
            t = dot(kvt, q_pad[:, cols])
            if i == 0:
                r = lax.broadcasted_iota(jnp.int32, (blk, blk), 0)
                c = lax.broadcasted_iota(jnp.int32, (blk, blk), 1)
                shift = (1 - PAIR * core) * tok
                k_pos = jnp.where(r < tok, r, r - tok + shift)
                q_pos = jnp.where(c < tok, c, c - tok + shift)
                t = jnp.where(k_pos <= q_pos, t, MASK_VALUE)
            s_ref[i, :, cols] = t
            tops.append(column_max(t))
        return cat_lanes(tops) * LOG2E

    def accumulate(i, m):
        v_t = kv_block(i)[e:PAIR * e]
        sums, outs = [], []
        for cols in head_cols:
            p = jnp.exp2(s_ref[i, :, cols] * LOG2E - m[:, cols])
            sums.append(column_sum(p))
            outs.append(dot(v_t, p.astype(BF16)))
        return cat_lanes(sums), cat_lanes(outs)

    ml_ref[0:1] = scores(0)
    ml_ref[1:2] = jnp.zeros_like(ml_ref[1:2])
    acc_ref[:] = jnp.zeros_like(acc_ref)

    for i in range(1, chips):
        @pl.when(i <= chip)
        def _(i=i):
            m = ml_ref[0:1]
            add_l, add_o = accumulate(i - 1, m)
            m_new = jnp.maximum(m, scores(i))
            alpha = jnp.exp2(m - m_new)
            acc_ref[:] = (acc_ref[:] + add_o) * alpha
            ml_ref[1:2] = (ml_ref[1:2] + add_l) * alpha
            ml_ref[0:1] = m_new

    m = ml_ref[0:1]
    add_l, add_o = accumulate(chip, m)
    l = ml_ref[1:2] + add_l
    o_t = (acc_ref[:] + add_o) * (1.0 / l)
    dot_t = heads_to_lanes(do0_ref, do1_ref)
    ml_ref[1:2] = column_sum(o_t * dot_t.astype(F32))
    ml_ref[0:1] = m + jnp.log2(l)
    o_b = o_t.astype(BF16)
    o_full = cat_rows([o_b[:, cols] for cols in head_cols])
    odd = lax.rem(b_id, 2)
    lhs_ref[odd, rows:PAIR * rows] = o_full
    own_ref[0, 0] = o_full[:, :tok]
    par_ref[0, 0] = o_full[:, tok:]
    acc_ref[:] = jnp.zeros_like(acc_ref)

    def score_grads(i):
        dot_t = heads_to_lanes(do0_ref, do1_ref)
        do_pad = cat_rows([jnp.zeros_like(dot_t), dot_t])
        kvt = kvt_ref[i]
        for cols in head_cols:
            p = jnp.exp2(s_ref[i, :, cols] * LOG2E - ml_ref[0:1, cols])
            dp = dot(kvt, do_pad[:, cols])
            p_ref[i, :, cols] = p.astype(BF16)
            ds_ref[i, :, cols] = (p * (dp - ml_ref[1:2, cols])).astype(BF16)

    def input_grads(i):
        qt = heads_to_lanes(q0_ref, q1_ref)
        dot_t = heads_to_lanes(do0_ref, do1_ref)
        k_t = kv_block(i)[0:e]
        dv = dot(dot_t, p_ref[i], NT)
        dk = dot(qt, ds_ref[i], NT)
        send_ref[chip - i, 0:PAIR * e, pl.ds(pl.multiple_of(b_id * blk, blk), blk)] = cat_rows([dk, dv]).astype(BF16)
        acc_ref[:] += dot(k_t, ds_ref[i])

    score_grads(0)
    for i in range(1, chips):
        @pl.when(i <= chip)
        def _(i=i):
            input_grads(i - 1)
            score_grads(i)

    input_grads(chip)

    def zero_step(j, carry):
        send_ref[j, 0:PAIR * e, pl.ds(pl.multiple_of(b_id * blk, blk), blk)] = jnp.zeros((PAIR * e, blk), BF16)
        return carry

    lax.fori_loop(chip + 1, chips, zero_step, 0)

    cos = cat_lanes([cos_ref[0], cos_ref[1]])
    sin = cat_lanes([sin_ref[0], sin_ref[1]])
    dq_rows = []
    for cols in head_cols:
        dq = (acc_ref[:, cols] * (e ** -0.5)).astype(BF16).astype(F32)
        dq_rows.append(rope_rows(dq, cos, sin, -1.0).astype(BF16))
    dq_full = cat_rows(dq_rows)
    own_ref[1, 0] = dq_full[:, :tok]
    par_ref[1, 0] = dq_full[:, tok:]

    d = h0_ref.shape[2]
    step = 512
    lhs_ref[odd, 0:rows] = dq_full

    def weight_grads(first):
        for c in range(0, d, step):
            cs = slice(c, c + step)
            for r, (a_ref, b_ref) in enumerate(((h0_ref, h1_ref), (g0_ref, g1_ref))):
                rs = slice(r * rows, (r + 1) * rows)
                lhs = cat_lanes([lhs_ref[0, rs], lhs_ref[1, rs]])
                rhs = cat_rows([a_ref[0, :, cs], b_ref[0, :, cs], a_ref[1, :, cs], b_ref[1, :, cs]])
                if first:
                    gacc_ref[rs, cs] = dot(lhs, rhs)
                else:
                    gacc_ref[rs, cs] += dot(lhs, rhs)

    pl.when(b_id == 1)(lambda: weight_grads(True))
    pl.when((odd == 1) & (b_id > 1))(lambda: weight_grads(False))

    @pl.when(b_id == pl.num_programs(0) - 1)
    def _():
        for j in range(chips):
            n = rows // chips
            base = PAIR * e
            send_ref[j, base:base + n] = gacc_ref[j * n:(j + 1) * n].astype(BF16)
            send_ref[j, base + n:base + PAIR * n] = gacc_ref[rows + j * n:rows + (j + 1) * n].astype(BF16)

    if has_sum:
        ring_sum.behind(b_id, pl.num_programs(0) - 1)


def kv_grad_kernel(*refs, stages):
    recv = refs[:stages]
    h0_ref, h1_ref, cos_ref, sin_ref, prev_ref, own_ref, par_ref, send_ref, shard_ref, gacc_ref = refs[stages:stages + 10]
    ring_sum = RingSum(prev_ref, [shard_ref], (1, 2), own_ref.shape[1] // stages, *refs[stages + 10:])
    ring_sum.ahead(pl.program_id(0))
    nb, tok, d = h0_ref.shape
    e2 = own_ref.shape[1] // stages
    e = e2 // 2
    side = cat_lanes([cos_ref[0], cos_ref[1]]), cat_lanes([sin_ref[0], sin_ref[1]])
    cos, sin = (cat_lanes([t] * nb) for t in side)
    parts = []
    for r in recv:
        total = r[:].astype(F32)
        parts.append(cat_rows([rope_rows(total[0:e], cos, sin, -1.0), total[e:PAIR * e]]).astype(BF16))
    gf = cat_rows(parts)
    for b in range(nb):
        own_ref[b] = gf[:, PAIR * b * tok:(PAIR * b + 1) * tok]
        par_ref[b] = gf[:, (PAIR * b + 1) * tok:(PAIR * b + 2) * tok]

    def weight_grads(first):
        step = 512
        for c in range(0, d, step):
            cs = slice(c, c + step)
            hh = cat_rows([r[b, :, cs] for b in range(nb) for r in (h0_ref, h1_ref)])
            if first:
                gacc_ref[:, cs] = dot(gf, hh)
            else:
                gacc_ref[:, cs] += dot(gf, hh)

    pl.when(pl.program_id(0) == 0)(lambda: weight_grads(True))
    pl.when(pl.program_id(0) > 0)(lambda: weight_grads(False))

    @pl.when(pl.program_id(0) == pl.num_programs(0) - 1)
    def _():
        n = send_ref.shape[1]
        for j in range(send_ref.shape[0]):
            send_ref[j] = gacc_ref[j * n:(j + 1) * n].astype(BF16)

    ring_sum.behind(pl.program_id(0), pl.num_programs(0) - 1)


def out_kernel(x_ref, w_ref, prev_ref, *refs, stages):
    core = lax.axis_index('core')
    o_refs, (y_ref, total_ref, lhs_ref) = refs[:PAIR * stages], refs[PAIR * stages:PAIR * stages + 3]
    ring_sum = RingSum(prev_ref, [total_ref], (1, 2), 0, *refs[PAIR * stages + 3:])
    ring_sum.ahead(pl.program_id(0))
    nb, tok, d = x_ref.shape
    rows = o_refs[0].shape[2]
    half = stages * rows
    for side in range(2):
        base = (core if side == 0 else 1 - core) * half
        for s in range(stages):
            for b in range(nb):
                lhs_ref[b * tok:(b + 1) * tok, pl.ds(pl.multiple_of(base + s * rows, rows), rows)] = o_refs[side * stages + s][0, b].T
    lhs = lhs_ref[:]
    step = 512
    for c in range(0, d, step):
        prod = dot(lhs, w_ref[:, c:c + step])
        y_ref[:, :, c:c + step] = (x_ref[:, :, c:c + step].astype(F32) + prod.reshape(nb, tok, step)).astype(BF16)

    ring_sum.behind(pl.program_id(0), pl.num_programs(0) - 1)


def norm_grad_kernel(x_ref, go_ref, g_ref, w_ref, kv0_ref, kv1_ref, prev_ref, *refs, stages):
    core = lax.axis_index('core')
    q_refs = refs[:PAIR * stages]
    gh_ref, tail_ref, lhs_ref, tot_ref, gn_ref = refs[PAIR * stages:PAIR * stages + 5]
    n_kv = prev_ref.shape[1]
    ring_sum = RingSum(prev_ref, [tail_ref.at[pl.ds(0, n_kv)]], (1, 1), 0, *refs[PAIR * stages + 5:])
    ring_sum.ahead(pl.program_id(0))
    nb, tok, d = x_ref.shape
    rows = q_refs[0].shape[2]
    half = stages * rows
    e2 = kv0_ref.shape[1] // stages
    e = e2 // 2
    kv_half = stages * e
    for side in range(2):
        who = core if side == 0 else 1 - core
        kv_ref = kv0_ref if side == 0 else kv1_ref
        for b in range(nb):
            ts = slice(b * tok, (b + 1) * tok)
            for s in range(stages):
                lhs_ref[ts, pl.ds(pl.multiple_of(who * half + s * rows, rows), rows)] = q_refs[side * stages + s][0, b].T
            ks = cat_rows([kv_ref[b, i * e2:i * e2 + e] for i in range(stages)])
            vs = cat_rows([kv_ref[b, i * e2 + e:(i + 1) * e2] for i in range(stages)])
            base = PAIR * half
            lhs_ref[ts, pl.ds(pl.multiple_of(base + who * kv_half, kv_half), kv_half)] = ks.T
            base = base + PAIR * kv_half
            lhs_ref[ts, pl.ds(pl.multiple_of(base + who * kv_half, kv_half), kv_half)] = vs.T
    lhs = lhs_ref[:]
    step = 256
    for c in range(0, d, step):
        tot_ref[:, c:c + step] = dot(lhs, w_ref[c:c + step, :], NT)

    @pl.when(pl.program_id(0) == 0)
    def _():
        gn_ref[:] = jnp.zeros_like(gn_ref)

    g = g_ref[:].astype(F32)
    for b in range(nb):
        total = tot_ref[b * tok:(b + 1) * tok]
        x = x_ref[b].astype(F32)
        inv = lax.rsqrt(row_mean(x * x) + NORM_EPS)
        unit = x * inv
        gu = total * g
        mean_dot = row_mean(gu * unit)
        gh_ref[b] = (go_ref[b].astype(F32) + inv * (gu - unit * mean_dot)).astype(BF16)
        gn_ref[:] += jnp.sum((total * unit).reshape(tok // 8, 8, d), axis=0)

    @pl.when(pl.program_id(0) == pl.num_programs(0) - 1)
    def _():
        extra = tail_ref.shape[0] - n_kv
        total = column_sum(gn_ref[:])
        high = total.astype(BF16).astype(F32)
        row = lax.broadcasted_iota(jnp.int32, (extra, d), 0)
        tail_ref[n_kv:] = jnp.where(row == 0, high, jnp.where(row == 1, total - high, 0.0)).astype(BF16)

    ring_sum.behind(pl.program_id(0), pl.num_programs(0) - 1)


def transpose_to(out_ref, blk):
    for c in range(0, blk.shape[1], 256):
        out_ref[c:c + 256, :] = blk[:, c:c + 256].astype(F32).T


def assemble_main_kernel(*refs, stages, n_q):
    ins, (y_ref, gh_ref, wq_ref, wo_ref, y_out, gh_out) = refs[:stages], refs[stages:]
    y_out[:] = y_ref[:]
    gh_out[:] = gh_ref[:]
    for s in range(stages):
        @pl.when(pl.program_id(1) == s)
        def _(ref=ins[s]):
            chips, _, n, d = ref.shape
            transpose_to(wq_ref, ref[:, 0, 0:n_q].reshape(chips * n_q, d))
            wo_ref[:] = ref[:, 0, n_q:n].astype(F32)


def assemble_tail_kernel(in_ref, gn_ref, _, out_ref, norm_ref):
    norm_ref[:] = jnp.sum(gn_ref[:].astype(F32), axis=(0, 1, 2)).reshape(norm_ref.shape)
    chips, _, n, d = in_ref.shape
    transpose_to(out_ref, in_ref[:, 0].reshape(chips * n, d))


def solution(mesh):
    chips = mesh.shape['sp'] // CORES
    mesh2 = Mesh(mesh.devices.reshape(mesh.shape['dp'], chips, CORES), ('dp', 'x', 'core'))
    swap = [(i, CORES - 1 - i) for i in range(CORES)]

    def device_step(hidden, norm_w, w_qkv, w_out, long_factor, grad_out):
        n_batch, tok, d = hidden.shape
        n_heads, e = w_out.shape[0], w_out.shape[1]
        kv_heads = (w_qkv.shape[1] // e - n_heads) // 2
        reps = n_heads // kv_heads
        stages = kv_heads // CORES
        rows = reps * e
        q_half = stages * rows
        kv_half = stages * e
        e2 = PAIR * e
        half_rot = long_factor.shape[0]
        chip = lax.axis_index('x')
        core = lax.axis_index('core')
        ids = jnp.stack([chip, core]).astype(jnp.int32)
        tiles = 4
        nb = n_batch // tiles

        x_par = lax.ppermute(hidden, 'core', swap)
        go_par = lax.ppermute(grad_out, 'core', swap)
        w_o = w_out.reshape(n_heads * e, d)
        norm2 = norm_w.reshape(1, d)

        exponent = jnp.arange(half_rot, dtype=F32) / half_rot
        inv_freq = 1.0 / (long_factor * jnp.power(ROPE_BASE, exponent))
        sides = jnp.stack([core, 1 - core])
        positions = ((chip * CORES + sides)[:, None] * tok + jnp.arange(tok)[None, :]).astype(F32)
        angles = inv_freq[None, :, None] * positions[:, None, :]
        cos_t, sin_t = jnp.cos(angles) * ROPE_GAIN, jnp.sin(angles) * ROPE_GAIN

        tok_spec = along(0, nb, tok, d)
        rot_spec = whole(half_rot, tok)

        def kv_proj(x, side, filled):
            kb = PAIR * q_half // kv_half
            kt = 4
            kn = n_batch // kt
            x_spec = along(0, kn, tok, d)
            any_spec = pl.BlockSpec(memory_space=pl.ANY)
            return pl.pallas_call(
                drop_scalar(kv_proj_kernel),
                out_shape=[jax.ShapeDtypeStruct((n_batch, tok, d), BF16)]
                + [jax.ShapeDtypeStruct((2, n_batch, e2, tok), BF16)] * PAIR
                + [jax.ShapeDtypeStruct((stages - 2, 2, n_batch, e2, tok), BF16)],
                grid_spec=pltpu.PrefetchScalarGridSpec(
                    num_scalar_prefetch=1, grid=(kt,),
                    in_specs=[x_spec, whole(1, d),
                              pl.BlockSpec((d, kv_half), lambda i, c: (0, kb + c[1])),
                              pl.BlockSpec((d, kv_half), lambda i, c: (0, kb + CORES + c[1])), rot_spec, rot_spec]
                    + [any_spec] * len(filled),
                    out_specs=[x_spec] + [pl.BlockSpec((1, kn, e2, tok), lambda i, _: (side, i, 0, 0))] * PAIR
                    + [pl.BlockSpec((stages - 2, 1, kn, e2, tok), lambda i, _: (0, side, i, 0, 0))]),
                input_output_aliases={7 + i: 1 + i for i in range(len(filled))},
                compiler_params=params(), name='kv_proj',
                cost_estimate=cost(PAIR * n_batch * tok * d * PAIR * kv_half, 3 * n_batch * tok * d * 2),
            )(ids, x, norm2, w_qkv, w_qkv, cos_t[side], sin_t[side], *filled)

        first = lambda i: jnp.minimum(i, tiles - 1)
        second = lambda i: jnp.maximum(i - tiles, 0)
        own_spec = pl.BlockSpec((nb, tok, d), lambda i, _: (first(i), 0, 0))
        par_spec = pl.BlockSpec((nb, tok, d), lambda i, _: (second(i), 0, 0))
        own_out = pl.BlockSpec((nb, q_half, tok), lambda i, _: (first(i), 0, 0))
        par_out = pl.BlockSpec((nb, q_half, tok), lambda i, _: (second(i), 0, 0))
        both_rot = whole(2, half_rot, tok)
        q_shapes = [jax.ShapeDtypeStruct((n_batch, q_half, tok), BF16)] * PAIR

        def q_do_proj(h0, h1, g0, g1):
            return pl.pallas_call(
                drop_scalar(q_do_proj_kernel), out_shape=q_shapes * PAIR,
                grid_spec=pltpu.PrefetchScalarGridSpec(
                    num_scalar_prefetch=1, grid=(PAIR * tiles,),
                    in_specs=[own_spec, par_spec, own_spec, par_spec, pl.BlockSpec((d, q_half), lambda i, c: (0, c[1])),
                              pl.BlockSpec((q_half, d), lambda i, c: (c[1], 0)), both_rot, both_rot],
                    out_specs=[own_out, par_out] * PAIR),
                compiler_params=params(), name='q_do_proj',
                cost_estimate=cost(8 * n_batch * tok * d * q_half, 8 * n_batch * tok * d * 2),
            )(ids, h0, h1, g0, g1, w_qkv, w_o, cos_t, sin_t)

        h_own, *kv_sides = kv_proj(hidden, 0, [])
        h_par, *kv_sides = kv_proj(x_par, 1, kv_sides)
        gathered = [lax.all_gather(kv, 'x') for kv in kv_sides]
        q_own, q_par, do_own, do_par = q_do_proj(h_own, h_par, grad_out, go_par)

        n_g = PAIR * rows // chips
        n_s = e2 + n_g
        hbm = pl.BlockSpec(memory_space=pl.ANY)
        shard_spec = lambda n: whole(n, d)

        def gather_shard(shard):
            return lax.all_gather(shard, ('x', 'core')).reshape(chips, CORES, *shard.shape)

        def attention(s, prev):
            blk = PAIR * tok
            has_sum = prev is not None
            if s < 2:
                kv_spec = along(2, chips, 2, 1, e2, tok)
            else:
                kv_spec = pl.BlockSpec((chips, None, 2, 1, e2, tok), lambda b: (0, s - 2, 0, b, 0, 0))
            q_spec = pl.BlockSpec((1, rows, tok), lambda b: (b, s, 0))
            t_spec = pl.BlockSpec((2, tok, d), lambda b: (b // 2, 0, 0))
            r_spec = whole(2, half_rot, tok)
            o_spec = along(1, 2, 1, rows, tok)
            return pl.pallas_call(
                functools.partial(attn_kernel, has_sum=has_sum),
                out_shape=[jax.ShapeDtypeStruct((2, n_batch, rows, tok), BF16)] * 2
                + [jax.ShapeDtypeStruct((chips, n_s, d), BF16)]
                + [jax.ShapeDtypeStruct((n, d), BF16) for n in (e2, n_g)] * has_sum,
                grid=(n_batch,),
                in_specs=[q_spec, q_spec, q_spec, q_spec, kv_spec,
                          t_spec, t_spec, t_spec, t_spec, r_spec, r_spec]
                + [hbm] * has_sum,
                out_specs=[o_spec, o_spec, whole(chips, n_s, d)]
                + [shard_spec(e2), shard_spec(n_g)] * has_sum,
                scratch_shapes=[pltpu.VMEM((chips, blk, reps * blk), F32), pltpu.VMEM((chips, blk, reps * blk), BF16),
                                pltpu.VMEM((chips, blk, reps * blk), BF16), pltpu.VMEM((e, reps * blk), F32),
                                pltpu.VMEM((8, reps * blk), F32),
                                pltpu.VMEM((chips, blk, e2), BF16), pltpu.VMEM((2, PAIR * rows, blk), BF16),
                                pltpu.VMEM((PAIR * rows, d), F32)]
                + RingSum.scratch(n_s, d) * has_sum,
                compiler_params=comm_params(s) if has_sum else params(),
                cost_estimate=cost(4e10, 3e7, 3e7),
            )(q_own, q_par, do_own, do_par, gathered[min(s, 2)], h_own, h_par, grad_out, go_par, cos_t, sin_t,
              *([prev] * has_sum))

        own, par, totals, main = [], [], [], []
        prev = None
        for s in range(stages):
            own_s, par_s, send, *sums = attention(s, prev)
            own.append(own_s)
            par.append(lax.ppermute(par_s, 'core', swap))
            prev = send
            totals += sums[:1]
            if s < stages - 1:
                main += [gather_shard(g) for g in sums[1:]]

        nb2 = 2
        t2_spec = along(0, nb2, tok, d)
        block_out, total = pl.pallas_call(
            functools.partial(out_kernel, stages=stages),
            out_shape=[jax.ShapeDtypeStruct((n_batch, tok, d), BF16), jax.ShapeDtypeStruct((e2, d), BF16)],
            grid=(n_batch // nb2,),
            in_specs=[t2_spec, whole(n_heads * e, d), hbm]
            + [along(1, 1, nb2, rows, tok)] * (PAIR * stages),
            out_specs=[t2_spec, shard_spec(e2)],
            scratch_shapes=[pltpu.VMEM((nb2 * tok, n_heads * e), BF16)] + RingSum.scratch(e2, d),
            compiler_params=comm_params(stages), name='out_proj',
            cost_estimate=cost(PAIR * n_batch * tok * d * n_heads * e, 3e7),
        )(hidden, w_o, prev, *own, *par)
        late, total = lax.optimization_barrier((sums[-1], total))
        main.append(gather_shard(late))
        totals.append(total)

        gb = 2
        gf_spec = along(0, gb, stages * e2, tok)
        n_kv = stages * e2 // chips
        kv_own_g, kv_par_g, send_kv, shard = pl.pallas_call(
            functools.partial(kv_grad_kernel, stages=stages),
            out_shape=[jax.ShapeDtypeStruct((n_batch, stages * e2, tok), BF16)] * 2
            + [jax.ShapeDtypeStruct((chips, n_kv, d), BF16), jax.ShapeDtypeStruct((n_g, d), BF16)],
            grid=(n_batch // gb,),
            in_specs=[along(1, e2, PAIR * tok * gb)] * stages
            + [along(0, gb, tok, d)] * 2 + [whole(2, half_rot, tok)] * 2
            + [hbm],
            out_specs=[gf_spec, gf_spec, whole(chips, n_kv, d), shard_spec(n_g)],
            scratch_shapes=[pltpu.VMEM((stages * e2, d), F32)] + RingSum.scratch(n_g, d),
            compiler_params=comm_params(stages + 1), name='kv_grad',
            cost_estimate=cost(PAIR * PAIR * n_batch * tok * d * stages * e2, 3e7),
        )(*totals, h_own, h_par, cos_t, sin_t, prev)
        main.append(gather_shard(shard))
        kv_other_g = lax.ppermute(kv_par_g, 'core', swap)

        nb3 = 2
        t3_spec = along(0, nb3, tok, d)
        n_t = n_kv + 16
        grad_hidden, tail_block = pl.pallas_call(
            functools.partial(norm_grad_kernel, stages=stages),
            out_shape=[jax.ShapeDtypeStruct((n_batch, tok, d), BF16), jax.ShapeDtypeStruct((n_t, d), BF16)],
            grid=(n_batch // nb3,),
            in_specs=[t3_spec, t3_spec, whole(1, d), whole(*w_qkv.shape)]
            + [along(0, nb3, stages * e2, tok)] * 2 + [hbm]
            + [pl.BlockSpec((1, nb3, rows, tok), lambda b: (1, b, 0, 0))] * (PAIR * stages),
            out_specs=[t3_spec, shard_spec(n_t)],
            scratch_shapes=[pltpu.VMEM((nb3 * tok, w_qkv.shape[1]), BF16), pltpu.VMEM((nb3 * tok, d), F32), pltpu.VMEM((8, d), F32)]
            + RingSum.scratch(n_kv, d),
            compiler_params=comm_params(stages + 2), name='norm_grad',
            cost_estimate=cost(PAIR * n_batch * tok * d * w_qkv.shape[1], 4e7),
        )(hidden, grad_out, norm2, w_qkv, kv_own_g, kv_other_g, send_kv, *own, *par)

        tail = gather_shard(tail_block)
        n_q = rows // chips
        b_spec = pl.BlockSpec((n_batch // (CORES * stages), tok, d), lambda p, s: (p * stages + s, 0, 0))
        w_cols, grad_w_out, block_out, grad_hidden = pl.pallas_call(
            functools.partial(assemble_main_kernel, stages=stages, n_q=n_q),
            out_shape=[jax.ShapeDtypeStruct(w_qkv.shape, F32), jax.ShapeDtypeStruct((n_heads, e, d), F32)]
            + [jax.ShapeDtypeStruct((n_batch, tok, d), BF16)] * PAIR,
            grid=(CORES, stages),
            in_specs=[along(1, chips, 1, n_g, d)] * stages + [b_spec] * PAIR,
            out_specs=[pl.BlockSpec((d, rows), lambda p, s: (0, p * stages + s)),
                       pl.BlockSpec((reps, e, d), lambda p, s: (p * stages + s, 0, 0)), b_spec, b_spec],
            compiler_params=params(2), name='assemble_main', cost_estimate=cost(2e9, 6e7),
        )(*main, block_out, grad_hidden)
        kcol = PAIR * q_half // kv_half
        extra = n_t - n_kv
        grad_w_qkv, grad_norm_w = pl.pallas_call(
            assemble_tail_kernel,
            out_shape=[jax.ShapeDtypeStruct(w_qkv.shape, F32), jax.ShapeDtypeStruct((1, d), F32)],
            grid=(CORES, PAIR),
            in_specs=[pl.BlockSpec((chips, 1, e, d), lambda p, k: (0, p, k, 0)),
                      pl.BlockSpec((chips, CORES, extra, d), lambda p, k: (0, 0, n_kv // extra, 0)),
                      pl.BlockSpec(memory_space=pl.ANY)],
            out_specs=[pl.BlockSpec((d, kv_half), lambda p, k: (0, kcol + k * CORES + p)), whole(1, d)],
            input_output_aliases={2: 0},
            compiler_params=params(2), name='assemble_tail', cost_estimate=cost(1e9, 2e7),
        )(tail, tail, w_cols)
        grad_norm_w = grad_norm_w.reshape(d)
        return block_out, grad_hidden, grad_w_qkv, grad_w_out, grad_norm_w

    tok_spec = P('dp', ('x', 'core'), None)
    return jax.shard_map(device_step, mesh=mesh2,
                         in_specs=(tok_spec, P(), P(), P(), P(), tok_spec),
                         out_specs=(tok_spec, tok_spec, P('dp', None), P('dp', None, None), P('dp')),
                         check_vma=False)
```

```python
import functools
import math

import jax
import jax.numpy as jnp
from jax import lax
from jax.experimental import pallas as pl
from jax.experimental.pallas import tpu as pltpu
from jax.sharding import Mesh, PartitionSpec as P


NORM_EPS = 1e-5
ROPE_BASE = 10000.0
ROPE_GAIN = math.sqrt(1.0 + math.log(32.0) / math.log(4096.0))
MASK_VALUE = -1e30
LOG2E = math.log2(math.e)
CORES = 2
PAIR = 2
BF16 = jnp.bfloat16
F32 = jnp.float32
VMEM_LIMIT = 60 * 1024 * 1024

NN = (((1,), (0,)), ((), ()))
NT = (((1,), (1,)), ((), ()))


cat_rows = functools.partial(jnp.concatenate, axis=0)
cat_lanes = functools.partial(jnp.concatenate, axis=1)
column_max = functools.partial(jnp.max, axis=0, keepdims=True)
column_sum = functools.partial(jnp.sum, axis=0, keepdims=True)
row_mean = functools.partial(jnp.mean, axis=-1, keepdims=True)


def whole(*shape):
    return pl.BlockSpec(shape, lambda *_: (0,) * len(shape))


def along(axis, *shape):
    return pl.BlockSpec(shape, lambda i, *_: tuple(i if n == axis else 0 for n in range(len(shape))))


def dot(a, b, dims=NN):
    return lax.dot_general(a, b, dims, preferred_element_type=F32)


def cost(flops, nbytes, trans=0):
    return pl.CostEstimate(flops=int(flops), bytes_accessed=int(nbytes), transcendentals=int(trans))


def params(n_axes=1):
    return pltpu.CompilerParams(dimension_semantics=("arbitrary",) * n_axes, vmem_limit_bytes=VMEM_LIMIT)


def rope_rows(block, cos, sin, direction):
    half = cos.shape[0]
    a, b = block[:half], block[half:PAIR * half]
    s = sin * direction
    return cat_rows([a * cos - b * s, b * cos + a * s])


def kv_proj_kernel(x_ref, g_ref, wk_ref, wv_ref, cos_ref, sin_ref, *refs):
    nb, tok, d = x_ref.shape
    stages = (wk_ref.shape[1] // (PAIR * cos_ref.shape[0]))
    h_ref, first_ref, second_ref, rest_ref = refs[-4:]
    kv_refs = [first_ref, second_ref] + [rest_ref.at[i] for i in range(stages - 2)]
    e2 = first_ref.shape[2]
    e = e2 // 2
    x = x_ref[:].reshape(nb * tok, d).astype(F32)
    inv = lax.rsqrt(row_mean(x * x) + NORM_EPS)
    h = (x * inv * g_ref[:].astype(F32)).astype(BF16)
    h_ref[:] = h.reshape(nb, tok, d)
    cos, sin = cos_ref[:], sin_ref[:]
    k = dot(h, wk_ref[:]).T
    v = dot(h, wv_ref[:]).T
    for i in range(stages):
        for b in range(nb):
            kv_refs[i][0, b, 0:e] = rope_rows(k[i * e:(i + 1) * e, b * tok:(b + 1) * tok], cos, sin, 1.0).astype(BF16)
            kv_refs[i][0, b, e:PAIR * e] = v[i * e:(i + 1) * e, b * tok:(b + 1) * tok].astype(BF16)


def q_do_proj_kernel(h0_ref, h1_ref, g0_ref, g1_ref, wq_ref, wo_ref, cos_ref, sin_ref, q0_ref, q1_ref, do0_ref, do1_ref):
    nb, tok, d = h0_ref.shape
    e = PAIR * cos_ref.shape[1]
    rows = wo_ref.shape[0]
    scale = e ** -0.5
    step = 4 * e

    def run(h_ref, g_ref, q_ref, do_ref, side):
        h = h_ref[:].reshape(nb * tok, d)
        g = g_ref[:].reshape(nb * tok, d)
        cos, sin = cos_ref[side], sin_ref[side]
        for r in range(0, rows, step):
            blk = dot(h, wq_ref[:, r:r + step]).T
            for i in range(0, step, e):
                for b in range(nb):
                    q_ref[b, r + i:r + i + e] = (rope_rows(blk[i:i + e, b * tok:(b + 1) * tok], cos, sin, 1.0).astype(BF16)
                                                 * scale).astype(BF16)
        for r in range(0, rows, 512):
            blk = dot(wo_ref[r:r + 512], g, NT)
            for b in range(nb):
                do_ref[b, r:r + 512] = blk[:, b * tok:(b + 1) * tok].astype(BF16)

    half = pl.num_programs(0) // 2
    pl.when(pl.program_id(0) < half)(lambda: run(h0_ref, g0_ref, q0_ref, do0_ref, 0))
    pl.when(pl.program_id(0) >= half)(lambda: run(h1_ref, g1_ref, q1_ref, do1_ref, 1))


def drop_scalar(kernel):
    def wrapped(_, *refs):
        kernel(*refs)

    return wrapped


def ring_peers(chips):
    chip, core = lax.axis_index('x'), lax.axis_index('core')
    return chip, lax.rem(chip + 1, chips), lax.rem(chip + chips - 1, chips), lax.rem(chip + 2, chips), core, 1 - core


def ring_barrier(chips):
    _, right, left, _, _, mate = ring_peers(chips)
    sem = pltpu.get_barrier_semaphore()
    for who in ({'x': right}, {'x': left}, {'core': mate}):
        pl.semaphore_signal(sem, inc=1, device_id=who, device_id_type=pl.DeviceIdType.MESH)
    pl.semaphore_wait(sem, 3)


def mate_copy(n, src, dst, s_sem, r_sem):
    return pltpu.make_async_remote_copy(src_ref=src, dst_ref=dst, send_sem=s_sem.at[n], recv_sem=r_sem.at[n],
                                        device_id={'core': 1 - lax.axis_index('core')}, device_id_type=pl.DeviceIdType.MESH)


class RingSum:
    @staticmethod
    def scratch(rows, d):
        half = rows // 2
        return [pltpu.VMEM((PAIR, half, d), BF16), pltpu.VMEM((PAIR, half, d), BF16), pltpu.VMEM((rows, d), BF16),
                pltpu.VMEM((PAIR, rows, d), BF16), pltpu.SemaphoreType.DMA((6,)), pltpu.SemaphoreType.DMA((6,)),
                pltpu.SemaphoreType.DMA((3,))]

    def __init__(self, send_ref, totals, plan, base, mid, buf, own, recv, s_sem, r_sem, l_sem):
        self.chips = chips = send_ref.shape[0]
        rows = own.shape[0]
        half = rows // 2
        chip, right, left, far, _, _ = ring_peers(chips)
        top, low = pl.ds(0, half), pl.ds(half, half)
        from_top, from_low = pl.ds(base, half), pl.ds(base + half, half)

        def remote(n, src, dst, who):
            return pltpu.make_async_remote_copy(src_ref=src, dst_ref=dst, send_sem=s_sem.at[n], recv_sem=r_sem.at[n],
                                                device_id={'x': who}, device_id_type=pl.DeviceIdType.MESH)

        self.far = [remote(0, send_ref.at[far, from_top], mid.at[0], right),
                    remote(1, send_ref.at[far, from_low], mid.at[1], left)]
        self.direct = [remote(2, send_ref.at[left, from_top], recv.at[1, top], left),
                       remote(3, send_ref.at[right, from_low], recv.at[0, low], right)]
        self.second = [remote(4, buf.at[0], recv.at[0, top], right), remote(5, buf.at[1], recv.at[1, low], left)]
        self.local = [pltpu.make_async_copy(send_ref.at[right, from_top], buf.at[0], l_sem.at[0]),
                      pltpu.make_async_copy(send_ref.at[left, from_low], buf.at[1], l_sem.at[1]),
                      pltpu.make_async_copy(send_ref.at[chip, pl.ds(base, rows)], own, l_sem.at[2])]
        self.mid, self.buf, self.own, self.recv, self.totals = mid, buf, own, recv, totals
        self.plan = plan

    def start(self):
        ring_barrier(self.chips)
        for c in self.far + self.local:
            c.start()

    def start_direct(self):
        for c in self.direct:
            c.start()

    def merge(self):
        for far, local, buf, mid in zip(self.far, self.local, (self.buf.at[0], self.buf.at[1]), (self.mid.at[0], self.mid.at[1])):
            local.wait()
            far.wait_recv()
            buf[:] = (buf[:].astype(F32) + mid[:].astype(F32)).astype(BF16)

    def send(self):
        for c in self.second:
            c.start()

    def finish(self):
        self.local[-1].wait()
        for c in self.direct + self.second:
            c.wait_recv()
        row = 0
        for ref in self.totals:
            r = slice(row, row + ref.shape[0])
            ref[:] = (self.own[r].astype(F32) + self.recv[0, r].astype(F32) + self.recv[1, r].astype(F32)).astype(BF16)
            row += ref.shape[0]
        for c in self.far + self.direct + self.second:
            c.wait_send()

    def ahead(self, step):
        direct, merge = self.plan
        run_at(step, 0, self.start)
        run_at(step, direct, self.start_direct)
        run_at(step, merge + 1, self.send)

    def behind(self, step, final):
        run_at(step, self.plan[1], self.merge)
        run_at(step, final, self.finish)


def run_at(step, n, *actions):
    @pl.when(step == n)
    def _():
        for a in actions:
            a()


def comm_params(cid, n_axes=1):
    return pltpu.CompilerParams(dimension_semantics=("arbitrary",) * n_axes, vmem_limit_bytes=VMEM_LIMIT,
                                collective_id=cid, has_side_effects=True)


def attn_kernel(q0_ref, q1_ref, do0_ref, do1_ref, kv_ref, h0_ref, h1_ref, g0_ref, g1_ref, cos_ref, sin_ref, *refs,
                has_sum):
    refs = list(refs)
    prev_ref = refs.pop(0) if has_sum else None
    own_ref, other_ref, send_ref = refs[:3]
    refs = refs[3:]
    totals = [refs.pop(0), refs.pop(0)] if has_sum else []
    s_ref, p_ref, ds_ref, acc_ref, ml_ref, kvt_ref, lhs_ref, gacc_ref, par_ref, m_send, m_recv = refs[:11]
    chip, core = lax.axis_index('x'), lax.axis_index('core')
    b_id = pl.program_id(0)
    if has_sum:
        ring_sum = RingSum(prev_ref, totals, (2, 3), 0, *refs[11:])
        ring_sum.ahead(b_id)
    else:
        run_at(b_id, 0, lambda: ring_barrier(kv_ref.shape[0]))
    half_b = par_ref.shape[1] // PAIR
    to_mate = [mate_copy(i, par_ref.at[:, pl.ds(i * half_b, half_b)], other_ref.at[:, pl.ds(i * half_b, half_b)], m_send, m_recv)
               for i in range(PAIR)]
    run_at(b_id, half_b + 1, to_mate[0].start)
    chips = kv_ref.shape[0]
    rows, tok = q0_ref.shape[1], q0_ref.shape[2]
    e = kv_ref.shape[3] // 2
    reps = rows // e
    blk = PAIR * tok

    def heads_to_lanes(first_ref, second_ref):
        full = cat_lanes([first_ref[0], second_ref[0]])
        return cat_lanes([full[i * e:(i + 1) * e] for i in range(reps)])

    head_cols = [slice(i * blk, (i + 1) * blk) for i in range(reps)]

    def kv_block(i):
        return cat_lanes([kv_ref[chip - i, 0, 0], kv_ref[chip - i, 1, 0]])

    def scores(i):
        qt = heads_to_lanes(q0_ref, q1_ref)
        q_pad = cat_rows([qt, jnp.zeros_like(qt)])
        kvt = kv_block(i).T
        kvt_ref[i] = kvt
        tops = []
        for cols in head_cols:
            t = dot(kvt, q_pad[:, cols])
            if i == 0:
                r = lax.broadcasted_iota(jnp.int32, (blk, blk), 0)
                c = lax.broadcasted_iota(jnp.int32, (blk, blk), 1)
                shift = (1 - PAIR * core) * tok
                k_pos = jnp.where(r < tok, r, r - tok + shift)
                q_pos = jnp.where(c < tok, c, c - tok + shift)
                t = jnp.where(k_pos <= q_pos, t, MASK_VALUE)
            s_ref[i, :, cols] = t
            tops.append(column_max(t))
        return cat_lanes(tops) * LOG2E

    def accumulate(i, m):
        v_t = kv_block(i)[e:PAIR * e]
        sums, outs = [], []
        for cols in head_cols:
            p = jnp.exp2(s_ref[i, :, cols] * LOG2E - m[:, cols])
            sums.append(column_sum(p))
            outs.append(dot(v_t, p.astype(BF16)))
        return cat_lanes(sums), cat_lanes(outs)

    ml_ref[0:1] = scores(0)
    ml_ref[1:2] = jnp.zeros_like(ml_ref[1:2])
    acc_ref[:] = jnp.zeros_like(acc_ref)

    for i in range(1, chips):
        @pl.when(i <= chip)
        def _(i=i):
            m = ml_ref[0:1]
            add_l, add_o = accumulate(i - 1, m)
            m_new = jnp.maximum(m, scores(i))
            alpha = jnp.exp2(m - m_new)
            acc_ref[:] = (acc_ref[:] + add_o) * alpha
            ml_ref[1:2] = (ml_ref[1:2] + add_l) * alpha
            ml_ref[0:1] = m_new

    m = ml_ref[0:1]
    add_l, add_o = accumulate(chip, m)
    l = ml_ref[1:2] + add_l
    o_t = (acc_ref[:] + add_o) * (1.0 / l)
    dot_t = heads_to_lanes(do0_ref, do1_ref)
    ml_ref[1:2] = column_sum(o_t * dot_t.astype(F32))
    ml_ref[0:1] = m + jnp.log2(l)
    o_b = o_t.astype(BF16)
    o_full = cat_rows([o_b[:, cols] for cols in head_cols])
    odd = lax.rem(b_id, 2)
    lhs_ref[odd, rows:PAIR * rows] = o_full
    own_ref[0, 0] = o_full[:, :tok]
    par_ref[0, b_id] = o_full[:, tok:]
    acc_ref[:] = jnp.zeros_like(acc_ref)

    def score_grads(i):
        dot_t = heads_to_lanes(do0_ref, do1_ref)
        do_pad = cat_rows([jnp.zeros_like(dot_t), dot_t])
        kvt = kvt_ref[i]
        for cols in head_cols:
            p = jnp.exp2(s_ref[i, :, cols] * LOG2E - ml_ref[0:1, cols])
            dp = dot(kvt, do_pad[:, cols])
            p_ref[i, :, cols] = p.astype(BF16)
            ds_ref[i, :, cols] = (p * (dp - ml_ref[1:2, cols])).astype(BF16)

    def input_grads(i):
        qt = heads_to_lanes(q0_ref, q1_ref)
        dot_t = heads_to_lanes(do0_ref, do1_ref)
        k_t = kv_block(i)[0:e]
        dv = dot(dot_t, p_ref[i], NT)
        dk = dot(qt, ds_ref[i], NT)
        send_ref[chip - i, 0:PAIR * e, pl.ds(pl.multiple_of(b_id * blk, blk), blk)] = cat_rows([dk, dv]).astype(BF16)
        acc_ref[:] += dot(k_t, ds_ref[i])

    score_grads(0)
    for i in range(1, chips):
        @pl.when(i <= chip)
        def _(i=i):
            input_grads(i - 1)
            score_grads(i)

    input_grads(chip)

    def zero_step(j, carry):
        send_ref[j, 0:PAIR * e, pl.ds(pl.multiple_of(b_id * blk, blk), blk)] = jnp.zeros((PAIR * e, blk), BF16)
        return carry

    lax.fori_loop(chip + 1, chips, zero_step, 0)

    cos = cat_lanes([cos_ref[0], cos_ref[1]])
    sin = cat_lanes([sin_ref[0], sin_ref[1]])
    dq_rows = []
    for cols in head_cols:
        dq = (acc_ref[:, cols] * (e ** -0.5)).astype(BF16).astype(F32)
        dq_rows.append(rope_rows(dq, cos, sin, -1.0).astype(BF16))
    dq_full = cat_rows(dq_rows)
    own_ref[1, 0] = dq_full[:, :tok]
    par_ref[1, b_id] = dq_full[:, tok:]

    d = h0_ref.shape[2]
    step = 512
    lhs_ref[odd, 0:rows] = dq_full

    def weight_grads(first):
        for c in range(0, d, step):
            cs = slice(c, c + step)
            for r, (a_ref, b_ref) in enumerate(((h0_ref, h1_ref), (g0_ref, g1_ref))):
                rs = slice(r * rows, (r + 1) * rows)
                lhs = cat_lanes([lhs_ref[0, rs], lhs_ref[1, rs]])
                rhs = cat_rows([a_ref[0, :, cs], b_ref[0, :, cs], a_ref[1, :, cs], b_ref[1, :, cs]])
                if first:
                    gacc_ref[rs, cs] = dot(lhs, rhs)
                else:
                    gacc_ref[rs, cs] += dot(lhs, rhs)

    pl.when(b_id == 1)(lambda: weight_grads(True))
    pl.when((odd == 1) & (b_id > 1))(lambda: weight_grads(False))

    @pl.when(b_id == pl.num_programs(0) - 1)
    def _():
        for j in range(chips):
            n = rows // chips
            base = PAIR * e
            send_ref[j, base:base + n] = gacc_ref[j * n:(j + 1) * n].astype(BF16)
            send_ref[j, base + n:base + PAIR * n] = gacc_ref[rows + j * n:rows + (j + 1) * n].astype(BF16)

    final = pl.num_programs(0) - 1
    run_at(b_id, final, to_mate[1].start)
    if has_sum:
        ring_sum.behind(b_id, final)
    run_at(b_id, final, to_mate[0].wait, to_mate[1].wait)


def kv_grad_kernel(*refs, stages):
    recv = refs[:stages]
    h0_ref, h1_ref, cos_ref, sin_ref, prev_ref, own_ref, other_ref, send_ref, shard_ref, gacc_ref = refs[stages:stages + 10]
    par_ref, m_send, m_recv = refs[stages + 10:stages + 13]
    to_mate = mate_copy(0, par_ref, other_ref, m_send, m_recv)
    ring_sum = RingSum(prev_ref, [shard_ref], (1, 2), own_ref.shape[1] // stages, *refs[stages + 13:])
    ring_sum.ahead(pl.program_id(0))
    nb, tok, d = h0_ref.shape
    e2 = own_ref.shape[1] // stages
    e = e2 // 2
    side = cat_lanes([cos_ref[0], cos_ref[1]]), cat_lanes([sin_ref[0], sin_ref[1]])
    cos, sin = (cat_lanes([t] * nb) for t in side)
    parts = []
    for r in recv:
        total = r[:].astype(F32)
        parts.append(cat_rows([rope_rows(total[0:e], cos, sin, -1.0), total[e:PAIR * e]]).astype(BF16))
    gf = cat_rows(parts)
    for b in range(nb):
        own_ref[b] = gf[:, PAIR * b * tok:(PAIR * b + 1) * tok]
        par_ref[pl.program_id(0) * nb + b] = gf[:, (PAIR * b + 1) * tok:(PAIR * b + 2) * tok]

    def weight_grads(first):
        step = 512
        for c in range(0, d, step):
            cs = slice(c, c + step)
            hh = cat_rows([r[b, :, cs] for b in range(nb) for r in (h0_ref, h1_ref)])
            if first:
                gacc_ref[:, cs] = dot(gf, hh)
            else:
                gacc_ref[:, cs] += dot(gf, hh)

    pl.when(pl.program_id(0) == 0)(lambda: weight_grads(True))
    pl.when(pl.program_id(0) > 0)(lambda: weight_grads(False))

    @pl.when(pl.program_id(0) == pl.num_programs(0) - 1)
    def _():
        n = send_ref.shape[1]
        for j in range(send_ref.shape[0]):
            send_ref[j] = gacc_ref[j * n:(j + 1) * n].astype(BF16)

    final = pl.num_programs(0) - 1
    run_at(pl.program_id(0), final, to_mate.start)
    ring_sum.behind(pl.program_id(0), final)
    run_at(pl.program_id(0), final, to_mate.wait)


def out_kernel(x_ref, w_ref, prev_ref, *refs, stages):
    core = lax.axis_index('core')
    o_refs, (y_ref, total_ref, lhs_ref) = refs[:PAIR * stages], refs[PAIR * stages:PAIR * stages + 3]
    ring_sum = RingSum(prev_ref, [total_ref], (1, 2), 0, *refs[PAIR * stages + 3:])
    ring_sum.ahead(pl.program_id(0))
    nb, tok, d = x_ref.shape
    rows = o_refs[0].shape[2]
    half = stages * rows
    for side in range(2):
        base = (core if side == 0 else 1 - core) * half
        for s in range(stages):
            for b in range(nb):
                lhs_ref[b * tok:(b + 1) * tok, pl.ds(pl.multiple_of(base + s * rows, rows), rows)] = o_refs[side * stages + s][0, b].T
    lhs = lhs_ref[:]
    step = 512
    for c in range(0, d, step):
        prod = dot(lhs, w_ref[:, c:c + step])
        y_ref[:, :, c:c + step] = (x_ref[:, :, c:c + step].astype(F32) + prod.reshape(nb, tok, step)).astype(BF16)

    ring_sum.behind(pl.program_id(0), pl.num_programs(0) - 1)


def norm_grad_kernel(x_ref, go_ref, g_ref, w_ref, kv0_ref, kv1_ref, prev_ref, *refs, stages):
    core = lax.axis_index('core')
    q_refs = refs[:PAIR * stages]
    gh_ref, tail_ref, lhs_ref, tot_ref, gn_ref = refs[PAIR * stages:PAIR * stages + 5]
    n_kv = prev_ref.shape[1]
    ring_sum = RingSum(prev_ref, [tail_ref.at[pl.ds(0, n_kv)]], (1, 1), 0, *refs[PAIR * stages + 5:])
    ring_sum.ahead(pl.program_id(0))
    nb, tok, d = x_ref.shape
    rows = q_refs[0].shape[2]
    half = stages * rows
    e2 = kv0_ref.shape[1] // stages
    e = e2 // 2
    kv_half = stages * e
    for side in range(2):
        who = core if side == 0 else 1 - core
        kv_ref = kv0_ref if side == 0 else kv1_ref
        for b in range(nb):
            ts = slice(b * tok, (b + 1) * tok)
            for s in range(stages):
                lhs_ref[ts, pl.ds(pl.multiple_of(who * half + s * rows, rows), rows)] = q_refs[side * stages + s][0, b].T
            ks = cat_rows([kv_ref[b, i * e2:i * e2 + e] for i in range(stages)])
            vs = cat_rows([kv_ref[b, i * e2 + e:(i + 1) * e2] for i in range(stages)])
            base = PAIR * half
            lhs_ref[ts, pl.ds(pl.multiple_of(base + who * kv_half, kv_half), kv_half)] = ks.T
            base = base + PAIR * kv_half
            lhs_ref[ts, pl.ds(pl.multiple_of(base + who * kv_half, kv_half), kv_half)] = vs.T
    lhs = lhs_ref[:]
    step = 256
    for c in range(0, d, step):
        tot_ref[:, c:c + step] = dot(lhs, w_ref[c:c + step, :], NT)

    @pl.when(pl.program_id(0) == 0)
    def _():
        gn_ref[:] = jnp.zeros_like(gn_ref)

    g = g_ref[:].astype(F32)
    for b in range(nb):
        total = tot_ref[b * tok:(b + 1) * tok]
        x = x_ref[b].astype(F32)
        inv = lax.rsqrt(row_mean(x * x) + NORM_EPS)
        unit = x * inv
        gu = total * g
        mean_dot = row_mean(gu * unit)
        gh_ref[b] = (go_ref[b].astype(F32) + inv * (gu - unit * mean_dot)).astype(BF16)
        gn_ref[:] += jnp.sum((total * unit).reshape(tok // 8, 8, d), axis=0)

    @pl.when(pl.program_id(0) == pl.num_programs(0) - 1)
    def _():
        extra = tail_ref.shape[0] - n_kv
        total = column_sum(gn_ref[:])
        high = total.astype(BF16).astype(F32)
        row = lax.broadcasted_iota(jnp.int32, (extra, d), 0)
        tail_ref[n_kv:] = jnp.where(row == 0, high, jnp.where(row == 1, total - high, 0.0)).astype(BF16)

    ring_sum.behind(pl.program_id(0), pl.num_programs(0) - 1)


def transpose_to(out_ref, blk):
    for c in range(0, blk.shape[1], 256):
        out_ref[c:c + 256, :] = blk[:, c:c + 256].astype(F32).T


def assemble_main_kernel(*refs, stages, n_q):
    ins, (y_ref, gh_ref, wq_ref, wo_ref, y_out, gh_out) = refs[:stages], refs[stages:]
    y_out[:] = y_ref[:]
    gh_out[:] = gh_ref[:]
    for s in range(stages):
        @pl.when(pl.program_id(1) == s)
        def _(ref=ins[s]):
            chips, _, n, d = ref.shape
            transpose_to(wq_ref, ref[:, 0, 0:n_q].reshape(chips * n_q, d))
            wo_ref[:] = ref[:, 0, n_q:n].astype(F32)


def assemble_tail_kernel(in_ref, gn_ref, _, out_ref, norm_ref):
    norm_ref[:] = jnp.sum(gn_ref[:].astype(F32), axis=(0, 1, 2)).reshape(norm_ref.shape)
    chips, _, n, d = in_ref.shape
    transpose_to(out_ref, in_ref[:, 0].reshape(chips * n, d))


def solution(mesh):
    chips = mesh.shape['sp'] // CORES
    mesh2 = Mesh(mesh.devices.reshape(mesh.shape['dp'], chips, CORES), ('dp', 'x', 'core'))
    swap = [(i, CORES - 1 - i) for i in range(CORES)]

    def device_step(hidden, norm_w, w_qkv, w_out, long_factor, grad_out):
        n_batch, tok, d = hidden.shape
        n_heads, e = w_out.shape[0], w_out.shape[1]
        kv_heads = (w_qkv.shape[1] // e - n_heads) // 2
        reps = n_heads // kv_heads
        stages = kv_heads // CORES
        rows = reps * e
        q_half = stages * rows
        kv_half = stages * e
        e2 = PAIR * e
        half_rot = long_factor.shape[0]
        chip = lax.axis_index('x')
        core = lax.axis_index('core')
        ids = jnp.stack([chip, core]).astype(jnp.int32)
        tiles = 4
        nb = n_batch // tiles

        x_par = lax.ppermute(hidden, 'core', swap)
        go_par = lax.ppermute(grad_out, 'core', swap)
        w_o = w_out.reshape(n_heads * e, d)
        norm2 = norm_w.reshape(1, d)

        exponent = jnp.arange(half_rot, dtype=F32) / half_rot
        inv_freq = 1.0 / (long_factor * jnp.power(ROPE_BASE, exponent))
        sides = jnp.stack([core, 1 - core])
        positions = ((chip * CORES + sides)[:, None] * tok + jnp.arange(tok)[None, :]).astype(F32)
        angles = inv_freq[None, :, None] * positions[:, None, :]
        cos_t, sin_t = jnp.cos(angles) * ROPE_GAIN, jnp.sin(angles) * ROPE_GAIN

        tok_spec = along(0, nb, tok, d)
        rot_spec = whole(half_rot, tok)

        def kv_proj(x, side, filled):
            kb = PAIR * q_half // kv_half
            kt = 4
            kn = n_batch // kt
            x_spec = along(0, kn, tok, d)
            any_spec = pl.BlockSpec(memory_space=pl.ANY)
            return pl.pallas_call(
                drop_scalar(kv_proj_kernel),
                out_shape=[jax.ShapeDtypeStruct((n_batch, tok, d), BF16)]
                + [jax.ShapeDtypeStruct((2, n_batch, e2, tok), BF16)] * PAIR
                + [jax.ShapeDtypeStruct((stages - 2, 2, n_batch, e2, tok), BF16)],
                grid_spec=pltpu.PrefetchScalarGridSpec(
                    num_scalar_prefetch=1, grid=(kt,),
                    in_specs=[x_spec, whole(1, d),
                              pl.BlockSpec((d, kv_half), lambda i, c: (0, kb + c[1])),
                              pl.BlockSpec((d, kv_half), lambda i, c: (0, kb + CORES + c[1])), rot_spec, rot_spec]
                    + [any_spec] * len(filled),
                    out_specs=[x_spec] + [pl.BlockSpec((1, kn, e2, tok), lambda i, _: (side, i, 0, 0))] * PAIR
                    + [pl.BlockSpec((stages - 2, 1, kn, e2, tok), lambda i, _: (0, side, i, 0, 0))]),
                input_output_aliases={7 + i: 1 + i for i in range(len(filled))},
                compiler_params=params(), name='kv_proj',
                cost_estimate=cost(PAIR * n_batch * tok * d * PAIR * kv_half, 3 * n_batch * tok * d * 2),
            )(ids, x, norm2, w_qkv, w_qkv, cos_t[side], sin_t[side], *filled)

        first = lambda i: jnp.minimum(i, tiles - 1)
        second = lambda i: jnp.maximum(i - tiles, 0)
        own_spec = pl.BlockSpec((nb, tok, d), lambda i, _: (first(i), 0, 0))
        par_spec = pl.BlockSpec((nb, tok, d), lambda i, _: (second(i), 0, 0))
        own_out = pl.BlockSpec((nb, q_half, tok), lambda i, _: (first(i), 0, 0))
        par_out = pl.BlockSpec((nb, q_half, tok), lambda i, _: (second(i), 0, 0))
        both_rot = whole(2, half_rot, tok)
        q_shapes = [jax.ShapeDtypeStruct((n_batch, q_half, tok), BF16)] * PAIR

        def q_do_proj(h0, h1, g0, g1):
            return pl.pallas_call(
                drop_scalar(q_do_proj_kernel), out_shape=q_shapes * PAIR,
                grid_spec=pltpu.PrefetchScalarGridSpec(
                    num_scalar_prefetch=1, grid=(PAIR * tiles,),
                    in_specs=[own_spec, par_spec, own_spec, par_spec, pl.BlockSpec((d, q_half), lambda i, c: (0, c[1])),
                              pl.BlockSpec((q_half, d), lambda i, c: (c[1], 0)), both_rot, both_rot],
                    out_specs=[own_out, par_out] * PAIR),
                compiler_params=params(), name='q_do_proj',
                cost_estimate=cost(8 * n_batch * tok * d * q_half, 8 * n_batch * tok * d * 2),
            )(ids, h0, h1, g0, g1, w_qkv, w_o, cos_t, sin_t)

        h_own, *kv_sides = kv_proj(hidden, 0, [])
        h_par, *kv_sides = kv_proj(x_par, 1, kv_sides)
        gathered = [lax.all_gather(kv, 'x') for kv in kv_sides]
        q_own, q_par, do_own, do_par = q_do_proj(h_own, h_par, grad_out, go_par)

        n_g = PAIR * rows // chips
        n_s = e2 + n_g
        hbm = pl.BlockSpec(memory_space=pl.ANY)
        shard_spec = lambda n: whole(n, d)

        def gather_shard(shard):
            return lax.all_gather(shard, ('x', 'core')).reshape(chips, CORES, *shard.shape)

        def attention(s, prev):
            blk = PAIR * tok
            has_sum = prev is not None
            if s < 2:
                kv_spec = along(2, chips, 2, 1, e2, tok)
            else:
                kv_spec = pl.BlockSpec((chips, None, 2, 1, e2, tok), lambda b: (0, s - 2, 0, b, 0, 0))
            q_spec = pl.BlockSpec((1, rows, tok), lambda b: (b, s, 0))
            t_spec = pl.BlockSpec((2, tok, d), lambda b: (b // 2, 0, 0))
            r_spec = whole(2, half_rot, tok)
            o_spec = along(1, 2, 1, rows, tok)
            return pl.pallas_call(
                functools.partial(attn_kernel, has_sum=has_sum),
                out_shape=[jax.ShapeDtypeStruct((2, n_batch, rows, tok), BF16)] * 2
                + [jax.ShapeDtypeStruct((chips, n_s, d), BF16)]
                + [jax.ShapeDtypeStruct((n, d), BF16) for n in (e2, n_g)] * has_sum,
                grid=(n_batch,),
                in_specs=[q_spec, q_spec, q_spec, q_spec, kv_spec,
                          t_spec, t_spec, t_spec, t_spec, r_spec, r_spec]
                + [hbm] * has_sum,
                out_specs=[o_spec, hbm, whole(chips, n_s, d)]
                + [shard_spec(e2), shard_spec(n_g)] * has_sum,
                scratch_shapes=[pltpu.VMEM((chips, blk, reps * blk), F32), pltpu.VMEM((chips, blk, reps * blk), BF16),
                                pltpu.VMEM((chips, blk, reps * blk), BF16), pltpu.VMEM((e, reps * blk), F32),
                                pltpu.VMEM((8, reps * blk), F32),
                                pltpu.VMEM((chips, blk, e2), BF16), pltpu.VMEM((2, PAIR * rows, blk), BF16),
                                pltpu.VMEM((PAIR * rows, d), F32), pltpu.VMEM((PAIR, n_batch, rows, tok), BF16),
                                pltpu.SemaphoreType.DMA((PAIR,)), pltpu.SemaphoreType.DMA((PAIR,))]
                + RingSum.scratch(n_s, d) * has_sum,
                compiler_params=comm_params(s),
                cost_estimate=cost(4e10, 3e7, 3e7),
            )(q_own, q_par, do_own, do_par, gathered[min(s, 2)], h_own, h_par, grad_out, go_par, cos_t, sin_t,
              *([prev] * has_sum))

        own, par, totals, main = [], [], [], []
        prev = None
        for s in range(stages):
            own_s, other_s, send, *sums = attention(s, prev)
            own.append(own_s)
            par.append(other_s)
            prev = send
            totals += sums[:1]
            main += [gather_shard(g) for g in sums[1:]]

        nb2 = 2
        t2_spec = along(0, nb2, tok, d)
        block_out, total = pl.pallas_call(
            functools.partial(out_kernel, stages=stages),
            out_shape=[jax.ShapeDtypeStruct((n_batch, tok, d), BF16), jax.ShapeDtypeStruct((e2, d), BF16)],
            grid=(n_batch // nb2,),
            in_specs=[t2_spec, whole(n_heads * e, d), hbm]
            + [along(1, 1, nb2, rows, tok)] * (PAIR * stages),
            out_specs=[t2_spec, shard_spec(e2)],
            scratch_shapes=[pltpu.VMEM((nb2 * tok, n_heads * e), BF16)] + RingSum.scratch(e2, d),
            compiler_params=comm_params(stages), name='out_proj',
            cost_estimate=cost(PAIR * n_batch * tok * d * n_heads * e, 3e7),
        )(hidden, w_o, prev, *own, *par)
        totals.append(total)

        gb = 2
        gf_spec = along(0, gb, stages * e2, tok)
        n_kv = stages * e2 // chips
        kv_own_g, kv_other_g, send_kv, shard = pl.pallas_call(
            functools.partial(kv_grad_kernel, stages=stages),
            out_shape=[jax.ShapeDtypeStruct((n_batch, stages * e2, tok), BF16)] * 2
            + [jax.ShapeDtypeStruct((chips, n_kv, d), BF16), jax.ShapeDtypeStruct((n_g, d), BF16)],
            grid=(n_batch // gb,),
            in_specs=[along(1, e2, PAIR * tok * gb)] * stages
            + [along(0, gb, tok, d)] * 2 + [whole(2, half_rot, tok)] * 2
            + [hbm],
            out_specs=[gf_spec, hbm, whole(chips, n_kv, d), shard_spec(n_g)],
            scratch_shapes=[pltpu.VMEM((stages * e2, d), F32), pltpu.VMEM((n_batch, stages * e2, tok), BF16),
                            pltpu.SemaphoreType.DMA((1,)), pltpu.SemaphoreType.DMA((1,))] + RingSum.scratch(n_g, d),
            compiler_params=comm_params(stages + 1), name='kv_grad',
            cost_estimate=cost(PAIR * PAIR * n_batch * tok * d * stages * e2, 3e7),
        )(*totals, h_own, h_par, cos_t, sin_t, prev)
        main.append(gather_shard(shard))

        nb3 = 2
        t3_spec = along(0, nb3, tok, d)
        n_t = n_kv + 16
        grad_hidden, tail_block = pl.pallas_call(
            functools.partial(norm_grad_kernel, stages=stages),
            out_shape=[jax.ShapeDtypeStruct((n_batch, tok, d), BF16), jax.ShapeDtypeStruct((n_t, d), BF16)],
            grid=(n_batch // nb3,),
            in_specs=[t3_spec, t3_spec, whole(1, d), whole(*w_qkv.shape)]
            + [along(0, nb3, stages * e2, tok)] * 2 + [hbm]
            + [pl.BlockSpec((1, nb3, rows, tok), lambda b: (1, b, 0, 0))] * (PAIR * stages),
            out_specs=[t3_spec, shard_spec(n_t)],
            scratch_shapes=[pltpu.VMEM((nb3 * tok, w_qkv.shape[1]), BF16), pltpu.VMEM((nb3 * tok, d), F32), pltpu.VMEM((8, d), F32)]
            + RingSum.scratch(n_kv, d),
            compiler_params=comm_params(stages + 2), name='norm_grad',
            cost_estimate=cost(PAIR * n_batch * tok * d * w_qkv.shape[1], 4e7),
        )(hidden, grad_out, norm2, w_qkv, kv_own_g, kv_other_g, send_kv, *own, *par)

        tail = gather_shard(tail_block)
        n_q = rows // chips
        b_spec = pl.BlockSpec((n_batch // (CORES * stages), tok, d), lambda p, s: (p * stages + s, 0, 0))
        w_cols, grad_w_out, block_out, grad_hidden = pl.pallas_call(
            functools.partial(assemble_main_kernel, stages=stages, n_q=n_q),
            out_shape=[jax.ShapeDtypeStruct(w_qkv.shape, F32), jax.ShapeDtypeStruct((n_heads, e, d), F32)]
            + [jax.ShapeDtypeStruct((n_batch, tok, d), BF16)] * PAIR,
            grid=(CORES, stages),
            in_specs=[along(1, chips, 1, n_g, d)] * stages + [b_spec] * PAIR,
            out_specs=[pl.BlockSpec((d, rows), lambda p, s: (0, p * stages + s)),
                       pl.BlockSpec((reps, e, d), lambda p, s: (p * stages + s, 0, 0)), b_spec, b_spec],
            compiler_params=params(2), name='assemble_main', cost_estimate=cost(2e9, 6e7),
        )(*main, block_out, grad_hidden)
        kcol = PAIR * q_half // kv_half
        extra = n_t - n_kv
        grad_w_qkv, grad_norm_w = pl.pallas_call(
            assemble_tail_kernel,
            out_shape=[jax.ShapeDtypeStruct(w_qkv.shape, F32), jax.ShapeDtypeStruct((1, d), F32)],
            grid=(CORES, PAIR),
            in_specs=[pl.BlockSpec((chips, 1, e, d), lambda p, k: (0, p, k, 0)),
                      pl.BlockSpec((chips, CORES, extra, d), lambda p, k: (0, 0, n_kv // extra, 0)),
                      pl.BlockSpec(memory_space=pl.ANY)],
            out_specs=[pl.BlockSpec((d, kv_half), lambda p, k: (0, kcol + k * CORES + p)), whole(1, d)],
            input_output_aliases={2: 0},
            compiler_params=params(2), name='assemble_tail', cost_estimate=cost(1e9, 2e7),
        )(tail, tail, w_cols)
        grad_norm_w = grad_norm_w.reshape(d)
        return block_out, grad_hidden, grad_w_qkv, grad_w_out, grad_norm_w

    tok_spec = P('dp', ('x', 'core'), None)
    return jax.shard_map(device_step, mesh=mesh2,
                         in_specs=(tok_spec, P(), P(), P(), P(), tok_spec),
                         out_specs=(tok_spec, tok_spec, P('dp', None), P('dp', None, None), P('dp')),
                         check_vma=False)
```
